256 devices in a mesh: dom: 64 (over y, z, core), grp: 4 (over x).
Axes of the slice: x: 4, y: 4, z: 8, core: 2. Of those that a mesh axis runs over, the one named last changes fastest.
Arguments:
- nodes: bfloat16 [4, 32768, 128], P('grp', 'dom'), may hold values from -6 to 6
- edges: bfloat16 [4, 256, 128, 128], P('grp', 'dom'), may hold values from -6 to 6
- senders: int32 [4, 256, 128], P('grp', 'dom'), may hold values from 0 to 767
- receivers: int32 [4, 256, 128], P('grp', 'dom'), may hold values from 0 to 511
- block_count: int32 [4, 64], P('grp', 'dom'), may hold values from 1 to 4
- send_rows: int32 [4, 64, 2, 128], P('grp', 'dom'), may hold values from 0 to 511
- node_cot: bfloat16 [4, 32768, 128], P('grp', 'dom'), may hold values from -6 to 6
- edge_cot: bfloat16 [4, 256, 128, 128], P('grp', 'dom'), may hold values from -6 to 6
- edge_w1: bfloat16 [384, 128], replicated, may hold values from -0.3125 to 0.3125
- edge_b1: float32 [128], replicated, may hold values from -3 to 3
- edge_w2: bfloat16 [128, 128], replicated, may hold values from -0.5 to 0.5
- edge_b2: float32 [128], replicated, may hold values from -3 to 3
- edge_gain: float32 [128], replicated, may hold values from 0.5 to 1.5
- edge_shift: float32 [128], replicated, may hold values from -3 to 3
- node_w1: bfloat16 [256, 128], replicated, may hold values from -0.375 to 0.375
- node_b1: float32 [128], replicated, may hold values from -3 to 3
- node_w2: bfloat16 [128, 128], replicated, may hold values from -0.5 to 0.5
- node_b2: float32 [128], replicated, may hold values from -3 to 3
- node_gain: float32 [128], replicated, may hold values from 0.5 to 1.5
- node_shift: float32 [128], replicated, may hold values from -3 to 3
Outputs:
- node_out: bfloat16 [4, 32768, 128], P('grp', 'dom')
- edge_out: bfloat16 [4, 256, 128, 128], P('grp', 'dom')
- grad_node: bfloat16 [4, 32768, 128], P('grp', 'dom')
- grad_edge: bfloat16 [4, 256, 128, 128], P('grp', 'dom')
- weight_grads: float32 [115712], replicated
The draws below stay inside these ranges and needn't reach their ends.
Inputs may be any that keep to these rules, and one draw needn't show every extreme that they name: `senders`: rows below 512 are the device's own nodes; row 512 + k holds the k-th row sent by the lower neighbouring partition, row 640 + k the k-th row sent by the upper one. `receivers`: receivers are own nodes of the device that holds the edge. `block_count`: A device's live blocks are its first ones; the rest are padding. send_rows[g, d, 0, :] are own rows of device d sent to device d - 1 of group g, send_rows[g, d, 1, :] those sent to device d + 1; they may repeat; lists toward no device are unused.
All inputs are finite; a program needn't handle non-finite values.
Results may differ from the reference program's by a relative error of at most 0.0054.
Values may be sent and summed in bfloat16 or wider, within the bound.
No kernel may reach another device: no remote copies, remote signals or barrier semaphores. Data moves between devices by JAX's collectives and lax.ppermute only.
A program may use at most 64 MiB of HBM per device.

```python
import math
import jax
import jax.numpy as jnp
from jax import lax

LAT = 128
HID = 128
NODE_DEV = 512
BLOCKS = 4
EBLOCK = 128
SLOTS = 128
GROUPS = 4
NODES = 32768
EDGE_BLOCKS = 256
N_DOM = 64
N_GRP = 4


def touch_ends(array, own_key, low, top_value):
    index_at = [jax.random.randint(jax.random.fold_in(own_key, axis), (), 0, length) for axis, length in enumerate(array.shape)]
    main_axis = array.shape.index(max(array.shape))
    neighbour = index_at[:main_axis] + [(index_at[main_axis] + 1) % array.shape[main_axis]] + index_at[main_axis + 1:]
    return array.at[tuple(index_at)].set(low).at[tuple(neighbour)].set(top_value)


def steps_of(key, dims, split, smallest, high):
    def one(position, shards_of):
        steps = jax.random.uniform(jax.random.fold_in(jax.random.fold_in(key, 6), position), (shards_of,), jnp.float32, smallest / len(split), high / len(split))
        return jnp.repeat(jnp.exp(steps), dims[position] // shards_of).reshape((-1,) + (1,) * (len(dims) - position - 1))

    factor_of = one(*split[0])
    for cut in split[1:]:
        factor_of = factor_of * one(*cut)
    return factor_of


def bell_draw(own_key, dims, scale, reach, pieces=(), kind=jnp.bfloat16):
    drawn = jax.random.normal(own_key, dims, jnp.float32) * scale
    if len(pieces) > 0:
        drawn = steps_of(own_key, dims, pieces, -0.22, 0.18) * drawn
    return jnp.clip(drawn, min=-reach, max=reach).astype(kind)


def setup_inputs(seed: int = 0) -> dict:
    arg_keys = jax.random.split(jax.random.key(seed), 21)
    nodes = bell_draw(arg_keys[0], (GROUPS, NODES, LAT), 1.0, 6.0, ((0, 4), (1, 64)))
    edges = bell_draw(arg_keys[1], (GROUPS, EDGE_BLOCKS, EBLOCK, LAT), 1.0, 6.0, ((0, 4), (1, 64)))
    senders = touch_ends(jax.random.randint(arg_keys[2], (GROUPS, EDGE_BLOCKS, EBLOCK), 0, NODE_DEV + 2 * SLOTS), jax.random.fold_in(arg_keys[2], 1), 0, (NODE_DEV + 2 * SLOTS) - 1).astype(jnp.int32)
    receivers = touch_ends(jax.random.randint(arg_keys[3], (GROUPS, EDGE_BLOCKS, EBLOCK), 0, NODE_DEV), jax.random.fold_in(arg_keys[3], 1), 0, NODE_DEV - 1).astype(jnp.int32)
    block_count = touch_ends(jax.random.randint(arg_keys[4], (GROUPS, N_DOM), max(1, BLOCKS // 4), BLOCKS + 1), jax.random.fold_in(arg_keys[4], 1), max(1, BLOCKS // 4), BLOCKS).astype(jnp.int32)
    send_rows = touch_ends(jax.random.randint(arg_keys[5], (GROUPS, N_DOM, 2, SLOTS), 0, NODE_DEV), jax.random.fold_in(arg_keys[5], 1), 0, NODE_DEV - 1).astype(jnp.int32)
    node_cot = bell_draw(arg_keys[6], (GROUPS, NODES, LAT), 1.0, 6.0, ((0, 4), (1, 64)))
    edge_cot = bell_draw(arg_keys[7], (GROUPS, EDGE_BLOCKS, EBLOCK, LAT), 1.0, 6.0, ((0, 4), (1, 64)))
    edge_w1 = bell_draw(arg_keys[8], (3 * LAT, HID), (3 * LAT) ** -0.5, 0.3125)
    edge_b1 = bell_draw(arg_keys[9], (HID,), 0.5, 3.0, (), jnp.float32)
    edge_w2 = bell_draw(arg_keys[10], (HID, LAT), HID ** -0.5, 0.5)
    edge_b2 = bell_draw(arg_keys[11], (LAT,), 0.5, 3.0, (), jnp.float32)
    edge_gain = jnp.clip(1.0 + 0.1 * jax.random.normal(arg_keys[12], (LAT,), jnp.float32), 0.5, 1.5)
    edge_shift = bell_draw(arg_keys[13], (LAT,), 0.5, 3.0, (), jnp.float32)
    node_w1 = bell_draw(arg_keys[14], (2 * LAT, HID), (2 * LAT) ** -0.5, 0.375)
    node_b1 = bell_draw(arg_keys[15], (HID,), 0.5, 3.0, (), jnp.float32)
    node_w2 = bell_draw(arg_keys[16], (HID, LAT), HID ** -0.5, 0.5)
    node_b2 = bell_draw(arg_keys[17], (LAT,), 0.5, 3.0, (), jnp.float32)
    node_gain = jnp.clip(1.0 + 0.1 * jax.random.normal(arg_keys[18], (LAT,), jnp.float32), 0.5, 1.5)
    node_shift = bell_draw(arg_keys[19], (LAT,), 0.5, 3.0, (), jnp.float32)
    return dict(nodes=nodes, edges=edges, senders=senders, receivers=receivers, block_count=block_count, send_rows=send_rows, node_cot=node_cot, edge_cot=edge_cot, edge_w1=edge_w1, edge_b1=edge_b1, edge_w2=edge_w2, edge_b2=edge_b2, edge_gain=edge_gain, edge_shift=edge_shift, node_w1=node_w1, node_b1=node_b1, node_w2=node_w2, node_b2=node_b2, node_gain=node_gain, node_shift=node_shift)


EPSILON = 1e-05

def norm_forward(pre_norm, norm_gain, norm_shift):
    average = lax.optimization_barrier(jnp.mean(pre_norm, axis=-1, keepdims=True))
    centred = pre_norm - average
    variance = lax.optimization_barrier(jnp.mean(centred * centred, axis=-1, keepdims=True))
    inverse = lax.rsqrt(variance + EPSILON)
    normed = centred * inverse
    return (normed * norm_gain + norm_shift, normed, inverse)

def norm_backward(grad_out, normed, inverse, norm_gain):
    scaled = grad_out * norm_gain
    return inverse * (scaled - lax.optimization_barrier(jnp.mean(scaled, axis=-1, keepdims=True)) - normed * lax.optimization_barrier(jnp.mean(scaled * normed, axis=-1, keepdims=True)))

def silu_slope(pre_act):
    sigmoid = jax.nn.sigmoid(pre_act)
    return sigmoid * (1.0 + pre_act * (1.0 - sigmoid))

def row_product(left, right):
    return lax.dot_general(left, right, (((0,), (0,)), ((), ())), preferred_element_type=jnp.float32)

def mlp_forward(inputs, weights):
    w_first, b_first, w_second, b_second, norm_gain, norm_shift = weights
    first_pre = jnp.dot(inputs, w_first, preferred_element_type=jnp.float32) + b_first
    hidden = jax.nn.silu(first_pre).astype(jnp.bfloat16)
    second_pre = jnp.dot(hidden, w_second, preferred_element_type=jnp.float32) + b_second
    output, normed, inverse = norm_forward(second_pre, norm_gain, norm_shift)
    return (output, (first_pre, hidden, normed, inverse))

def mlp_backward(inputs, saved, grad_out, weights):
    w_first, b_first, w_second, b_second, norm_gain, norm_shift = weights
    first_pre, hidden, normed, inverse = saved
    grad_second = norm_backward(grad_out, normed, inverse, norm_gain)
    second_low = grad_second.astype(jnp.bfloat16)
    grad_hidden = jnp.dot(second_low, w_second.T, preferred_element_type=jnp.float32)
    grad_first = grad_hidden * silu_slope(first_pre)
    first_low = grad_first.astype(jnp.bfloat16)
    grad_inputs = jnp.dot(first_low, w_first.T, preferred_element_type=jnp.float32)
    grads = (row_product(inputs, first_low), lax.optimization_barrier(jnp.sum(grad_first, axis=0)), row_product(hidden, second_low), lax.optimization_barrier(jnp.sum(grad_second, axis=0)), lax.optimization_barrier(jnp.sum(grad_out * normed, axis=0)), lax.optimization_barrier(jnp.sum(grad_out, axis=0)))
    return (grad_inputs, grads)

def device_pass(own_nodes, halo_rows, edge_feats, sender_ids, receiver_ids, live_blocks, node_grad_in, edge_grad_in, edge_weights, node_weights):
    node_rows, width = own_nodes.shape
    block_rows = sender_ids.shape[1]
    flat_edges = edge_feats.reshape(-1, width)
    flat_send = sender_ids.reshape(-1)
    flat_recv = receiver_ids.reshape(-1)
    edge_rows = flat_send.shape[0]
    live_mask = (jnp.arange(edge_rows, dtype=jnp.int32) // block_rows < live_blocks).astype(jnp.float32)[:, None]
    node_table = jnp.concatenate([own_nodes, halo_rows], axis=0)
    inputs = jnp.concatenate([flat_edges, node_table[flat_send], own_nodes[flat_recv]], axis=1)
    message, edge_saved = mlp_forward(inputs, edge_weights)
    live_message = message * live_mask
    aggregate = jnp.zeros((node_rows, width), jnp.float32).at[flat_recv].add(live_message)
    edge_out = (flat_edges.astype(jnp.float32) + live_message).astype(jnp.bfloat16)
    node_inputs = jnp.concatenate([own_nodes, aggregate.astype(jnp.bfloat16)], axis=1)
    update, node_saved = mlp_forward(node_inputs, node_weights)
    node_out = (own_nodes.astype(jnp.float32) + update).astype(jnp.bfloat16)
    node_grad = node_grad_in.astype(jnp.float32)
    grad_node_inputs, node_grads = mlp_backward(node_inputs, node_saved, node_grad, node_weights)
    flat_cot = edge_grad_in.reshape(-1, width).astype(jnp.float32)
    grad_message = live_mask * (flat_cot + grad_node_inputs[:, width:][flat_recv])
    grad_inputs, edge_grads = mlp_backward(inputs, edge_saved, grad_message, edge_weights)
    grad_edge = (flat_cot + grad_inputs[:, :width]).astype(jnp.bfloat16)
    table_grad = jnp.zeros((node_table.shape[0], width), jnp.float32).at[flat_send].add(grad_inputs[:, width:2 * width])
    recv_grad = jnp.zeros((node_rows, width), jnp.float32).at[flat_recv].add(grad_inputs[:, 2 * width:])
    local_grad = node_grad + grad_node_inputs[:, :width] + table_grad[:node_rows] + recv_grad
    flat_grads = jnp.concatenate([piece.reshape(-1) for piece in edge_grads + node_grads])
    return (node_out, edge_out.reshape(edge_feats.shape), grad_edge.reshape(edge_feats.shape), local_grad, table_grad[node_rows:], flat_grads)

def reference(nodes, edges, senders, receivers, block_count, send_rows, node_cot, edge_cot, edge_w1, edge_b1, edge_w2, edge_b2, edge_gain, edge_shift, node_w1, node_b1, node_w2, node_b2, node_gain, node_shift):
    edge_weights = (edge_w1, edge_b1, edge_w2, edge_b2, edge_gain, edge_shift)
    node_weights = (node_w1, node_b1, node_w2, node_b2, node_gain, node_shift)
    group_count = nodes.shape[0]
    width = nodes.shape[2]
    owners = jnp.arange(N_DOM, dtype=jnp.int32)[None, :, None] * NODE_DEV
    to_lower = (send_rows[:, :, 0, :] + owners).astype(jnp.int32)
    to_upper = (send_rows[:, :, 1, :] + owners).astype(jnp.int32)
    from_lower = jnp.roll(to_upper, 1, axis=1)
    from_upper = jnp.roll(to_lower, -1, axis=1)
    places = jnp.arange(N_DOM, dtype=jnp.int32)
    lower_valid = (places > 0).astype(jnp.float32)[None, :, None, None]
    upper_valid = (places < N_DOM - 1).astype(jnp.float32)[None, :, None, None]
    flat_rows = jnp.concatenate([from_lower, from_upper], axis=2).reshape(group_count, -1)
    valid = jnp.concatenate([jnp.broadcast_to(lower_valid, (group_count, N_DOM, SLOTS, 1)), jnp.broadcast_to(upper_valid, (group_count, N_DOM, SLOTS, 1))], axis=2)
    halo_all = jax.vmap(lambda node_table, row_ids: node_table[row_ids])(nodes, flat_rows)
    halo_all = (halo_all.reshape(group_count, N_DOM, 2 * SLOTS, width).astype(jnp.float32) * valid).astype(jnp.bfloat16)
    devices = group_count * N_DOM
    packed = (nodes.reshape(devices, NODE_DEV, width), halo_all.reshape(devices, 2 * SLOTS, width), edges.reshape(devices, BLOCKS, EBLOCK, width), senders.reshape(devices, BLOCKS, EBLOCK), receivers.reshape(devices, BLOCKS, EBLOCK), block_count.reshape(devices), node_cot.reshape(devices, NODE_DEV, width), edge_cot.reshape(devices, BLOCKS, EBLOCK, width))

    def run_device(device_item):
        return device_pass(*device_item, edge_weights, node_weights)
    node_out, edge_out, grad_edge, local_grad, halo_grad, device_grads = lax.map(run_device, packed)

    def scatter_back(row_ids, values):
        return jnp.zeros((N_DOM * NODE_DEV, width), jnp.float32).at[row_ids].add(values)
    masked_grad = halo_grad.reshape(group_count, N_DOM, 2 * SLOTS, width) * valid
    returned = jax.vmap(scatter_back)(flat_rows, masked_grad.reshape(group_count, -1, width))
    grad_node = (local_grad.reshape(group_count, N_DOM * NODE_DEV, width) + returned).astype(jnp.bfloat16)
    scale = 1.0 / math.sqrt(N_GRP * N_DOM * BLOCKS * EBLOCK)
    weight_grads = lax.optimization_barrier(jnp.sum(device_grads, axis=0)) * scale
    return (node_out.reshape(nodes.shape), edge_out.reshape(edges.shape), grad_node, grad_edge.reshape(edges.shape), weight_grads)
```

```python
import math

import jax
import jax.numpy as jnp
from jax import lax
from jax.experimental import pallas as pl
from jax.experimental.pallas import tpu as pltpu
from jax.sharding import Mesh
from jax.sharding import PartitionSpec as P

DOM = ("y", "z", "c")
PLANE = ("z", "x")
EPSILON = 1e-05
F32 = jnp.float32
BF16 = jnp.bfloat16
ROWS = 1024
HALF = 512
LIVE_ROWS = 904
VMEM = pl.BlockSpec(memory_space=pltpu.VMEM)
SMEM = pl.BlockSpec(memory_space=pltpu.SMEM)


def dot(left, right):
    return jnp.dot(left, right, preferred_element_type=F32)


def dot_nt(left, right):
    return lax.dot_general(left, right, (((1,), (1,)), ((), ())), preferred_element_type=F32)


def dot_tn(left, right):
    return lax.dot_general(left, right, (((0,), (0,)), ((), ())), preferred_element_type=F32)


def as_bf16(mask):
    return jnp.where(mask, 1.0, 0.0).astype(BF16)


def pick_rows(row, count):
    column = jnp.transpose(jnp.broadcast_to(row, (128, 128)))
    lanes = lax.broadcasted_iota(jnp.int32, (128, 128), 1)
    tiles = [as_bf16(column == lanes + 128 * j) for j in range(count // 128)]
    return jnp.concatenate(tiles, axis=1)


def place_rows(row, count):
    lines = lax.broadcasted_iota(jnp.int32, (count, 128), 0)
    return as_bf16(lines == row)


def split(value):
    high = value.astype(BF16)
    low = (value - high.astype(F32)).astype(BF16)
    return jnp.concatenate([high, low], axis=1)


def joined(value):
    return value[:, :128] + value[:, 128:]


def pack_kernel(nodes, lists, near, far):
    core = lax.axis_index("c")
    near[...] = dot(pick_rows(lists[pl.ds(1 - core, 1), :], 512), nodes[...]).astype(BF16)
    far[...] = dot(pick_rows(lists[pl.ds(core, 1), :], 512), nodes[...]).astype(BF16)


def norm_forward(second):
    average = jnp.mean(second, axis=-1, keepdims=True)
    centred = second - average
    variance = jnp.mean(centred * centred, axis=-1, keepdims=True)
    inverse = lax.rsqrt(variance + EPSILON)
    return centred * inverse, inverse


def norm_backward(cot, normed, inverse, gain):
    scaled = cot * gain
    return inverse * (
        scaled
        - jnp.mean(scaled, axis=-1, keepdims=True)
        - normed * jnp.mean(scaled * normed, axis=-1, keepdims=True)
    )


def partial_sum(value):
    return jnp.sum(value.reshape(-1, 8, 128), axis=0)


def total(value):
    return jnp.sum(value, axis=0, keepdims=True)


def main_kernel(
    count, nodes, near, far, edges, senders, receivers, node_cot, edge_cot,
    ew1, eb1, ew2, eb2, egain, eshift, nw1, nb1, nw2, nb2, ngain, nshift,
    node_out, edge_out, grad_edge, local_grad, near_grad, far_grad, keep, send,
    table, pick_recv, place_recv, place_send, messages, inputs, hidden, slope, normed, inverse,
    spread, dxs, dxr, first_low, second_low, node_inputs, node_hidden, node_first, node_second, grads,
):
    core = lax.axis_index("c")
    live_blocks = count[0, 0]
    table[pl.ds(0, 512), :] = nodes[...]
    table[pl.ds(pl.multiple_of(640 - 128 * core, 128), 128), :] = near[...]
    table[pl.ds(pl.multiple_of(512 + 128 * core, 128), 128), :] = far[...]

    for b in range(4):
        rows = pl.ds(b * 128, 128)
        live = jnp.where(b < live_blocks, 1.0, 0.0).astype(F32)
        send_row, recv_row = senders[pl.ds(b, 1), :], receivers[pl.ds(b, 1), :]
        pick = pick_rows(recv_row, 512)
        pick_recv[rows, :] = pick
        place_recv[:, rows] = place_rows(recv_row, 512)
        place_send[:, rows] = place_rows(send_row, 768)
        own = edges[rows, :]
        sender = dot(pick_rows(send_row, 768), table[...]).astype(BF16)
        receiver = dot(pick, nodes[...]).astype(BF16)
        gathered = jnp.concatenate([own, sender, receiver], axis=1)
        inputs[rows, :] = gathered
        first = dot(gathered, ew1[...]) + eb1[...]
        sigmoid = jax.nn.sigmoid(first)
        low = (first * sigmoid).astype(BF16)
        hidden[rows, :] = low
        slope[rows, :] = sigmoid * (1.0 + first * (1.0 - sigmoid))
        n, inv = norm_forward(dot(low, ew2[...]) + eb2[...])
        normed[rows, :] = n
        inverse[rows, :] = inv
        message = (n * egain[...] + eshift[...]) * live
        edge_out[rows, :] = (own.astype(F32) + message).astype(BF16)
        messages[rows, :] = split(message)

    sums = [jnp.zeros((8, 128), F32) for _ in range(8)]
    for b in range(4):
        rows = pl.ds(b * 128, 128)
        aggregate = joined(dot(place_recv[rows, :], messages[...])).astype(BF16)
        own = nodes[rows, :]
        gathered = jnp.concatenate([own, aggregate], axis=1)
        node_inputs[rows, :] = gathered
        first = dot(gathered, nw1[...]) + nb1[...]
        sigmoid = jax.nn.sigmoid(first)
        low = (first * sigmoid).astype(BF16)
        node_hidden[rows, :] = low
        n, inv = norm_forward(dot(low, nw2[...]) + nb2[...])
        node_out[rows, :] = (own.astype(F32) + (n * ngain[...] + nshift[...])).astype(BF16)
        cot = node_cot[rows, :].astype(F32)
        g2 = norm_backward(cot, n, inv, ngain[...])
        g2_low = g2.astype(BF16)
        g1 = dot_nt(g2_low, nw2[...]) * (sigmoid * (1.0 + first * (1.0 - sigmoid)))
        g1_low = g1.astype(BF16)
        node_first[rows, :] = g1_low
        node_second[rows, :] = g2_low
        back = dot_nt(g1_low, nw1[...])
        local_grad[rows, :] = cot + back[:, :128]
        spread[rows, :] = split(back[:, 128:])
        for k, piece in enumerate((g1, g2, cot * n, cot)):
            sums[4 + k] += partial_sum(piece)

    for b in range(4):
        rows = pl.ds(b * 128, 128)
        live = jnp.where(b < live_blocks, 1.0, 0.0).astype(F32)
        edge_grad = edge_cot[rows, :].astype(F32)
        cot = live * (edge_grad + joined(dot(pick_recv[rows, :], spread[...])))
        n = normed[rows, :]
        g2 = norm_backward(cot, n, inverse[rows, :], egain[...])
        g2_low = g2.astype(BF16)
        g1 = dot_nt(g2_low, ew2[...]) * slope[rows, :]
        g1_low = g1.astype(BF16)
        first_low[rows, :] = g1_low
        second_low[rows, :] = g2_low
        back = dot_nt(g1_low, ew1[...])
        grad_edge[rows, :] = (edge_grad + back[:, :128]).astype(BF16)
        dxs[rows, :] = split(back[:, 128:256])
        dxr[rows, :] = split(back[:, 256:])
        for k, piece in enumerate((g1, g2, cot * n, cot)):
            sums[k] += partial_sum(piece)

    lower = joined(dot(place_send[512:640, :], dxs[...])).astype(BF16)
    upper = joined(dot(place_send[640:768, :], dxs[...])).astype(BF16)
    is_first = core == 0
    near_grad[...] = jnp.where(is_first, upper, lower)
    far_grad[...] = jnp.where(is_first, lower, upper)

    grads[0:384, :] = dot_tn(inputs[...], first_low[...])
    grads[384:385, :] = total(sums[0])
    grads[385:513, :] = dot_tn(hidden[...], second_low[...])
    grads[513:514, :] = total(sums[1])
    grads[514:515, :] = total(sums[2])
    grads[515:516, :] = total(sums[3])
    grads[516:772, :] = dot_tn(node_inputs[...], node_first[...])
    grads[772:773, :] = total(sums[4])
    grads[773:901, :] = dot_tn(node_hidden[...], node_second[...])
    grads[901:902, :] = total(sums[5])
    grads[902:903, :] = total(sums[6])
    grads[903:904, :] = total(sums[7])
    grads[904:1024, :] = jnp.zeros((120, 128), F32)
    keep[...] = grads[pl.ds(pl.multiple_of(core * HALF, HALF), HALF), :]
    send[...] = grads[pl.ds(pl.multiple_of((1 - core) * HALF, HALF), HALF), :].astype(BF16)

    for b in range(4):
        rows = pl.ds(b * 128, 128)
        both = dot(place_send[rows, :], dxs[...]) + dot(place_recv[rows, :], dxr[...])
        local_grad[rows, :] += joined(both)


def finish_kernel(local_grad, near, far, lists, out):
    core = lax.axis_index("c")
    added = dot(place_rows(lists[pl.ds(1 - core, 1), :], 512), near[...])
    added += dot(place_rows(lists[pl.ds(core, 1), :], 512), far[...])
    out[...] = (local_grad[...] + added).astype(BF16)


def call(body, name, out_shape, operands, scratch=(), flops=1000000, smem_first=False, vmem=None):
    specs = [VMEM] * len(operands)
    if smem_first:
        specs[0] = SMEM
    return pl.pallas_call(
        body,
        name=name,
        out_shape=out_shape,
        in_specs=specs,
        out_specs=jax.tree.map(lambda _: VMEM, out_shape),
        scratch_shapes=scratch,
        compiler_params=pltpu.CompilerParams(vmem_limit_bytes=vmem),
        cost_estimate=pl.CostEstimate(flops=flops, bytes_accessed=1000000, transcendentals=0),
    )(*operands)


def shape(rows, width, kind):
    return jax.ShapeDtypeStruct((rows, width), kind)


def exchange(value, axis, size, flip):
    return lax.ppermute(value, axis, [(j, j ^ flip) for j in range(size)])


def shards(
    nodes, edges, senders, receivers, block_count, send_rows, node_cot, edge_cot,
    edge_w1, edge_b1, edge_w2, edge_b2, edge_gain, edge_shift,
    node_w1, node_b1, node_w2, node_b2, node_gain, node_shift,
):
    own_nodes = nodes[0]
    lists = send_rows[0, 0]
    line = lambda vector: vector.reshape(1, 128)
    near_pairs = [(j, j ^ 1) for j in range(64)]
    far_pairs = [(j, j + 1) for j in range(1, 63, 2)] + [(j + 1, j) for j in range(1, 63, 2)]

    near, far = call(pack_kernel, "pack", (shape(128, 128, BF16),) * 2, (own_nodes, lists))
    far = lax.ppermute(far, DOM, far_pairs)
    near = lax.ppermute(near, DOM, near_pairs)

    operands = (
        block_count, own_nodes, near, far, edges[0].reshape(512, 128), senders[0], receivers[0],
        node_cot[0], edge_cot[0].reshape(512, 128),
        edge_w1, line(edge_b1), edge_w2, line(edge_b2), line(edge_gain), line(edge_shift),
        node_w1, line(node_b1), node_w2, line(node_b2), line(node_gain), line(node_shift),
    )
    outs = (
        shape(512, 128, BF16), shape(512, 128, BF16), shape(512, 128, BF16), shape(512, 128, F32),
        shape(128, 128, BF16), shape(128, 128, BF16), shape(HALF, 128, F32), shape(HALF, 128, BF16),
    )
    scratch = [
        pltpu.VMEM(dims, kind)
        for dims, kind in (
            ((768, 128), BF16), ((512, 512), BF16), ((512, 512), BF16), ((768, 512), BF16),
            ((512, 256), BF16), ((512, 384), BF16), ((512, 128), BF16), ((512, 128), F32),
            ((512, 128), F32), ((512, 1), F32), ((512, 256), BF16), ((512, 256), BF16), ((512, 256), BF16),
            ((512, 128), BF16), ((512, 128), BF16), ((512, 256), BF16), ((512, 128), BF16),
            ((512, 128), BF16), ((512, 128), BF16), ((ROWS, 128), F32),
        )
    ]
    node_out, edge_out, grad_edge, local_grad, near_grad, far_grad, keep, send = call(
        main_kernel, "main", outs, operands, scratch, flops=2000000000, smem_first=True, vmem=24 << 20
    )

    arrived = exchange(send, "c", 2, 1)
    pair = (keep + arrived.astype(F32)).astype(BF16).reshape(32, 16, 128)
    far_back = lax.ppermute(far_grad, DOM, far_pairs)
    near_back = lax.ppermute(near_grad, DOM, near_pairs)
    tiles = lax.all_to_all(pair, PLANE, 0, 0, tiled=True)
    piece = jnp.sum(tiles.astype(F32), axis=0)
    piece = piece + exchange(piece, "y", 4, 1)
    piece = piece + exchange(piece, "y", 4, 3)
    scale = 1.0 / math.sqrt(lax.axis_size(DOM) * lax.axis_size("x") * 512)
    piece = (piece * scale).astype(BF16)
    copies = jnp.broadcast_to(piece, (32, 16, 128))
    half = lax.all_to_all(copies, PLANE, 0, 0, tiled=True).reshape(HALF, 128)
    whole = lax.all_gather(half, "c", axis=0, tiled=True)
    weight_grads = whole[:LIVE_ROWS].astype(F32).reshape(LIVE_ROWS * 128)

    grad_node = call(
        finish_kernel, "finish", shape(512, 128, BF16), (local_grad, near_back, far_back, lists)
    )
    return (
        node_out[None],
        edge_out.reshape(1, 4, 128, 128),
        grad_node[None],
        grad_edge.reshape(1, 4, 128, 128),
        weight_grads,
    )


def solution(mesh):
    finer = Mesh(mesh.devices.reshape(4, 8, 2, mesh.shape["grp"]), ("y", "z", "c", "x"))
    by_row = P("x", DOM)
    return jax.shard_map(
        shards,
        mesh=finer,
        in_specs=(by_row,) * 8 + (P(),) * 12,
        out_specs=(by_row,) * 4 + (P(),),
        check_vma=False,
    )
```

```python
import functools
import math

import jax
import jax.numpy as jnp
from jax import lax
from jax.experimental import pallas as pl
from jax.experimental.pallas import tpu as pltpu
from jax.sharding import Mesh
from jax.sharding import PartitionSpec as P

DOM = ("y", "z", "c")
COLUMN = ("z", "c")
PLANE = ("y", "x")
EPSILON = 1e-05
F32 = jnp.float32
BF16 = jnp.bfloat16
ROWS = 1024
LIVE_ROWS = 904
SMALL = 8 << 20
VMEM = pl.BlockSpec(memory_space=pltpu.VMEM)
SMEM = pl.BlockSpec(memory_space=pltpu.SMEM)
HBM = pl.BlockSpec(memory_space=pltpu.HBM)


def dot(left, right):
    return jnp.dot(left, right, preferred_element_type=F32)


def dot_nt(left, right):
    return lax.dot_general(left, right, (((1,), (1,)), ((), ())), preferred_element_type=F32)


def dot_tn(left, right):
    return lax.dot_general(left, right, (((0,), (0,)), ((), ())), preferred_element_type=F32)


def as_bf16(mask):
    return jnp.where(mask, 1.0, 0.0).astype(BF16)


def pick_rows(row, count):
    column = jnp.transpose(jnp.broadcast_to(row, (128, 128)))
    lanes = lax.broadcasted_iota(jnp.int32, (128, 128), 1)
    tiles = [as_bf16(column == lanes + 128 * j) for j in range(count // 128)]
    return jnp.concatenate(tiles, axis=1)


def place_rows(row, count):
    lines = lax.broadcasted_iota(jnp.int32, (count, 128), 0)
    return as_bf16(lines == row)


def split(value):
    high = value.astype(BF16)
    low = (value - high.astype(F32)).astype(BF16)
    return jnp.concatenate([high, low], axis=1)


def joined(value):
    return value[:, :128] + value[:, 128:]


def pack_kernel(nodes_in, lists_in, near, far, nodes, lists, arrive):
    loads = [
        pltpu.make_async_copy(nodes_in, nodes, arrive.at[0]),
        pltpu.make_async_copy(lists_in, lists, arrive.at[1]),
    ]
    for load in loads:
        load.start()
    for load in loads[::-1]:
        load.wait()
    core = lax.axis_index("c")
    near[...] = dot(pick_rows(lists[pl.ds(1 - core, 1), :], 512), nodes[...]).astype(BF16)
    far[...] = dot(pick_rows(lists[pl.ds(core, 1), :], 512), nodes[...]).astype(BF16)


def norm_forward(second):
    average = jnp.mean(second, axis=-1, keepdims=True)
    centred = second - average
    variance = jnp.mean(centred * centred, axis=-1, keepdims=True)
    inverse = lax.rsqrt(variance + EPSILON)
    return centred * inverse, inverse


def norm_backward(cot, normed, inverse, gain):
    scaled = cot * gain
    return inverse * (
        scaled
        - jnp.mean(scaled, axis=-1, keepdims=True)
        - normed * jnp.mean(scaled * normed, axis=-1, keepdims=True)
    )


def partial_sum(value):
    return jnp.sum(value.reshape(-1, 8, 128), axis=0)


def total(value):
    return jnp.sum(value, axis=0, keepdims=True)


def main_kernel(count, near, far, *refs):
    sources, refs = refs[:18], refs[18:]
    (node_out, edge_out, grad_edge, local_grad, near_grad, far_grad, send), refs = refs[:7], refs[7:]
    landed, refs = refs[:18], refs[18:]
    left, refs = refs[:3], refs[3:]
    (
        table, pick_recv, place_recv, place_send, messages, inputs, hidden, slope, normed, inverse,
        spread, dxs, dxr, first_low, second_low, node_inputs, node_hidden, node_first, node_second, grads,
        arrive, leave,
    ) = refs
    loads = [pltpu.make_async_copy(a, b, arrive.at[k]) for k, (a, b) in enumerate(zip(sources, landed))]
    stores = [
        pltpu.make_async_copy(a, b, leave.at[k])
        for k, (a, b) in enumerate(zip(left, (edge_out, node_out, grad_edge)))
    ]
    for load in loads:
        load.start()
    (
        nodes, senders, receivers, edges, ew1, eb1, ew2, eb2, egain, eshift,
        nw1, nb1, nw2, nb2, ngain, nshift, node_cot, edge_cot,
    ) = landed
    edge_left, node_left, grad_left = left
    core = lax.axis_index("c")
    live_blocks = count[0, 0]
    for load in loads[:10]:
        load.wait()
    table[pl.ds(0, 512), :] = nodes[...]
    table[pl.ds(pl.multiple_of(640 - 128 * core, 128), 128), :] = near[...]
    table[pl.ds(pl.multiple_of(512 + 128 * core, 128), 128), :] = far[...]

    for b in range(4):
        rows = pl.ds(b * 128, 128)
        live = jnp.where(b < live_blocks, 1.0, 0.0).astype(F32)
        send_row, recv_row = senders[pl.ds(b, 1), :], receivers[pl.ds(b, 1), :]
        pick = pick_rows(recv_row, 512)
        pick_recv[rows, :] = pick
        place_recv[:, rows] = place_rows(recv_row, 512)
        place_send[:, rows] = place_rows(send_row, 768)
        own = edges[rows, :]
        sender = dot(pick_rows(send_row, 768), table[...]).astype(BF16)
        receiver = dot(pick, nodes[...]).astype(BF16)
        gathered = jnp.concatenate([own, sender, receiver], axis=1)
        inputs[rows, :] = gathered
        first = dot(gathered, ew1[...]) + eb1[...]
        sigmoid = jax.nn.sigmoid(first)
        low = (first * sigmoid).astype(BF16)
        hidden[rows, :] = low
        slope[rows, :] = sigmoid * (1.0 + first * (1.0 - sigmoid))
        n, inv = norm_forward(dot(low, ew2[...]) + eb2[...])
        normed[rows, :] = n
        inverse[rows, :] = inv
        message = (n * egain[...] + eshift[...]) * live
        edge_left[rows, :] = (own.astype(F32) + message).astype(BF16)
        messages[rows, :] = split(message)

    stores[0].start()
    for load in loads[10:]:
        load.wait()
    sums = [jnp.zeros((8, 128), F32) for _ in range(8)]
    for b in range(4):
        rows = pl.ds(b * 128, 128)
        aggregate = joined(dot(place_recv[rows, :], messages[...])).astype(BF16)
        own = nodes[rows, :]
        gathered = jnp.concatenate([own, aggregate], axis=1)
        node_inputs[rows, :] = gathered
        first = dot(gathered, nw1[...]) + nb1[...]
        sigmoid = jax.nn.sigmoid(first)
        low = (first * sigmoid).astype(BF16)
        node_hidden[rows, :] = low
        n, inv = norm_forward(dot(low, nw2[...]) + nb2[...])
        node_left[rows, :] = (own.astype(F32) + (n * ngain[...] + nshift[...])).astype(BF16)
        cot = node_cot[rows, :].astype(F32)
        g2 = norm_backward(cot, n, inv, ngain[...])
        g2_low = g2.astype(BF16)
        g1 = dot_nt(g2_low, nw2[...]) * (sigmoid * (1.0 + first * (1.0 - sigmoid)))
        g1_low = g1.astype(BF16)
        node_first[rows, :] = g1_low
        node_second[rows, :] = g2_low
        back = dot_nt(g1_low, nw1[...])
        local_grad[rows, :] = cot + back[:, :128]
        spread[rows, :] = split(back[:, 128:])
        for k, piece in enumerate((g1, g2, cot * n, cot)):
            sums[4 + k] += partial_sum(piece)
    stores[1].start()

    for b in range(4):
        rows = pl.ds(b * 128, 128)
        live = jnp.where(b < live_blocks, 1.0, 0.0).astype(F32)
        edge_grad = edge_cot[rows, :].astype(F32)
        cot = live * (edge_grad + joined(dot(pick_recv[rows, :], spread[...])))
        n = normed[rows, :]
        g2 = norm_backward(cot, n, inverse[rows, :], egain[...])
        g2_low = g2.astype(BF16)
        g1 = dot_nt(g2_low, ew2[...]) * slope[rows, :]
        g1_low = g1.astype(BF16)
        first_low[rows, :] = g1_low
        second_low[rows, :] = g2_low
        back = dot_nt(g1_low, ew1[...])
        grad_left[rows, :] = (edge_grad + back[:, :128]).astype(BF16)
        dxs[rows, :] = split(back[:, 128:256])
        dxr[rows, :] = split(back[:, 256:])
        for k, piece in enumerate((g1, g2, cot * n, cot)):
            sums[k] += partial_sum(piece)
    stores[2].start()

    lower = joined(dot(place_send[512:640, :], dxs[...])).astype(BF16)
    upper = joined(dot(place_send[640:768, :], dxs[...])).astype(BF16)
    is_first = core == 0
    near_grad[...] = jnp.where(is_first, upper, lower)
    far_grad[...] = jnp.where(is_first, lower, upper)

    grads[0:384, :] = dot_tn(inputs[...], first_low[...])
    grads[384:385, :] = total(sums[0])
    grads[385:513, :] = dot_tn(hidden[...], second_low[...])
    grads[513:514, :] = total(sums[1])
    grads[514:515, :] = total(sums[2])
    grads[515:516, :] = total(sums[3])
    grads[516:772, :] = dot_tn(node_inputs[...], node_first[...])
    grads[772:773, :] = total(sums[4])
    grads[773:901, :] = dot_tn(node_hidden[...], node_second[...])
    grads[901:902, :] = total(sums[5])
    grads[902:903, :] = total(sums[6])
    grads[903:904, :] = total(sums[7])
    grads[904:1024, :] = jnp.zeros((120, 128), F32)
    send[...] = grads[...].astype(BF16)

    for b in range(4):
        rows = pl.ds(b * 128, 128)
        both = dot(place_send[rows, :], dxs[...]) + dot(place_recv[rows, :], dxr[...])
        local_grad[rows, :] += joined(both)
    for store in stores:
        store.wait()


def fold_kernel(scale, tiles, copies):
    summed = tiles[0].astype(F32)
    for k in range(1, 16):
        summed += tiles[k].astype(F32)
    low = (summed * scale).astype(BF16)
    for k in range(16):
        copies[k] = low


def finish_kernel(local_grad, near, far, lists, out):
    core = lax.axis_index("c")
    added = dot(place_rows(lists[pl.ds(1 - core, 1), :], 512), near[...])
    added += dot(place_rows(lists[pl.ds(core, 1), :], 512), far[...])
    out[...] = (local_grad[...] + added).astype(BF16)


def call(body, out_shape, operands, in_specs=None, out_specs=None, scratch=(), flops=1000000, vmem=None):
    return pl.pallas_call(
        body,
        out_shape=out_shape,
        in_specs=in_specs or [VMEM] * len(operands),
        out_specs=out_specs or jax.tree.map(lambda _: VMEM, out_shape),
        scratch_shapes=scratch,
        compiler_params=pltpu.CompilerParams(vmem_limit_bytes=vmem),
        cost_estimate=pl.CostEstimate(flops=flops, bytes_accessed=1000000, transcendentals=0),
    )(*operands)


def in_hbm(value):
    return pltpu.with_memory_space_constraint(value, pltpu.HBM)


def shape(rows, width, kind):
    return jax.ShapeDtypeStruct((rows, width), kind)


def layer(
    nodes, edges, senders, receivers, block_count, send_rows, node_cot, edge_cot,
    edge_w1, edge_b1, edge_w2, edge_b2, edge_gain, edge_shift,
    node_w1, node_b1, node_w2, node_b2, node_gain, node_shift,
):
    own_nodes = nodes[0]
    lists = send_rows[0, 0]
    line = lambda vector: vector.reshape(1, 128)
    near_pairs = [(j, j ^ 1) for j in range(64)]
    far_pairs = [(j, j + 1) for j in range(1, 63, 2)] + [(j + 1, j) for j in range(1, 63, 2)]

    near, far = call(
        pack_kernel, (shape(128, 128, BF16),) * 2, (in_hbm(own_nodes), in_hbm(lists)), [HBM] * 2,
        scratch=[
            pltpu.VMEM((512, 128), BF16), pltpu.VMEM((2, 128), jnp.int32), pltpu.SemaphoreType.DMA((2,))
        ],
        vmem=SMALL,
    )
    far = lax.ppermute(far, DOM, far_pairs)
    near = lax.ppermute(near, DOM, near_pairs)

    sources = (
        own_nodes, senders[0], receivers[0], edges[0].reshape(512, 128),
        edge_w1, line(edge_b1), edge_w2, line(edge_b2), line(edge_gain), line(edge_shift),
        node_w1, line(node_b1), node_w2, line(node_b2), line(node_gain), line(node_shift),
        node_cot[0], edge_cot[0].reshape(512, 128),
    )
    outs = (
        shape(512, 128, BF16), shape(512, 128, BF16), shape(512, 128, BF16), shape(512, 128, F32),
        shape(128, 128, BF16), shape(128, 128, BF16), shape(ROWS, 128, BF16),
    )
    scratch = [pltpu.VMEM(source.shape, source.dtype) for source in sources]
    scratch += [
        pltpu.VMEM(dims, kind)
        for dims, kind in (
            ((512, 128), BF16), ((512, 128), BF16), ((512, 128), BF16),
            ((768, 128), BF16), ((512, 512), BF16), ((512, 512), BF16), ((768, 512), BF16),
            ((512, 256), BF16), ((512, 384), BF16), ((512, 128), BF16), ((512, 128), F32),
            ((512, 128), F32), ((512, 1), F32), ((512, 256), BF16), ((512, 256), BF16), ((512, 256), BF16),
            ((512, 128), BF16), ((512, 128), BF16), ((512, 256), BF16), ((512, 128), BF16),
            ((512, 128), BF16), ((512, 128), BF16), ((ROWS, 128), F32),
        )
    ] + [pltpu.SemaphoreType.DMA((18,)), pltpu.SemaphoreType.DMA((3,))]
    node_out, edge_out, grad_edge, local_grad, near_grad, far_grad, send = call(
        main_kernel, outs, (block_count, near, far)
        + tuple(in_hbm(source) for source in sources),
        [SMEM, VMEM, VMEM] + [HBM] * 18, (HBM,) * 3 + (VMEM,) * 4, scratch, 2000000000, 24 << 20,
    )

    far_back = lax.ppermute(far_grad, DOM, far_pairs)
    near_back = lax.ppermute(near_grad, DOM, near_pairs)
    scale = 1.0 / math.sqrt(lax.axis_size(DOM) * lax.axis_size("x") * 512)
    stack = jax.ShapeDtypeStruct((16, 64, 128), BF16)
    tiles = lax.all_to_all(send.reshape(16, 64, 128), COLUMN, 0, 0, tiled=True)
    copies = call(functools.partial(fold_kernel, 1.0), stack, (tiles,), vmem=SMALL)
    tiles = lax.all_to_all(copies, PLANE, 0, 0, tiled=True)
    copies = call(functools.partial(fold_kernel, scale), stack, (tiles,), vmem=SMALL)
    whole = lax.all_to_all(copies, COLUMN, 0, 0, tiled=True).reshape(ROWS, 128)
    weight_grads = whole[:LIVE_ROWS].astype(F32).reshape(LIVE_ROWS * 128)

    grad_node = call(finish_kernel, shape(512, 128, BF16), (local_grad, near_back, far_back, lists), vmem=SMALL)
    return (
        node_out[None],
        edge_out.reshape(1, 4, 128, 128),
        grad_node[None],
        grad_edge.reshape(1, 4, 128, 128),
        weight_grads,
    )


def solution(mesh):
    finer = Mesh(mesh.devices.reshape(4, 8, 2, mesh.shape["grp"]), ("y", "z", "c", "x"))
    by_row = P("x", DOM)
    return jax.shard_map(
        layer,
        mesh=finer,
        in_specs=(by_row,) * 8 + (P(),) * 12,
        out_specs=(by_row,) * 4 + (P(),),
        check_vma=False,
    )
```

```python
import functools
import math

import jax
import jax.numpy as jnp
from jax import lax
from jax.experimental import pallas as pl
from jax.experimental.pallas import tpu as pltpu
from jax.sharding import Mesh
from jax.sharding import PartitionSpec as P

DOM = ("y", "z", "c")
PLANE = ("c", "y", "x")
COLUMN = ("z",)
EPSILON = 1e-05
F32 = jnp.float32
BF16 = jnp.bfloat16
ROWS = 1024
LIVE_ROWS = 904
SMALL = 8 << 20
VMEM = pl.BlockSpec(memory_space=pltpu.VMEM)
SMEM = pl.BlockSpec(memory_space=pltpu.SMEM)
HBM = pl.BlockSpec(memory_space=pltpu.HBM)


def dot(left, right):
    return jnp.dot(left, right, preferred_element_type=F32)


def dot_nt(left, right):
    return lax.dot_general(left, right, (((1,), (1,)), ((), ())), preferred_element_type=F32)


def dot_tn(left, right):
    return lax.dot_general(left, right, (((0,), (0,)), ((), ())), preferred_element_type=F32)


def as_bf16(mask):
    return jnp.where(mask, 1.0, 0.0).astype(BF16)


def pick_rows(row, count):
    column = jnp.transpose(jnp.broadcast_to(row, (128, 128)))
    lanes = lax.broadcasted_iota(jnp.int32, (128, 128), 1)
    tiles = [as_bf16(column == lanes + 128 * j) for j in range(count // 128)]
    return jnp.concatenate(tiles, axis=1)


def place_rows(row, count):
    lines = lax.broadcasted_iota(jnp.int32, (count, 128), 0)
    return as_bf16(lines == row)


def split(value):
    high = value.astype(BF16)
    low = (value - high.astype(F32)).astype(BF16)
    return jnp.concatenate([high, low], axis=1)


def joined(value):
    return value[:, :128] + value[:, 128:]


def pack_kernel(nodes_in, lists_in, near, far, nodes, lists, arrive):
    loads = [
        pltpu.make_async_copy(nodes_in, nodes, arrive.at[0]),
        pltpu.make_async_copy(lists_in, lists, arrive.at[1]),
    ]
    for load in loads:
        load.start()
    for load in loads[::-1]:
        load.wait()
    core = lax.axis_index("c")
    near[...] = dot(pick_rows(lists[pl.ds(1 - core, 1), :], 512), nodes[...]).astype(BF16)
    far[...] = dot(pick_rows(lists[pl.ds(core, 1), :], 512), nodes[...]).astype(BF16)


def norm_forward(second):
    average = jnp.mean(second, axis=-1, keepdims=True)
    centred = second - average
    variance = jnp.mean(centred * centred, axis=-1, keepdims=True)
    inverse = lax.rsqrt(variance + EPSILON)
    return centred * inverse, inverse


def norm_backward(cot, normed, inverse, gain):
    scaled = cot * gain
    return inverse * (
        scaled
        - jnp.mean(scaled, axis=-1, keepdims=True)
        - normed * jnp.mean(scaled * normed, axis=-1, keepdims=True)
    )


def partial_sum(value):
    return jnp.sum(value.reshape(-1, 8, 128), axis=0)


def total(value):
    return jnp.sum(value, axis=0, keepdims=True)


def main_kernel(count, near, far, *refs):
    sources, refs = refs[:18], refs[18:]
    (node_out, edge_out, grad_edge, local_grad, near_grad, far_grad, send), refs = refs[:7], refs[7:]
    landed, refs = refs[:18], refs[18:]
    left, refs = refs[:3], refs[3:]
    (
        table, pick_recv, place_recv, place_send, messages, inputs, hidden, slope, normed, inverse,
        spread, dxs, dxr, first_low, second_low, node_inputs, node_hidden, node_first, node_second, grads,
        arrive, leave,
    ) = refs
    loads = [pltpu.make_async_copy(a, b, arrive.at[k]) for k, (a, b) in enumerate(zip(sources, landed))]
    stores = [
        pltpu.make_async_copy(a, b, leave.at[k])
        for k, (a, b) in enumerate(zip(left, (edge_out, node_out, grad_edge)))
    ]
    for load in loads:
        load.start()
    (
        nodes, senders, receivers, edges, ew1, eb1, ew2, eb2, egain, eshift,
        nw1, nb1, nw2, nb2, ngain, nshift, node_cot, edge_cot,
    ) = landed
    edge_left, node_left, grad_left = left
    core = lax.axis_index("c")
    live_blocks = count[0, 0]
    for load in loads[:10]:
        load.wait()
    table[pl.ds(0, 512), :] = nodes[...]
    table[pl.ds(pl.multiple_of(640 - 128 * core, 128), 128), :] = near[...]
    table[pl.ds(pl.multiple_of(512 + 128 * core, 128), 128), :] = far[...]

    for b in range(4):
        rows = pl.ds(b * 128, 128)
        live = jnp.where(b < live_blocks, 1.0, 0.0).astype(F32)
        send_row, recv_row = senders[pl.ds(b, 1), :], receivers[pl.ds(b, 1), :]
        pick = pick_rows(recv_row, 512)
        pick_recv[rows, :] = pick
        place_recv[:, rows] = place_rows(recv_row, 512)
        place_send[:, rows] = place_rows(send_row, 768)
        own = edges[rows, :]
        sender = dot(pick_rows(send_row, 768), table[...]).astype(BF16)
        receiver = dot(pick, nodes[...]).astype(BF16)
        gathered = jnp.concatenate([own, sender, receiver], axis=1)
        inputs[rows, :] = gathered
        first = dot(gathered, ew1[...]) + eb1[...]
        sigmoid = jax.nn.sigmoid(first)
        low = (first * sigmoid).astype(BF16)
        hidden[rows, :] = low
        slope[rows, :] = sigmoid * (1.0 + first * (1.0 - sigmoid))
        n, inv = norm_forward(dot(low, ew2[...]) + eb2[...])
        normed[rows, :] = n
        inverse[rows, :] = inv
        message = (n * egain[...] + eshift[...]) * live
        edge_left[rows, :] = (own.astype(F32) + message).astype(BF16)
        messages[rows, :] = split(message)

    stores[0].start()
    for load in loads[10:]:
        load.wait()
    sums = [jnp.zeros((8, 128), F32) for _ in range(8)]
    for b in range(4):
        rows = pl.ds(b * 128, 128)
        aggregate = joined(dot(place_recv[rows, :], messages[...])).astype(BF16)
        own = nodes[rows, :]
        gathered = jnp.concatenate([own, aggregate], axis=1)
        node_inputs[rows, :] = gathered
        first = dot(gathered, nw1[...]) + nb1[...]
        sigmoid = jax.nn.sigmoid(first)
        low = (first * sigmoid).astype(BF16)
        node_hidden[rows, :] = low
        n, inv = norm_forward(dot(low, nw2[...]) + nb2[...])
        node_left[rows, :] = (own.astype(F32) + (n * ngain[...] + nshift[...])).astype(BF16)
        cot = node_cot[rows, :].astype(F32)
        g2 = norm_backward(cot, n, inv, ngain[...])
        g2_low = g2.astype(BF16)
        g1 = dot_nt(g2_low, nw2[...]) * (sigmoid * (1.0 + first * (1.0 - sigmoid)))
        g1_low = g1.astype(BF16)
        node_first[rows, :] = g1_low
        node_second[rows, :] = g2_low
        back = dot_nt(g1_low, nw1[...])
        local_grad[rows, :] = cot + back[:, :128]
        spread[rows, :] = split(back[:, 128:])
        for k, piece in enumerate((g1, g2, cot * n, cot)):
            sums[4 + k] += partial_sum(piece)
    stores[1].start()

    for b in range(4):
        rows = pl.ds(b * 128, 128)
        live = jnp.where(b < live_blocks, 1.0, 0.0).astype(F32)
        edge_grad = edge_cot[rows, :].astype(F32)
        cot = live * (edge_grad + joined(dot(pick_recv[rows, :], spread[...])))
        n = normed[rows, :]
        g2 = norm_backward(cot, n, inverse[rows, :], egain[...])
        g2_low = g2.astype(BF16)
        g1 = dot_nt(g2_low, ew2[...]) * slope[rows, :]
        g1_low = g1.astype(BF16)
        first_low[rows, :] = g1_low
        second_low[rows, :] = g2_low
        back = dot_nt(g1_low, ew1[...])
        grad_left[rows, :] = (edge_grad + back[:, :128]).astype(BF16)
        dxs[rows, :] = split(back[:, 128:256])
        dxr[rows, :] = split(back[:, 256:])
        for k, piece in enumerate((g1, g2, cot * n, cot)):
            sums[k] += partial_sum(piece)
    stores[2].start()

    lower = joined(dot(place_send[512:640, :], dxs[...])).astype(BF16)
    upper = joined(dot(place_send[640:768, :], dxs[...])).astype(BF16)
    is_first = core == 0
    near_grad[...] = jnp.where(is_first, upper, lower)
    far_grad[...] = jnp.where(is_first, lower, upper)

    grads[0:384, :] = dot_tn(inputs[...], first_low[...])
    grads[384:385, :] = total(sums[0])
    grads[385:513, :] = dot_tn(hidden[...], second_low[...])
    grads[513:514, :] = total(sums[1])
    grads[514:515, :] = total(sums[2])
    grads[515:516, :] = total(sums[3])
    grads[516:772, :] = dot_tn(node_inputs[...], node_first[...])
    grads[772:773, :] = total(sums[4])
    grads[773:901, :] = dot_tn(node_hidden[...], node_second[...])
    grads[901:902, :] = total(sums[5])
    grads[902:903, :] = total(sums[6])
    grads[903:904, :] = total(sums[7])
    grads[904:1024, :] = jnp.zeros((120, 128), F32)
    send[...] = grads[...].astype(BF16)

    for b in range(4):
        rows = pl.ds(b * 128, 128)
        both = dot(place_send[rows, :], dxs[...]) + dot(place_recv[rows, :], dxr[...])
        local_grad[rows, :] += joined(both)
    for store in stores:
        store.wait()


def fold_kernel(scale, tiles, copies):
    summed = tiles[0].astype(F32)
    for k in range(1, tiles.shape[0]):
        summed += tiles[k].astype(F32)
    low = (summed * scale).astype(BF16)
    for k in range(copies.shape[0]):
        copies[k] = low


def finish_kernel(local_grad, near, far, lists, out):
    core = lax.axis_index("c")
    added = dot(place_rows(lists[pl.ds(1 - core, 1), :], 512), near[...])
    added += dot(place_rows(lists[pl.ds(core, 1), :], 512), far[...])
    out[...] = (local_grad[...] + added).astype(BF16)


def call(body, name, out_shape, operands, in_specs=None, out_specs=None, scratch=(), flops=1000000, vmem=None):
    return pl.pallas_call(
        body,
        name=name,
        out_shape=out_shape,
        in_specs=in_specs or [VMEM] * len(operands),
        out_specs=out_specs or jax.tree.map(lambda _: VMEM, out_shape),
        scratch_shapes=scratch,
        compiler_params=pltpu.CompilerParams(vmem_limit_bytes=vmem),
        cost_estimate=pl.CostEstimate(flops=flops, bytes_accessed=1000000, transcendentals=0),
    )(*operands)


def fold(tiles, count, scale, name):
    out = jax.ShapeDtypeStruct((count, *tiles.shape[1:]), BF16)
    return call(functools.partial(fold_kernel, scale), name, out, (tiles,), vmem=SMALL)


def in_hbm(value):
    return pltpu.with_memory_space_constraint(value, pltpu.HBM)


def shape(rows, width, kind):
    return jax.ShapeDtypeStruct((rows, width), kind)


def shards(
    nodes, edges, senders, receivers, block_count, send_rows, node_cot, edge_cot,
    edge_w1, edge_b1, edge_w2, edge_b2, edge_gain, edge_shift,
    node_w1, node_b1, node_w2, node_b2, node_gain, node_shift,
):
    own_nodes = nodes[0]
    lists = send_rows[0, 0]
    line = lambda vector: vector.reshape(1, 128)
    near_pairs = [(j, j ^ 1) for j in range(64)]
    far_pairs = [(j, j + 1) for j in range(1, 63, 2)] + [(j + 1, j) for j in range(1, 63, 2)]

    near, far = call(
        pack_kernel, "pack", (shape(128, 128, BF16),) * 2, (in_hbm(own_nodes), in_hbm(lists)), [HBM] * 2,
        scratch=[
            pltpu.VMEM((512, 128), BF16), pltpu.VMEM((2, 128), jnp.int32), pltpu.SemaphoreType.DMA((2,))
        ],
        vmem=SMALL,
    )
    far = lax.ppermute(far, DOM, far_pairs)
    near = lax.ppermute(near, DOM, near_pairs)

    sources = (
        own_nodes, senders[0], receivers[0], edges[0].reshape(512, 128),
        edge_w1, line(edge_b1), edge_w2, line(edge_b2), line(edge_gain), line(edge_shift),
        node_w1, line(node_b1), node_w2, line(node_b2), line(node_gain), line(node_shift),
        node_cot[0], edge_cot[0].reshape(512, 128),
    )
    outs = (
        shape(512, 128, BF16), shape(512, 128, BF16), shape(512, 128, BF16), shape(512, 128, F32),
        shape(128, 128, BF16), shape(128, 128, BF16), shape(ROWS, 128, BF16),
    )
    scratch = [pltpu.VMEM(source.shape, source.dtype) for source in sources]
    scratch += [
        pltpu.VMEM(dims, kind)
        for dims, kind in (
            ((512, 128), BF16), ((512, 128), BF16), ((512, 128), BF16),
            ((768, 128), BF16), ((512, 512), BF16), ((512, 512), BF16), ((768, 512), BF16),
            ((512, 256), BF16), ((512, 384), BF16), ((512, 128), BF16), ((512, 128), F32),
            ((512, 128), F32), ((512, 1), F32), ((512, 256), BF16), ((512, 256), BF16), ((512, 256), BF16),
            ((512, 128), BF16), ((512, 128), BF16), ((512, 256), BF16), ((512, 128), BF16),
            ((512, 128), BF16), ((512, 128), BF16), ((ROWS, 128), F32),
        )
    ] + [pltpu.SemaphoreType.DMA((18,)), pltpu.SemaphoreType.DMA((3,))]
    node_out, edge_out, grad_edge, local_grad, near_grad, far_grad, send = call(
        main_kernel, "main", outs, (block_count, near, far)
        + tuple(in_hbm(source) for source in sources),
        [SMEM, VMEM, VMEM] + [HBM] * 18, (HBM,) * 3 + (VMEM,) * 4, scratch, 2000000000, 24 << 20,
    )

    far_back = lax.ppermute(far_grad, DOM, far_pairs)
    near_back = lax.ppermute(near_grad, DOM, near_pairs)
    scale = 1.0 / math.sqrt(lax.axis_size(DOM) * lax.axis_size("x") * 512)
    planes, columns = lax.axis_size(PLANE), lax.axis_size(COLUMN)
    rows = ROWS // planes
    tiles = lax.all_to_all(send.reshape(planes, rows, 128), PLANE, 0, 0, tiled=True)
    copies = fold(tiles, columns, 1.0, "fold_plane")
    tiles = lax.all_to_all(copies, COLUMN, 0, 0, tiled=True)
    copies = fold(tiles, planes, scale, "fold_column")
    whole = lax.all_to_all(copies, PLANE, 0, 0, tiled=True).reshape(ROWS, 128)
    weight_grads = whole[:LIVE_ROWS].astype(F32).reshape(LIVE_ROWS * 128)

    grad_node = call(
        finish_kernel, "finish", shape(512, 128, BF16), (local_grad, near_back, far_back, lists), vmem=SMALL
    )
    return (
        node_out[None],
        edge_out.reshape(1, 4, 128, 128),
        grad_node[None],
        grad_edge.reshape(1, 4, 128, 128),
        weight_grads,
    )


def solution(mesh):
    finer = Mesh(mesh.devices.reshape(4, 8, 2, mesh.shape["grp"]), ("y", "z", "c", "x"))
    by_row = P("x", DOM)
    return jax.shard_map(
        shards,
        mesh=finer,
        in_specs=(by_row,) * 8 + (P(),) * 12,
        out_specs=(by_row,) * 4 + (P(),),
        check_vma=False,
    )
```

```python
import functools
import math

import jax
import jax.numpy as jnp
from jax import lax
from jax.experimental import pallas as pl
from jax.experimental.pallas import tpu as pltpu
from jax.sharding import Mesh
from jax.sharding import PartitionSpec as P

DOM = ("y", "z", "c")
PLANE = ("c", "y", "x")
COLUMN = ("z",)
EPSILON = 1e-05
F32 = jnp.float32
BF16 = jnp.bfloat16
ROWS = 1024
LIVE_ROWS = 904
SMALL = 8 << 20
VMEM = pl.BlockSpec(memory_space=pltpu.VMEM)
SMEM = pl.BlockSpec(memory_space=pltpu.SMEM)
HBM = pl.BlockSpec(memory_space=pltpu.HBM)


def dot(left, right):
    return jnp.dot(left, right, preferred_element_type=F32)


def dot_nt(left, right):
    return lax.dot_general(left, right, (((1,), (1,)), ((), ())), preferred_element_type=F32)


def dot_tn(left, right):
    return lax.dot_general(left, right, (((0,), (0,)), ((), ())), preferred_element_type=F32)


def as_bf16(mask):
    return jnp.where(mask, 1.0, 0.0).astype(BF16)


def pick_rows(row, count):
    column = jnp.transpose(jnp.broadcast_to(row, (128, 128)))
    lanes = lax.broadcasted_iota(jnp.int32, (128, 128), 1)
    tiles = [as_bf16(column == lanes + 128 * j) for j in range(count // 128)]
    return jnp.concatenate(tiles, axis=1)


def place_rows(row, count):
    lines = lax.broadcasted_iota(jnp.int32, (count, 128), 0)
    return as_bf16(lines == row)


def split(value):
    high = value.astype(BF16)
    low = (value - high.astype(F32)).astype(BF16)
    return jnp.concatenate([high, low], axis=1)


def joined(value):
    return value[:, :128] + value[:, 128:]


def is_live(blocks):
    line = lax.broadcasted_iota(jnp.int32, (512, 128), 0)
    return jnp.where(line < blocks * 128, 1.0, 0.0).astype(F32)


def pack_kernel(nodes_in, lists_in, near, far, nodes, lists, arrive):
    loads = [
        pltpu.make_async_copy(nodes_in, nodes, arrive.at[0]),
        pltpu.make_async_copy(lists_in, lists, arrive.at[1]),
    ]
    for load in loads:
        load.start()
    for load in loads[::-1]:
        load.wait()
    core = lax.axis_index("c")
    near[...] = dot(pick_rows(lists[pl.ds(1 - core, 1), :], 512), nodes[...]).astype(BF16)
    far[...] = dot(pick_rows(lists[pl.ds(core, 1), :], 512), nodes[...]).astype(BF16)


def norm_forward(second):
    average = jnp.mean(second, axis=-1, keepdims=True)
    centred = second - average
    variance = jnp.mean(centred * centred, axis=-1, keepdims=True)
    inverse = lax.rsqrt(variance + EPSILON)
    return centred * inverse, inverse


def norm_backward(cot, normed, inverse, gain):
    scaled = cot * gain
    return inverse * (
        scaled
        - jnp.mean(scaled, axis=-1, keepdims=True)
        - normed * jnp.mean(scaled * normed, axis=-1, keepdims=True)
    )


def partial_sum(value):
    return jnp.sum(value.reshape(-1, 8, 128), axis=0)


def total(value):
    return jnp.sum(value, axis=0, keepdims=True)


def main_kernel(count, near, far, *refs):
    sources, refs = refs[:18], refs[18:]
    (node_out, edge_out, grad_edge, local_grad, near_grad, far_grad, send), refs = refs[:7], refs[7:]
    landed, refs = refs[:18], refs[18:]
    left, refs = refs[:3], refs[3:]
    (
        table, pick_recv, place_recv, place_send, messages, inputs, hidden, slope, normed, inverse,
        spread, dxs, dxr, first_low, second_low, node_inputs, node_hidden, node_first, node_second, grads,
        arrive, leave,
    ) = refs
    loads = [pltpu.make_async_copy(a, b, arrive.at[k]) for k, (a, b) in enumerate(zip(sources, landed))]
    stores = [
        pltpu.make_async_copy(a, b, leave.at[k])
        for k, (a, b) in enumerate(zip(left, (edge_out, node_out, grad_edge)))
    ]
    for load in loads:
        load.start()
    (
        senders, receivers, nodes, edges, ew1, eb1, ew2, eb2, egain, eshift,
        nw1, nb1, nw2, nb2, ngain, nshift, node_cot, edge_cot,
    ) = landed
    edge_left, node_left, grad_left = left
    core = lax.axis_index("c")
    live_blocks = count[0, 0]
    table[pl.ds(pl.multiple_of(640 - 128 * core, 128), 128), :] = near[...]
    table[pl.ds(pl.multiple_of(512 + 128 * core, 128), 128), :] = far[...]
    for load in loads[:10]:
        load.wait()
    for b in range(4):
        rows = pl.ds(b * 128, 128)
        send_row, recv_row = senders[pl.ds(b, 1), :], receivers[pl.ds(b, 1), :]
        pick_recv[rows, :] = pick_rows(recv_row, 512)
        place_recv[:, rows] = place_rows(recv_row, 512)
        place_send[:, rows] = place_rows(send_row, 768)

    table[pl.ds(0, 512), :] = nodes[...]
    live = is_live(live_blocks)
    own = edges[...]
    picks = jnp.concatenate([pick_rows(senders[pl.ds(k, 1), :], 768) for k in range(4)], axis=0)
    sender = dot(picks, table[...]).astype(BF16)
    receiver = dot(pick_recv[...], nodes[...]).astype(BF16)
    gathered = jnp.concatenate([own, sender, receiver], axis=1)
    inputs[...] = gathered
    first = dot(gathered, ew1[...]) + eb1[...]
    sigmoid = jax.nn.sigmoid(first)
    low = (first * sigmoid).astype(BF16)
    hidden[...] = low
    slope[...] = sigmoid * (1.0 + first * (1.0 - sigmoid))
    n, inv = norm_forward(dot(low, ew2[...]) + eb2[...])
    normed[...] = n
    inverse[...] = inv
    message = (n * egain[...] + eshift[...]) * live
    edge_left[...] = (own.astype(F32) + message).astype(BF16)
    messages[...] = split(message)

    stores[0].start()
    for load in loads[10:]:
        load.wait()
    sums = [jnp.zeros((8, 128), F32) for _ in range(8)]
    aggregate = joined(dot(place_recv[...], messages[...])).astype(BF16)
    own = nodes[...]
    gathered = jnp.concatenate([own, aggregate], axis=1)
    node_inputs[...] = gathered
    first = dot(gathered, nw1[...]) + nb1[...]
    sigmoid = jax.nn.sigmoid(first)
    low = (first * sigmoid).astype(BF16)
    node_hidden[...] = low
    n, inv = norm_forward(dot(low, nw2[...]) + nb2[...])
    node_left[...] = (own.astype(F32) + (n * ngain[...] + nshift[...])).astype(BF16)
    cot = node_cot[...].astype(F32)
    g2 = norm_backward(cot, n, inv, ngain[...])
    g2_low = g2.astype(BF16)
    g1 = dot_nt(g2_low, nw2[...]) * (sigmoid * (1.0 + first * (1.0 - sigmoid)))
    g1_low = g1.astype(BF16)
    node_first[...] = g1_low
    node_second[...] = g2_low
    back = dot_nt(g1_low, nw1[...])
    local_grad[...] = cot + back[:, :128]
    spread[...] = split(back[:, 128:])
    for k, piece in enumerate((g1, g2, cot * n, cot)):
        sums[4 + k] += partial_sum(piece)
    stores[1].start()

    live = is_live(live_blocks)
    edge_grad = edge_cot[...].astype(F32)
    cot = live * (edge_grad + joined(dot(pick_recv[...], spread[...])))
    n = normed[...]
    g2 = norm_backward(cot, n, inverse[...], egain[...])
    g2_low = g2.astype(BF16)
    g1 = dot_nt(g2_low, ew2[...]) * slope[...]
    g1_low = g1.astype(BF16)
    first_low[...] = g1_low
    second_low[...] = g2_low
    back = dot_nt(g1_low, ew1[...])
    grad_left[...] = (edge_grad + back[:, :128]).astype(BF16)
    dxs[...] = split(back[:, 128:256])
    dxr[...] = split(back[:, 256:])
    for k, piece in enumerate((g1, g2, cot * n, cot)):
        sums[k] += partial_sum(piece)
    stores[2].start()

    lower = joined(dot(place_send[512:640, :], dxs[...])).astype(BF16)
    upper = joined(dot(place_send[640:768, :], dxs[...])).astype(BF16)
    is_first = core == 0
    near_grad[...] = jnp.where(is_first, upper, lower)
    far_grad[...] = jnp.where(is_first, lower, upper)

    grads[0:384, :] = dot_tn(inputs[...], first_low[...])
    grads[384:385, :] = total(sums[0])
    grads[385:513, :] = dot_tn(hidden[...], second_low[...])
    grads[513:514, :] = total(sums[1])
    grads[514:515, :] = total(sums[2])
    grads[515:516, :] = total(sums[3])
    grads[516:772, :] = dot_tn(node_inputs[...], node_first[...])
    grads[772:773, :] = total(sums[4])
    grads[773:901, :] = dot_tn(node_hidden[...], node_second[...])
    grads[901:902, :] = total(sums[5])
    grads[902:903, :] = total(sums[6])
    grads[903:904, :] = total(sums[7])
    grads[904:1024, :] = jnp.zeros((120, 128), F32)
    send[...] = grads[...].astype(BF16)

    for b in range(4):
        rows = pl.ds(b * 128, 128)
        both = dot(place_send[rows, :], dxs[...]) + dot(place_recv[rows, :], dxr[...])
        local_grad[rows, :] += joined(both)
    for store in stores:
        store.wait()


def fold_kernel(scale, tiles, copies):
    summed = tiles[0].astype(F32)
    for k in range(1, tiles.shape[0]):
        summed += tiles[k].astype(F32)
    low = (summed * scale).astype(BF16)
    for k in range(copies.shape[0]):
        copies[k] = low


def finish_kernel(local_grad, near, far, lists, out):
    core = lax.axis_index("c")
    added = dot(place_rows(lists[pl.ds(1 - core, 1), :], 512), near[...])
    added += dot(place_rows(lists[pl.ds(core, 1), :], 512), far[...])
    out[...] = (local_grad[...] + added).astype(BF16)


def call(body, out_shape, operands, in_specs=None, out_specs=None, scratch=(), flops=1000000, vmem=None):
    return pl.pallas_call(
        body,
        out_shape=out_shape,
        in_specs=in_specs or [VMEM] * len(operands),
        out_specs=out_specs or jax.tree.map(lambda _: VMEM, out_shape),
        scratch_shapes=scratch,
        compiler_params=pltpu.CompilerParams(vmem_limit_bytes=vmem),
        cost_estimate=pl.CostEstimate(flops=flops, bytes_accessed=1000000, transcendentals=0),
    )(*operands)


def fold(tiles, count, scale):
    out = jax.ShapeDtypeStruct((count, *tiles.shape[1:]), BF16)
    return call(functools.partial(fold_kernel, scale), out, (tiles,), vmem=SMALL)


def in_hbm(value):
    return pltpu.with_memory_space_constraint(value, pltpu.HBM)


def shape(rows, width, kind):
    return jax.ShapeDtypeStruct((rows, width), kind)


def layer(
    nodes, edges, senders, receivers, block_count, send_rows, node_cot, edge_cot,
    edge_w1, edge_b1, edge_w2, edge_b2, edge_gain, edge_shift,
    node_w1, node_b1, node_w2, node_b2, node_gain, node_shift,
):
    own_nodes = nodes[0]
    lists = send_rows[0, 0]
    line = lambda vector: vector.reshape(1, 128)
    near_pairs = [(j, j ^ 1) for j in range(64)]
    far_pairs = [(j, j + 1) for j in range(1, 63, 2)] + [(j + 1, j) for j in range(1, 63, 2)]

    near, far = call(
        pack_kernel, (shape(128, 128, BF16),) * 2, (in_hbm(own_nodes), in_hbm(lists)), [HBM] * 2,
        scratch=[
            pltpu.VMEM((512, 128), BF16), pltpu.VMEM((2, 128), jnp.int32), pltpu.SemaphoreType.DMA((2,))
        ],
        vmem=SMALL,
    )
    far = lax.ppermute(far, DOM, far_pairs)
    near = lax.ppermute(near, DOM, near_pairs)

    sources = (
        senders[0], receivers[0], own_nodes, edges[0].reshape(512, 128),
        edge_w1, line(edge_b1), edge_w2, line(edge_b2), line(edge_gain), line(edge_shift),
        node_w1, line(node_b1), node_w2, line(node_b2), line(node_gain), line(node_shift),
        node_cot[0], edge_cot[0].reshape(512, 128),
    )
    outs = (
        shape(512, 128, BF16), shape(512, 128, BF16), shape(512, 128, BF16), shape(512, 128, F32),
        shape(128, 128, BF16), shape(128, 128, BF16), shape(ROWS, 128, BF16),
    )
    scratch = [pltpu.VMEM(source.shape, source.dtype) for source in sources]
    scratch += [
        pltpu.VMEM(dims, kind)
        for dims, kind in (
            ((512, 128), BF16), ((512, 128), BF16), ((512, 128), BF16),
            ((768, 128), BF16), ((512, 512), BF16), ((512, 512), BF16), ((768, 512), BF16),
            ((512, 256), BF16), ((512, 384), BF16), ((512, 128), BF16), ((512, 128), F32),
            ((512, 128), F32), ((512, 1), F32), ((512, 256), BF16), ((512, 256), BF16), ((512, 256), BF16),
            ((512, 128), BF16), ((512, 128), BF16), ((512, 256), BF16), ((512, 128), BF16),
            ((512, 128), BF16), ((512, 128), BF16), ((ROWS, 128), F32),
        )
    ] + [pltpu.SemaphoreType.DMA((18,)), pltpu.SemaphoreType.DMA((3,))]
    node_out, edge_out, grad_edge, local_grad, near_grad, far_grad, send = call(
        main_kernel, outs, (block_count, near, far)
        + tuple(in_hbm(source) for source in sources),
        [SMEM, VMEM, VMEM] + [HBM] * 18, (HBM,) * 3 + (VMEM,) * 4, scratch, 2000000000, 24 << 20,
    )

    far_back = lax.ppermute(far_grad, DOM, far_pairs)
    near_back = lax.ppermute(near_grad, DOM, near_pairs)
    scale = 1.0 / math.sqrt(lax.axis_size(DOM) * lax.axis_size("x") * 512)
    planes, columns = lax.axis_size(PLANE), lax.axis_size(COLUMN)
    rows = ROWS // planes
    tiles = lax.all_to_all(send.reshape(planes, rows, 128), PLANE, 0, 0, tiled=True)
    copies = fold(tiles, columns, 1.0)
    tiles = lax.all_to_all(copies, COLUMN, 0, 0, tiled=True)
    copies = fold(tiles, planes, scale)
    whole = lax.all_to_all(copies, PLANE, 0, 0, tiled=True).reshape(ROWS, 128)
    weight_grads = whole[:LIVE_ROWS].astype(F32).reshape(LIVE_ROWS * 128)

    grad_node = call(finish_kernel, shape(512, 128, BF16), (local_grad, near_back, far_back, lists), vmem=SMALL)
    return (
        node_out[None],
        edge_out.reshape(1, 4, 128, 128),
        grad_node[None],
        grad_edge.reshape(1, 4, 128, 128),
        weight_grads,
    )


def solution(mesh):
    finer = Mesh(mesh.devices.reshape(4, 8, 2, mesh.shape["grp"]), ("y", "z", "c", "x"))
    by_row = P("x", DOM)
    return jax.shard_map(
        layer,
        mesh=finer,
        in_specs=(by_row,) * 8 + (P(),) * 12,
        out_specs=(by_row,) * 4 + (P(),),
        check_vma=False,
    )
```

```python
import functools
import math

import jax
import jax.numpy as jnp
from jax import lax
from jax.experimental import pallas as pl
from jax.experimental.pallas import tpu as pltpu
from jax.sharding import Mesh
from jax.sharding import PartitionSpec as P

DOM = ("y", "z", "c")
PLANE = ("y", "x")
COLUMN = ("z",)
EPSILON = 1e-05
F32 = jnp.float32
BF16 = jnp.bfloat16
ROWS = 1024
LIVE_ROWS = 904
HALF = 512
SMALL = 8 << 20
VMEM = pl.BlockSpec(memory_space=pltpu.VMEM)
SMEM = pl.BlockSpec(memory_space=pltpu.SMEM)
HBM = pl.BlockSpec(memory_space=pltpu.HBM)


def dot(left, right):
    return jnp.dot(left, right, preferred_element_type=F32)


def dot_nt(left, right):
    return lax.dot_general(left, right, (((1,), (1,)), ((), ())), preferred_element_type=F32)


def dot_tn(left, right):
    return lax.dot_general(left, right, (((0,), (0,)), ((), ())), preferred_element_type=F32)


def as_bf16(mask):
    return jnp.where(mask, 1.0, 0.0).astype(BF16)


def pick_rows(row, count):
    column = jnp.transpose(jnp.broadcast_to(row, (128, 128)))
    lanes = lax.broadcasted_iota(jnp.int32, (128, 128), 1)
    tiles = [as_bf16(column == lanes + 128 * j) for j in range(count // 128)]
    return jnp.concatenate(tiles, axis=1)


def place_rows(row, count):
    lines = lax.broadcasted_iota(jnp.int32, (count, 128), 0)
    return as_bf16(lines == row)


def split(value):
    high = value.astype(BF16)
    low = (value - high.astype(F32)).astype(BF16)
    return jnp.concatenate([high, low], axis=1)


def joined(value):
    return value[:, :128] + value[:, 128:]


def pack_kernel(nodes_in, lists_in, near, far, nodes, lists, arrive):
    loads = [
        pltpu.make_async_copy(nodes_in, nodes, arrive.at[0]),
        pltpu.make_async_copy(lists_in, lists, arrive.at[1]),
    ]
    for load in loads:
        load.start()
    for load in loads[::-1]:
        load.wait()
    core = lax.axis_index("c")
    near[...] = dot(pick_rows(lists[pl.ds(1 - core, 1), :], 512), nodes[...]).astype(BF16)
    far[...] = dot(pick_rows(lists[pl.ds(core, 1), :], 512), nodes[...]).astype(BF16)


def norm_forward(second):
    average = jnp.mean(second, axis=-1, keepdims=True)
    centred = second - average
    variance = jnp.mean(centred * centred, axis=-1, keepdims=True)
    inverse = lax.rsqrt(variance + EPSILON)
    return centred * inverse, inverse


def norm_backward(cot, normed, inverse, gain):
    scaled = cot * gain
    return inverse * (
        scaled
        - jnp.mean(scaled, axis=-1, keepdims=True)
        - normed * jnp.mean(scaled * normed, axis=-1, keepdims=True)
    )


def partial_sum(value):
    return jnp.sum(value.reshape(-1, 8, 128), axis=0)


def total(value):
    return jnp.sum(value, axis=0, keepdims=True)


def prepare_kernel(*refs):
    sources, landed, (receiver, partial, live, pick_send, pick_recv, place_recv, place_send), (arrive,) = (
        refs[:19], refs[19:38], refs[38:45], refs[45:],
    )
    loads = [pltpu.make_async_copy(a, b, arrive.at[k]) for k, (a, b) in enumerate(zip(sources, landed))]
    for load in loads:
        load.start()
    count, senders, receivers, nodes, edges, ew1, eb1 = landed[:7]
    for load in loads[:3]:
        load.wait()
    line = lax.broadcasted_iota(jnp.int32, (512, 128), 0)
    live[...] = jnp.where(line < count[0:1, :] * 128, 1.0, 0.0).astype(F32)
    for b in range(4):
        rows = pl.ds(b * 128, 128)
        send_row, recv_row = senders[pl.ds(b, 1), :], receivers[pl.ds(b, 1), :]
        pick_send[rows, :] = pick_rows(send_row, 768)
        pick_recv[rows, :] = pick_rows(recv_row, 512)
        place_recv[:, rows] = place_rows(recv_row, 512)
        place_send[:, rows] = place_rows(send_row, 768)
    for load in loads[3:]:
        load.wait()
    low = dot(pick_recv[...], nodes[...]).astype(BF16)
    receiver[...] = low
    partial[...] = dot(jnp.concatenate([edges[...], low], axis=1), around(ew1)) + eb1[...]


def around(weight):
    return jnp.concatenate([weight[0:128, :], weight[256:384, :]], axis=0)


def main_kernel(near, far, *refs):
    (
        (_, _, _, nodes, edges, ew1, _, ew2, eb2, egain, eshift, nw1, nb1, nw2, nb2, ngain, nshift, node_cot, edge_cot),
        (receiver, partial, live, pick_send, pick_recv, place_recv, place_send),
        (node_out, edge_out, grad_edge, local_grad, far_grad, keep, send),
        left,
        (
            table, messages, hidden, slope, normed, inverse, spread, dxs, dxr, sender, first_low, second_low,
            node_inputs, node_hidden, node_first, node_second, grads, leave,
        ),
    ) = refs[:19], refs[19:26], refs[26:33], refs[33:36], refs[36:]
    stores = [
        pltpu.make_async_copy(a, b, leave.at[k])
        for k, (a, b) in enumerate(zip(left, (edge_out, node_out, grad_edge)))
    ]
    edge_left, node_left, grad_left = left
    core = lax.axis_index("c")
    table[pl.ds(0, 512), :] = nodes[...]
    table[pl.ds(pl.multiple_of(640 - 128 * core, 128), 128), :] = near[...]
    table[pl.ds(pl.multiple_of(512 + 128 * core, 128), 128), :] = far[...]

    own = edges[...]
    low = dot(pick_send[...], table[...]).astype(BF16)
    sender[...] = low
    first = partial[...] + dot(low, ew1[128:256, :])
    sigmoid = jax.nn.sigmoid(first)
    low = (first * sigmoid).astype(BF16)
    hidden[...] = low
    slope[...] = sigmoid * (1.0 + first * (1.0 - sigmoid))
    n, inv = norm_forward(dot(low, ew2[...]) + eb2[...])
    normed[...] = n
    inverse[...] = inv
    message = (n * egain[...] + eshift[...]) * live[...]
    edge_left[...] = (own.astype(F32) + message).astype(BF16)
    messages[...] = split(message)

    stores[0].start()
    sums = [jnp.zeros((8, 128), F32) for _ in range(8)]
    aggregate = joined(dot(place_recv[...], messages[...])).astype(BF16)
    own = nodes[...]
    gathered = jnp.concatenate([own, aggregate], axis=1)
    node_inputs[...] = gathered
    first = dot(gathered, nw1[...]) + nb1[...]
    sigmoid = jax.nn.sigmoid(first)
    low = (first * sigmoid).astype(BF16)
    node_hidden[...] = low
    n, inv = norm_forward(dot(low, nw2[...]) + nb2[...])
    node_left[...] = (own.astype(F32) + (n * ngain[...] + nshift[...])).astype(BF16)
    cot = node_cot[...].astype(F32)
    g2 = norm_backward(cot, n, inv, ngain[...])
    g2_low = g2.astype(BF16)
    g1 = dot_nt(g2_low, nw2[...]) * (sigmoid * (1.0 + first * (1.0 - sigmoid)))
    g1_low = g1.astype(BF16)
    node_first[...] = g1_low
    node_second[...] = g2_low
    back = dot_nt(g1_low, nw1[...])
    local_grad[...] = cot + back[:, :128]
    spread[...] = split(back[:, 128:])
    for k, piece in enumerate((g1, g2, cot * n, cot)):
        sums[4 + k] += partial_sum(piece)
    stores[1].start()

    edge_grad = edge_cot[...].astype(F32)
    cot = live[...] * (edge_grad + joined(dot(pick_recv[...], spread[...])))
    n = normed[...]
    g2 = norm_backward(cot, n, inverse[...], egain[...])
    g2_low = g2.astype(BF16)
    g1 = dot_nt(g2_low, ew2[...]) * slope[...]
    g1_low = g1.astype(BF16)
    first_low[...] = g1_low
    second_low[...] = g2_low
    back = dot_nt(g1_low, ew1[...])
    grad_left[...] = (edge_grad + back[:, :128]).astype(BF16)
    dxs[...] = split(back[:, 128:256])
    dxr[...] = split(back[:, 256:])
    for k, piece in enumerate((g1, g2, cot * n, cot)):
        sums[k] += partial_sum(piece)
    stores[2].start()

    lower = joined(dot(place_send[512:640, :], dxs[...])).astype(BF16)
    upper = joined(dot(place_send[640:768, :], dxs[...])).astype(BF16)
    is_first = core == 0
    send[HALF:, :] = jnp.where(is_first, upper, lower)
    far_grad[...] = jnp.where(is_first, lower, upper)

    grads[0:128, :] = dot_tn(edges[...], first_low[...])
    grads[128:256, :] = dot_tn(sender[...], first_low[...])
    grads[256:384, :] = dot_tn(receiver[...], first_low[...])
    grads[384:385, :] = total(sums[0])
    grads[385:513, :] = dot_tn(hidden[...], second_low[...])
    grads[513:514, :] = total(sums[1])
    grads[514:515, :] = total(sums[2])
    grads[515:516, :] = total(sums[3])
    grads[516:772, :] = dot_tn(node_inputs[...], node_first[...])
    grads[772:773, :] = total(sums[4])
    grads[773:901, :] = dot_tn(node_hidden[...], node_second[...])
    grads[901:902, :] = total(sums[5])
    grads[902:903, :] = total(sums[6])
    grads[903:904, :] = total(sums[7])
    grads[904:1024, :] = jnp.zeros((120, 128), F32)
    keep[...] = grads[pl.ds(pl.multiple_of(core * HALF, HALF), HALF), :]
    send[0:HALF, :] = grads[pl.ds(pl.multiple_of((1 - core) * HALF, HALF), HALF), :].astype(BF16)

    for b in range(4):
        rows = pl.ds(b * 128, 128)
        both = dot(place_send[rows, :], dxs[...]) + dot(place_recv[rows, :], dxr[...])
        local_grad[rows, :] += joined(both)
    for store in stores:
        store.wait()


def fold_kernel(scale, tiles, copies):
    summed = tiles[0].astype(F32)
    for k in range(1, tiles.shape[0]):
        summed += tiles[k].astype(F32)
    low = (summed * scale).astype(BF16)
    for k in range(copies.shape[0]):
        copies[k] = low


def finish_kernel(local_grad, near, far, lists, out):
    core = lax.axis_index("c")
    added = dot(place_rows(lists[pl.ds(1 - core, 1), :], 512), near[...])
    added += dot(place_rows(lists[pl.ds(core, 1), :], 512), far[...])
    out[...] = (local_grad[...] + added).astype(BF16)


def call(body, out_shape, operands, in_specs=None, out_specs=None, scratch=(), flops=1000000, vmem=None):
    return pl.pallas_call(
        body,
        out_shape=out_shape,
        in_specs=in_specs or [VMEM] * len(operands),
        out_specs=out_specs or jax.tree.map(lambda _: VMEM, out_shape),
        scratch_shapes=scratch,
        compiler_params=pltpu.CompilerParams(vmem_limit_bytes=vmem),
        cost_estimate=pl.CostEstimate(flops=flops, bytes_accessed=1000000, transcendentals=0),
    )(*operands)


def fold(tiles, count, scale):
    out = jax.ShapeDtypeStruct((count, *tiles.shape[1:]), BF16)
    return call(functools.partial(fold_kernel, scale), out, (tiles,), vmem=SMALL)


def in_hbm(value):
    return pltpu.with_memory_space_constraint(value, pltpu.HBM)


def shape(rows, width, kind):
    return jax.ShapeDtypeStruct((rows, width), kind)


def prepare(sources):
    outs = tuple(jax.ShapeDtypeStruct(source.shape, source.dtype) for source in sources) + (
        shape(512, 128, BF16), shape(512, 128, F32), shape(512, 128, F32), shape(512, 768, BF16),
        shape(512, 512, BF16), shape(512, 512, BF16), shape(768, 512, BF16),
    )
    return call(
        prepare_kernel, outs, (sources[0], *(in_hbm(source) for source in sources[1:])), [VMEM] + [HBM] * 18,
        scratch=[pltpu.SemaphoreType.DMA((19,))], flops=400000000, vmem=16 << 20,
    )


def compute(near, far, prepared):
    outs = (
        shape(512, 128, BF16), shape(512, 128, BF16), shape(512, 128, BF16), shape(512, 128, F32),
        shape(128, 128, BF16), shape(HALF, 128, F32), shape(HALF + 128, 128, BF16),
    )
    scratch = [
        pltpu.VMEM(dims, kind)
        for dims, kind in (
            ((512, 128), BF16), ((512, 128), BF16), ((512, 128), BF16),
            ((768, 128), BF16), ((512, 256), BF16), ((512, 128), BF16), ((512, 128), F32),
            ((512, 128), F32), ((512, 1), F32), ((512, 256), BF16), ((512, 256), BF16), ((512, 256), BF16),
            ((512, 128), BF16), ((512, 128), BF16), ((512, 128), BF16), ((512, 256), BF16), ((512, 128), BF16),
            ((512, 128), BF16), ((512, 128), BF16), ((ROWS, 128), F32),
        )
    ] + [pltpu.SemaphoreType.DMA((3,))]
    return call(
        main_kernel, outs, (near, far, *prepared), [VMEM] * 28,
        (HBM,) * 3 + (VMEM,) * 4, scratch, 2000000000, 24 << 20,
    )


def layer(
    nodes, edges, senders, receivers, block_count, send_rows, node_cot, edge_cot,
    edge_w1, edge_b1, edge_w2, edge_b2, edge_gain, edge_shift,
    node_w1, node_b1, node_w2, node_b2, node_gain, node_shift,
):
    own_nodes = nodes[0]
    lists = send_rows[0, 0]
    line = lambda vector: vector.reshape(1, 128)
    near_pairs = [(j, j ^ 1) for j in range(64)]
    far_pairs = [(j, j + 1) for j in range(1, 63, 2)] + [(j + 1, j) for j in range(1, 63, 2)]

    near, far = call(
        pack_kernel, (shape(128, 128, BF16),) * 2, (in_hbm(own_nodes), in_hbm(lists)), [HBM] * 2,
        scratch=[
            pltpu.VMEM((512, 128), BF16), pltpu.VMEM((2, 128), jnp.int32), pltpu.SemaphoreType.DMA((2,))
        ],
        vmem=SMALL,
    )
    far = lax.ppermute(far, DOM, far_pairs)
    near = lax.ppermute(near, DOM, near_pairs)

    sources = (
        jnp.broadcast_to(block_count, (8, 128)), senders[0], receivers[0], own_nodes, edges[0].reshape(512, 128),
        edge_w1, line(edge_b1), edge_w2, line(edge_b2), line(edge_gain), line(edge_shift),
        node_w1, line(node_b1), node_w2, line(node_b2), line(node_gain), line(node_shift),
        node_cot[0], edge_cot[0].reshape(512, 128),
    )
    prepared = prepare(sources)
    node_out, edge_out, grad_edge, local_grad, far_grad, keep, send = compute(near, far, prepared)

    arrived = lax.ppermute(send, "c", [(0, 1), (1, 0)])
    far_back = lax.ppermute(far_grad, DOM, far_pairs)
    near_back = arrived[HALF:]
    scale = 1.0 / math.sqrt(lax.axis_size(DOM) * lax.axis_size("x") * 512)
    planes, columns = lax.axis_size(PLANE), lax.axis_size(COLUMN)
    rows = HALF // planes
    pair = (keep + arrived[:HALF].astype(F32)).astype(BF16)
    tiles = lax.all_to_all(pair.reshape(planes, rows, 128), PLANE, 0, 0, tiled=True)
    copies = fold(tiles, columns, 1.0)
    tiles = lax.all_to_all(copies, COLUMN, 0, 0, tiled=True)
    copies = fold(tiles, planes, scale)
    half = lax.all_to_all(copies, PLANE, 0, 0, tiled=True).reshape(HALF, 128)
    whole = lax.all_gather(half, "c", axis=0, tiled=True)
    weight_grads = whole[:LIVE_ROWS].astype(F32).reshape(LIVE_ROWS * 128)

    grad_node = call(finish_kernel, shape(512, 128, BF16), (local_grad, near_back, far_back, lists), vmem=SMALL)
    return (
        node_out[None],
        edge_out.reshape(1, 4, 128, 128),
        grad_node[None],
        grad_edge.reshape(1, 4, 128, 128),
        weight_grads,
    )


def solution(mesh):
    finer = Mesh(mesh.devices.reshape(4, 8, 2, mesh.shape["grp"]), ("y", "z", "c", "x"))
    by_row = P("x", DOM)
    return jax.shard_map(
        layer,
        mesh=finer,
        in_specs=(by_row,) * 8 + (P(),) * 12,
        out_specs=(by_row,) * 4 + (P(),),
        check_vma=False,
    )
```

```python
import math

import jax
import jax.numpy as jnp
from jax import lax
from jax.experimental import pallas as pl
from jax.experimental.pallas import tpu as pltpu
from jax.sharding import Mesh
from jax.sharding import PartitionSpec as P

DOM = ("y", "z", "c")
PLANE = ("y", "x")
COLUMN = ("z",)
EPSILON = 1e-05
F32 = jnp.float32
BF16 = jnp.bfloat16
ROWS = 1024
LIVE_ROWS = 904
SMALL = 8 << 20
VMEM = pl.BlockSpec(memory_space=pltpu.VMEM)
SMEM = pl.BlockSpec(memory_space=pltpu.SMEM)
HBM = pl.BlockSpec(memory_space=pltpu.HBM)


def dot(left, right):
    return jnp.dot(left, right, preferred_element_type=F32)


def dot_nt(left, right):
    return lax.dot_general(left, right, (((1,), (1,)), ((), ())), preferred_element_type=F32)


def dot_tn(left, right):
    return lax.dot_general(left, right, (((0,), (0,)), ((), ())), preferred_element_type=F32)


def as_bf16(mask):
    return jnp.where(mask, 1.0, 0.0).astype(BF16)


def pick_rows(row, count):
    column = jnp.transpose(jnp.broadcast_to(row, (128, 128)))
    lanes = lax.broadcasted_iota(jnp.int32, (128, 128), 1)
    tiles = [as_bf16(column == lanes + 128 * j) for j in range(count // 128)]
    return jnp.concatenate(tiles, axis=1)


def place_rows(row, count):
    lines = lax.broadcasted_iota(jnp.int32, (count, 128), 0)
    return as_bf16(lines == row)


def split(value):
    high = value.astype(BF16)
    low = (value - high.astype(F32)).astype(BF16)
    return jnp.concatenate([high, low], axis=1)


def joined(value):
    return value[:, :128] + value[:, 128:]


def pack_kernel(nodes_in, lists_in, near, far, nodes, lists, arrive):
    loads = [
        pltpu.make_async_copy(nodes_in, nodes, arrive.at[0]),
        pltpu.make_async_copy(lists_in, lists, arrive.at[1]),
    ]
    for load in loads:
        load.start()
    for load in loads[::-1]:
        load.wait()
    core = lax.axis_index("c")
    near[...] = dot(pick_rows(lists[pl.ds(1 - core, 1), :], 512), nodes[...]).astype(BF16)
    far[...] = dot(pick_rows(lists[pl.ds(core, 1), :], 512), nodes[...]).astype(BF16)


def norm_forward(second):
    average = jnp.mean(second, axis=-1, keepdims=True)
    centred = second - average
    variance = jnp.mean(centred * centred, axis=-1, keepdims=True)
    inverse = lax.rsqrt(variance + EPSILON)
    return centred * inverse, inverse


def norm_backward(cot, normed, inverse, gain):
    scaled = cot * gain
    return inverse * (
        scaled
        - jnp.mean(scaled, axis=-1, keepdims=True)
        - normed * jnp.mean(scaled * normed, axis=-1, keepdims=True)
    )


def partial_sum(value):
    return jnp.sum(value.reshape(-1, 8, 128), axis=0)


def total(value):
    return jnp.sum(value, axis=0, keepdims=True)


def prepare_kernel(*refs):
    sources, landed, (receiver, partial, live, pick_send, pick_recv, place_recv, place_send), (arrive,) = (
        refs[:19], refs[19:38], refs[38:45], refs[45:],
    )
    loads = [pltpu.make_async_copy(a, b, arrive.at[k]) for k, (a, b) in enumerate(zip(sources, landed))]
    for load in loads:
        load.start()
    count, senders, receivers, nodes, edges, ew1, eb1 = landed[:7]
    for load in loads[:3]:
        load.wait()
    line = lax.broadcasted_iota(jnp.int32, (512, 128), 0)
    live[...] = jnp.where(line < count[0:1, :] * 128, 1.0, 0.0).astype(F32)
    for b in range(4):
        rows = pl.ds(b * 128, 128)
        send_row, recv_row = senders[pl.ds(b, 1), :], receivers[pl.ds(b, 1), :]
        pick_send[rows, :] = pick_rows(send_row, 768)
        pick_recv[rows, :] = pick_rows(recv_row, 512)
        place_recv[:, rows] = place_rows(recv_row, 512)
        place_send[:, rows] = place_rows(send_row, 768)
    for load in loads[3:]:
        load.wait()
    low = dot(pick_recv[...], nodes[...]).astype(BF16)
    receiver[...] = low
    partial[...] = dot(jnp.concatenate([edges[...], low], axis=1), around(ew1)) + eb1[...]


def around(weight):
    return jnp.concatenate([weight[0:128, :], weight[256:384, :]], axis=0)


def main_kernel(near, far, *refs):
    (
        (_, _, _, nodes, edges, ew1, _, ew2, eb2, egain, eshift, nw1, nb1, nw2, nb2, ngain, nshift, node_cot, edge_cot),
        (receiver, partial, live, pick_send, pick_recv, place_recv, place_send),
        (node_out, edge_out, grad_edge, local_grad, keep, send),
        left,
        (
            table, messages, hidden, slope, normed, inverse, spread, dxs, dxr, sender, first_low, second_low,
            node_inputs, node_hidden, node_first, node_second, leave,
        ),
    ) = refs[:19], refs[19:26], refs[26:32], refs[32:35], refs[35:]
    stores = [
        pltpu.make_async_copy(a, b, leave.at[k])
        for k, (a, b) in enumerate(zip(left, (edge_out, node_out, grad_edge)))
    ]
    edge_left, node_left, grad_left = left
    core = lax.axis_index("c")
    table[pl.ds(0, 512), :] = nodes[...]
    table[pl.ds(pl.multiple_of(640 - 128 * core, 128), 128), :] = near[...]
    place = lax.axis_index("y") * lax.axis_size("z") + lax.axis_index("z")
    last = lax.axis_size("y") * lax.axis_size("z") - 1
    alone = place == core * last
    table[pl.ds(pl.multiple_of(512 + 128 * core, 128), 128), :] = jnp.where(alone, 0.0, far[...].astype(F32)).astype(BF16)

    own = edges[...]
    low = dot(pick_send[...], table[...]).astype(BF16)
    sender[...] = low
    first = partial[...] + dot(low, ew1[128:256, :])
    sigmoid = jax.nn.sigmoid(first)
    low = (first * sigmoid).astype(BF16)
    hidden[...] = low
    slope[...] = sigmoid * (1.0 + first * (1.0 - sigmoid))
    n, inv = norm_forward(dot(low, ew2[...]) + eb2[...])
    normed[...] = n
    inverse[...] = inv
    message = (n * egain[...] + eshift[...]) * live[...]
    edge_left[...] = (own.astype(F32) + message).astype(BF16)
    messages[...] = split(message)

    stores[0].start()
    sums = [jnp.zeros((8, 128), F32) for _ in range(8)]
    aggregate = joined(dot(place_recv[...], messages[...])).astype(BF16)
    own = nodes[...]
    gathered = jnp.concatenate([own, aggregate], axis=1)
    node_inputs[...] = gathered
    first = dot(gathered, nw1[...]) + nb1[...]
    sigmoid = jax.nn.sigmoid(first)
    low = (first * sigmoid).astype(BF16)
    node_hidden[...] = low
    n, inv = norm_forward(dot(low, nw2[...]) + nb2[...])
    node_left[...] = (own.astype(F32) + (n * ngain[...] + nshift[...])).astype(BF16)
    cot = node_cot[...].astype(F32)
    g2 = norm_backward(cot, n, inv, ngain[...])
    g2_low = g2.astype(BF16)
    g1 = dot_nt(g2_low, nw2[...]) * (sigmoid * (1.0 + first * (1.0 - sigmoid)))
    g1_low = g1.astype(BF16)
    node_first[...] = g1_low
    node_second[...] = g2_low
    back = dot_nt(g1_low, nw1[...])
    local_grad[...] = cot + back[:, :128]
    spread[...] = split(back[:, 128:])
    for k, piece in enumerate((g1, g2, cot * n, cot)):
        sums[4 + k] += partial_sum(piece)
    stores[1].start()

    edge_grad = edge_cot[...].astype(F32)
    cot = live[...] * (edge_grad + joined(dot(pick_recv[...], spread[...])))
    n = normed[...]
    g2 = norm_backward(cot, n, inverse[...], egain[...])
    g2_low = g2.astype(BF16)
    g1 = dot_nt(g2_low, ew2[...]) * slope[...]
    g1_low = g1.astype(BF16)
    first_low[...] = g1_low
    second_low[...] = g2_low
    back = dot_nt(g1_low, ew1[...])
    grad_left[...] = (edge_grad + back[:, :128]).astype(BF16)
    dxs[...] = split(back[:, 128:256])
    dxr[...] = split(back[:, 256:])
    for k, piece in enumerate((g1, g2, cot * n, cot)):
        sums[k] += partial_sum(piece)
    stores[2].start()

    lower = joined(dot(place_send[512:640, :], dxs[...])).astype(BF16)
    upper = joined(dot(place_send[640:768, :], dxs[...])).astype(BF16)
    is_first = core == 0
    send[ROWS : ROWS + 128, :] = jnp.where(is_first, upper, lower)
    send[ROWS + 128 :, :] = jnp.where(is_first, lower, upper)

    keep[0:128, :] = dot_tn(edges[...], first_low[...])
    keep[128:256, :] = dot_tn(sender[...], first_low[...])
    keep[256:384, :] = dot_tn(receiver[...], first_low[...])
    keep[384:385, :] = total(sums[0])
    keep[385:513, :] = dot_tn(hidden[...], second_low[...])
    keep[513:514, :] = total(sums[1])
    keep[514:515, :] = total(sums[2])
    keep[515:516, :] = total(sums[3])
    keep[516:772, :] = dot_tn(node_inputs[...], node_first[...])
    keep[772:773, :] = total(sums[4])
    keep[773:901, :] = dot_tn(node_hidden[...], node_second[...])
    keep[901:902, :] = total(sums[5])
    keep[902:903, :] = total(sums[6])
    keep[903:904, :] = total(sums[7])
    keep[904:1024, :] = jnp.zeros((120, 128), F32)
    send[0:ROWS, :] = keep[...].astype(BF16)

    for b in range(4):
        rows = pl.ds(b * 128, 128)
        both = dot(place_send[rows, :], dxs[...]) + dot(place_recv[rows, :], dxr[...])
        local_grad[rows, :] += joined(both)
    for store in stores:
        store.wait()


def finish_kernel(
    local_grad, near, turned, downward, result, received, lists, grad_node, weight_grads, node_left, weight_left, leave
):
    core = lax.axis_index("c")
    is_first = core == 0
    stores = [
        pltpu.make_async_copy(weight_left, weight_grads, leave.at[0]),
        pltpu.make_async_copy(node_left, grad_node, leave.at[1]),
    ]
    whole = jnp.where(is_first, received[0:LIVE_ROWS, :].astype(F32), result[0:LIVE_ROWS, :].astype(F32))
    weight_left[...] = whole
    stores[0].start()
    far = jnp.where(is_first, turned[0:128, :].astype(F32), downward[...].astype(F32)).astype(BF16)
    added = dot(place_rows(lists[pl.ds(1 - core, 1), :], 512), near[...])
    added += dot(place_rows(lists[pl.ds(core, 1), :], 512), far)
    node_left[...] = (local_grad[...] + added).astype(BF16)
    stores[1].start()
    for store in stores:
        store.wait()


def call(body, out_shape, operands, in_specs=None, out_specs=None, scratch=(), flops=1000000, vmem=None):
    return pl.pallas_call(
        body,
        out_shape=out_shape,
        in_specs=in_specs or [VMEM] * len(operands),
        out_specs=out_specs or jax.tree.map(lambda _: VMEM, out_shape),
        scratch_shapes=scratch,
        compiler_params=pltpu.CompilerParams(vmem_limit_bytes=vmem),
        cost_estimate=pl.CostEstimate(flops=flops, bytes_accessed=1000000, transcendentals=0),
    )(*operands)


def in_hbm(value):
    return pltpu.with_memory_space_constraint(value, pltpu.HBM)


def shape(rows, width, kind):
    return jax.ShapeDtypeStruct((rows, width), kind)


def prepare(sources):
    outs = tuple(jax.ShapeDtypeStruct(source.shape, source.dtype) for source in sources) + (
        shape(512, 128, BF16), shape(512, 128, F32), shape(512, 128, F32), shape(512, 768, BF16),
        shape(512, 512, BF16), shape(512, 512, BF16), shape(768, 512, BF16),
    )
    return call(
        prepare_kernel, outs, (sources[0], *(in_hbm(source) for source in sources[1:])), [VMEM] + [HBM] * 18,
        scratch=[pltpu.SemaphoreType.DMA((19,))], flops=400000000, vmem=16 << 20,
    )


def compute(near, far, prepared):
    outs = (
        shape(512, 128, BF16), shape(512, 128, BF16), shape(512, 128, BF16), shape(512, 128, F32),
        shape(ROWS, 128, F32), shape(ROWS + 256, 128, BF16),
    )
    scratch = [
        pltpu.VMEM(dims, kind)
        for dims, kind in (
            ((512, 128), BF16), ((512, 128), BF16), ((512, 128), BF16),
            ((768, 128), BF16), ((512, 256), BF16), ((512, 128), BF16), ((512, 128), F32),
            ((512, 128), F32), ((512, 1), F32), ((512, 256), BF16), ((512, 256), BF16), ((512, 256), BF16),
            ((512, 128), BF16), ((512, 128), BF16), ((512, 128), BF16), ((512, 256), BF16), ((512, 128), BF16),
            ((512, 128), BF16), ((512, 128), BF16),
        )
    ] + [pltpu.SemaphoreType.DMA((3,))]
    return call(
        main_kernel, outs, (near, far, *prepared), [VMEM] * 28,
        (HBM,) * 3 + (VMEM,) * 3, scratch, 2000000000, 24 << 20,
    )


def layer(
    nodes, edges, senders, receivers, block_count, send_rows, node_cot, edge_cot,
    edge_w1, edge_b1, edge_w2, edge_b2, edge_gain, edge_shift,
    node_w1, node_b1, node_w2, node_b2, node_gain, node_shift,
):
    own_nodes = nodes[0]
    lists = send_rows[0, 0]
    line = lambda vector: vector.reshape(1, 128)
    near_pairs = [(j, j ^ 1) for j in range(64)]
    far_pairs = [(j, (j + 1) % 64) for j in range(1, 64, 2)] + [((j + 1) % 64, j) for j in range(1, 64, 2)]
    down = [(j, j - 2) for j in range(2, 64, 2)]
    up = [(j - 2, j) for j in range(2, 64, 2)]

    near, far = call(
        pack_kernel, (shape(128, 128, BF16),) * 2, (in_hbm(own_nodes), in_hbm(lists)), [HBM] * 2,
        scratch=[
            pltpu.VMEM((512, 128), BF16), pltpu.VMEM((2, 128), jnp.int32), pltpu.SemaphoreType.DMA((2,))
        ],
        vmem=SMALL,
    )
    far = lax.ppermute(far, DOM, far_pairs)
    near = lax.ppermute(near, DOM, near_pairs)

    sources = (
        jnp.broadcast_to(block_count, (8, 128)), senders[0], receivers[0], own_nodes, edges[0].reshape(512, 128),
        edge_w1, line(edge_b1), edge_w2, line(edge_b2), line(edge_gain), line(edge_shift),
        node_w1, line(node_b1), node_w2, line(node_b2), line(node_gain), line(node_shift),
        node_cot[0], edge_cot[0].reshape(512, 128),
    )
    prepared = prepare(sources)
    node_out, edge_out, grad_edge, local_grad, keep, send = compute(near, far, prepared)

    scale = 1.0 / math.sqrt(lax.axis_size(DOM) * lax.axis_size("x") * 512)
    planes, columns = lax.axis_size(PLANE), lax.axis_size(COLUMN)
    arrived = lax.ppermute(send, "c", [(0, 1), (1, 0)])
    pair = (keep + arrived[:ROWS].astype(F32)).astype(BF16)
    near_back = arrived[ROWS : ROWS + 128]

    def carry(pair, mine, other):
        upward, downward = lax.ppermute(other, DOM, up), lax.ppermute(mine, DOM, down)
        return pair, jnp.concatenate([upward, downward], axis=0)

    def reduce(pair, mine, other):
        tiles = lax.all_to_all(pair.reshape(planes, -1, 128), PLANE, 0, 0, tiled=True)
        piece = jnp.sum(tiles.astype(F32), axis=0).astype(BF16)
        copies = jnp.broadcast_to(piece, (columns, *piece.shape))
        tiles = lax.all_to_all(copies, COLUMN, 0, 0, tiled=True)
        piece = (jnp.sum(tiles.astype(F32), axis=0) * scale).astype(BF16)
        copies = jnp.broadcast_to(piece, (planes, *piece.shape))
        tiles = lax.all_to_all(copies, PLANE, 0, 0, tiled=True)
        whole = tiles.reshape(ROWS, 128)
        return whole, whole[0:256]

    result, turned = lax.cond(
        lax.axis_index("c") == 0, carry, reduce, pair, send[ROWS + 128 :], arrived[ROWS + 128 :]
    )
    received = lax.ppermute(result, "c", [(0, 1), (1, 0)])
    downward = lax.ppermute(turned[128:], "c", [(0, 1), (1, 0)])
    grad_node, weight_grads = call(
        finish_kernel, (shape(512, 128, BF16), shape(LIVE_ROWS, 128, F32)),
        (local_grad, near_back, turned, downward, result, received, lists), [VMEM] * 7, (HBM,) * 2,
        [
            pltpu.VMEM((512, 128), BF16), pltpu.VMEM((LIVE_ROWS, 128), F32), pltpu.SemaphoreType.DMA((2,))
        ],
        vmem=SMALL,
    )
    return (
        node_out[None],
        edge_out.reshape(1, 4, 128, 128),
        grad_node[None],
        grad_edge.reshape(1, 4, 128, 128),
        weight_grads.reshape(LIVE_ROWS * 128),
    )


def solution(mesh):
    finer = Mesh(mesh.devices.reshape(4, 8, 2, mesh.shape["grp"]), ("y", "z", "c", "x"))
    by_row = P("x", DOM)
    return jax.shard_map(
        layer,
        mesh=finer,
        in_specs=(by_row,) * 8 + (P(),) * 12,
        out_specs=(by_row,) * 4 + (P(),),
        check_vma=False,
    )
```

```python
import math

import jax
import jax.numpy as jnp
from jax import lax
from jax.experimental import pallas as pl
from jax.experimental.pallas import tpu as pltpu
from jax.sharding import Mesh
from jax.sharding import PartitionSpec as P

DOM = ("y", "z", "c")
PLANE = ("y", "x")
COLUMN = ("z",)
EPSILON = 1e-05
F32 = jnp.float32
BF16 = jnp.bfloat16
ROWS = 1024
LIVE_ROWS = 904
SMALL = 8 << 20
VMEM = pl.BlockSpec(memory_space=pltpu.VMEM)
SMEM = pl.BlockSpec(memory_space=pltpu.SMEM)
HBM = pl.BlockSpec(memory_space=pltpu.HBM)


def dot(left, right):
    return jnp.dot(left, right, preferred_element_type=F32)


def dot_nt(left, right):
    return lax.dot_general(left, right, (((1,), (1,)), ((), ())), preferred_element_type=F32)


def dot_tn(left, right):
    return lax.dot_general(left, right, (((0,), (0,)), ((), ())), preferred_element_type=F32)


def as_bf16(mask):
    return jnp.where(mask, jnp.ones((), BF16), jnp.zeros((), BF16))


def pick_rows(row, count):
    column = jnp.transpose(jnp.broadcast_to(row, (128, 128))).astype(jnp.int16)
    lanes = lax.broadcasted_iota(jnp.int16, (128, 128), 1)
    tiles = [as_bf16(column - jnp.int16(128 * j) == lanes) for j in range(count // 128)]
    return jnp.concatenate(tiles, axis=1)


def place_rows(row, count):
    lines = lax.broadcasted_iota(jnp.int16, (128, 128), 0)
    wide = jnp.broadcast_to(row, (128, 128)).astype(jnp.int16)
    tiles = [as_bf16(wide - jnp.int16(128 * j) == lines) for j in range(count // 128)]
    return jnp.concatenate(tiles, axis=0)


def split(value):
    high = value.astype(BF16)
    low = (value - high.astype(F32)).astype(BF16)
    return jnp.concatenate([high, low], axis=1)


def joined(value):
    return value[:, :128] + value[:, 128:]


def pack_kernel(*refs):
    sources, (near, far), landed, (lists, arrive) = refs[:4], refs[4:6], refs[6:9], refs[9:]
    loads = [
        pltpu.make_async_copy(a, b, arrive.at[k])
        for k, (a, b) in enumerate(zip(sources, (lists, *landed)))
    ]
    for load in loads:
        load.start()
    nodes = landed[0]
    for load in loads[:2]:
        load.wait()
    core = lax.axis_index("c")
    near[...] = dot(pick_rows(lists[pl.ds(1 - core, 1), :], 512), nodes[...]).astype(BF16)
    far[...] = dot(pick_rows(lists[pl.ds(core, 1), :], 512), nodes[...]).astype(BF16)
    for load in loads[2:]:
        load.wait()


def norm_forward(second):
    average = jnp.mean(second, axis=-1, keepdims=True)
    centred = second - average
    variance = jnp.mean(centred * centred, axis=-1, keepdims=True)
    inverse = lax.rsqrt(variance + EPSILON)
    return centred * inverse, inverse


def norm_backward(cot, normed, inverse, gain):
    scaled = cot * gain
    return inverse * (
        scaled
        - jnp.mean(scaled, axis=-1, keepdims=True)
        - normed * jnp.mean(scaled * normed, axis=-1, keepdims=True)
    )


def partial_sum(value):
    return jnp.sum(value.reshape(-1, 8, 128), axis=0)


def total(value):
    return jnp.sum(value, axis=0, keepdims=True)


def prepare_kernel(nodes, senders, receivers, count, *refs):
    sources, landed, (receiver, partial, live, pick_send, pick_recv, place_recv, place_send), (arrive,) = (
        refs[:15], refs[15:30], refs[30:37], refs[37:],
    )
    loads = [pltpu.make_async_copy(a, b, arrive.at[k]) for k, (a, b) in enumerate(zip(sources, landed))]
    for load in loads:
        load.start()
    edges, ew1, eb1 = landed[:3]
    line = lax.broadcasted_iota(jnp.int32, (512, 128), 0)
    live[...] = jnp.where(line < count[0:1, 0:1] * 128, 1.0, 0.0).astype(F32)
    for b in range(4):
        rows = pl.ds(b * 128, 128)
        send_row, recv_row = senders[pl.ds(b, 1), :], receivers[pl.ds(b, 1), :]
        pick_send[rows, :] = pick_rows(send_row, 768)
        pick_recv[rows, :] = pick_rows(recv_row, 512)
        place_recv[:, rows] = place_rows(recv_row, 512)
        place_send[:, rows] = place_rows(send_row, 768)
    for load in loads:
        load.wait()
    low = dot(pick_recv[...], nodes[...]).astype(BF16)
    receiver[...] = low
    partial[...] = dot(jnp.concatenate([edges[...], low], axis=1), around(ew1)) + eb1[...]


def around(weight):
    return jnp.concatenate([weight[0:128, :], weight[256:384, :]], axis=0)


def main_kernel(near, far, nodes, *refs):
    (
        (edges, ew1, _, ew2, eb2, egain, eshift, nw1, nb1, nw2, nb2, ngain, nshift, node_cot, edge_cot),
        (receiver, partial, live, pick_send, pick_recv, place_recv, place_send),
        (node_out, edge_out, grad_edge, local_grad, keep, send),
        left,
        (
            table, messages, hidden, slope, normed, inverse, spread, dxs, dxr, sender, first_low, second_low,
            node_inputs, node_hidden, node_first, node_second, leave,
        ),
    ) = refs[:15], refs[15:22], refs[22:28], refs[28:31], refs[31:]
    stores = [
        pltpu.make_async_copy(a, b, leave.at[k])
        for k, (a, b) in enumerate(zip(left, (edge_out, node_out, grad_edge)))
    ]
    edge_left, node_left, grad_left = left
    core = lax.axis_index("c")
    table[pl.ds(0, 512), :] = nodes[...]
    table[pl.ds(pl.multiple_of(640 - 128 * core, 128), 128), :] = near[...]
    place = lax.axis_index("y") * lax.axis_size("z") + lax.axis_index("z")
    last = lax.axis_size("y") * lax.axis_size("z") - 1
    alone = place == core * last
    table[pl.ds(pl.multiple_of(512 + 128 * core, 128), 128), :] = jnp.where(alone, 0.0, far[...].astype(F32)).astype(BF16)

    own = edges[...]
    low = dot(pick_send[...], table[...]).astype(BF16)
    sender[...] = low
    first = partial[...] + dot(low, ew1[128:256, :])
    sigmoid = jax.nn.sigmoid(first)
    low = (first * sigmoid).astype(BF16)
    hidden[...] = low
    slope[...] = sigmoid * (1.0 + first * (1.0 - sigmoid))
    n, inv = norm_forward(dot(low, ew2[...]) + eb2[...])
    normed[...] = n
    inverse[...] = inv
    message = (n * egain[...] + eshift[...]) * live[...]
    edge_left[...] = (own.astype(F32) + message).astype(BF16)
    messages[...] = split(message)

    stores[0].start()
    sums = [jnp.zeros((8, 128), F32) for _ in range(8)]
    aggregate = joined(dot(place_recv[...], messages[...])).astype(BF16)
    own = nodes[...]
    gathered = jnp.concatenate([own, aggregate], axis=1)
    node_inputs[...] = gathered
    first = dot(gathered, nw1[...]) + nb1[...]
    sigmoid = jax.nn.sigmoid(first)
    low = (first * sigmoid).astype(BF16)
    node_hidden[...] = low
    n, inv = norm_forward(dot(low, nw2[...]) + nb2[...])
    node_left[...] = (own.astype(F32) + (n * ngain[...] + nshift[...])).astype(BF16)
    cot = node_cot[...].astype(F32)
    g2 = norm_backward(cot, n, inv, ngain[...])
    g2_low = g2.astype(BF16)
    g1 = dot_nt(g2_low, nw2[...]) * (sigmoid * (1.0 + first * (1.0 - sigmoid)))
    g1_low = g1.astype(BF16)
    node_first[...] = g1_low
    node_second[...] = g2_low
    back = dot_nt(g1_low, nw1[...])
    local_grad[...] = cot + back[:, :128]
    spread[...] = split(back[:, 128:])
    for k, piece in enumerate((g1, g2, cot * n, cot)):
        sums[4 + k] += partial_sum(piece)
    stores[1].start()

    edge_grad = edge_cot[...].astype(F32)
    cot = live[...] * (edge_grad + joined(dot(pick_recv[...], spread[...])))
    n = normed[...]
    g2 = norm_backward(cot, n, inverse[...], egain[...])
    g2_low = g2.astype(BF16)
    g1 = dot_nt(g2_low, ew2[...]) * slope[...]
    g1_low = g1.astype(BF16)
    first_low[...] = g1_low
    second_low[...] = g2_low
    back = dot_nt(g1_low, ew1[...])
    grad_left[...] = (edge_grad + back[:, :128]).astype(BF16)
    dxs[...] = split(back[:, 128:256])
    dxr[...] = split(back[:, 256:])
    for k, piece in enumerate((g1, g2, cot * n, cot)):
        sums[k] += partial_sum(piece)
    stores[2].start()

    lower = joined(dot(place_send[512:640, :], dxs[...])).astype(BF16)
    upper = joined(dot(place_send[640:768, :], dxs[...])).astype(BF16)
    is_first = core == 0
    send[ROWS : ROWS + 128, :] = jnp.where(is_first, upper, lower)
    send[ROWS + 128 :, :] = jnp.where(is_first, lower, upper)

    keep[0:128, :] = dot_tn(edges[...], first_low[...])
    keep[128:256, :] = dot_tn(sender[...], first_low[...])
    keep[256:384, :] = dot_tn(receiver[...], first_low[...])
    keep[384:385, :] = total(sums[0])
    keep[385:513, :] = dot_tn(hidden[...], second_low[...])
    keep[513:514, :] = total(sums[1])
    keep[514:515, :] = total(sums[2])
    keep[515:516, :] = total(sums[3])
    keep[516:772, :] = dot_tn(node_inputs[...], node_first[...])
    keep[772:773, :] = total(sums[4])
    keep[773:901, :] = dot_tn(node_hidden[...], node_second[...])
    keep[901:902, :] = total(sums[5])
    keep[902:903, :] = total(sums[6])
    keep[903:904, :] = total(sums[7])
    keep[904:1024, :] = jnp.zeros((120, 128), F32)
    send[0:ROWS, :] = keep[...].astype(BF16)

    for b in range(4):
        rows = pl.ds(b * 128, 128)
        both = dot(place_send[rows, :], dxs[...]) + dot(place_recv[rows, :], dxr[...])
        local_grad[rows, :] += joined(both)
    for store in stores:
        store.wait()


def finish_kernel(
    local_grad, near, turned, downward, result, received, lists, grad_node, weight_grads, node_left, weight_left, leave
):
    core = lax.axis_index("c")
    is_first = core == 0
    stores = [
        pltpu.make_async_copy(weight_left, weight_grads, leave.at[0]),
        pltpu.make_async_copy(node_left, grad_node, leave.at[1]),
    ]
    whole = jnp.where(is_first, received[0:LIVE_ROWS, :].astype(F32), result[0:LIVE_ROWS, :].astype(F32))
    weight_left[...] = whole
    stores[0].start()
    far = jnp.where(is_first, turned[0:128, :].astype(F32), downward[...].astype(F32)).astype(BF16)
    added = dot(place_rows(lists[pl.ds(1 - core, 1), :], 512), near[...])
    added += dot(place_rows(lists[pl.ds(core, 1), :], 512), far)
    node_left[...] = (local_grad[...] + added).astype(BF16)
    stores[1].start()
    for store in stores:
        store.wait()


def call(body, out_shape, operands, in_specs=None, out_specs=None, scratch=(), flops=1000000, vmem=None):
    return pl.pallas_call(
        body,
        out_shape=out_shape,
        in_specs=in_specs or [VMEM] * len(operands),
        out_specs=out_specs or jax.tree.map(lambda _: VMEM, out_shape),
        scratch_shapes=scratch,
        compiler_params=pltpu.CompilerParams(vmem_limit_bytes=vmem),
        cost_estimate=pl.CostEstimate(flops=flops, bytes_accessed=1000000, transcendentals=0),
    )(*operands)


def in_hbm(value):
    return pltpu.with_memory_space_constraint(value, pltpu.HBM)


def shape(rows, width, kind):
    return jax.ShapeDtypeStruct((rows, width), kind)


def prepare(early, sources):
    outs = tuple(jax.ShapeDtypeStruct(source.shape, source.dtype) for source in sources) + (
        shape(512, 128, BF16), shape(512, 128, F32), shape(512, 128, F32), shape(512, 768, BF16),
        shape(512, 512, BF16), shape(512, 512, BF16), shape(768, 512, BF16),
    )
    return call(
        prepare_kernel, outs, (*early, *(in_hbm(source) for source in sources)),
        [VMEM] * 4 + [HBM] * 15, scratch=[pltpu.SemaphoreType.DMA((15,))], flops=400000000, vmem=16 << 20,
    )


def compute(near, far, nodes, prepared):
    outs = (
        shape(512, 128, BF16), shape(512, 128, BF16), shape(512, 128, BF16), shape(512, 128, F32),
        shape(ROWS, 128, F32), shape(ROWS + 256, 128, BF16),
    )
    scratch = [
        pltpu.VMEM(dims, kind)
        for dims, kind in (
            ((512, 128), BF16), ((512, 128), BF16), ((512, 128), BF16),
            ((768, 128), BF16), ((512, 256), BF16), ((512, 128), BF16), ((512, 128), F32),
            ((512, 128), F32), ((512, 1), F32), ((512, 256), BF16), ((512, 256), BF16), ((512, 256), BF16),
            ((512, 128), BF16), ((512, 128), BF16), ((512, 128), BF16), ((512, 256), BF16), ((512, 128), BF16),
            ((512, 128), BF16), ((512, 128), BF16),
        )
    ] + [pltpu.SemaphoreType.DMA((3,))]
    return call(
        main_kernel, outs, (near, far, nodes, *prepared), [VMEM] * 25,
        (HBM,) * 3 + (VMEM,) * 3, scratch, 2000000000, 24 << 20,
    )


def layer(
    nodes, edges, senders, receivers, block_count, send_rows, node_cot, edge_cot,
    edge_w1, edge_b1, edge_w2, edge_b2, edge_gain, edge_shift,
    node_w1, node_b1, node_w2, node_b2, node_gain, node_shift,
):
    own_nodes = nodes[0]
    lists = send_rows[0, 0]
    line = lambda vector: vector.reshape(1, 128)
    near_pairs = [(j, j ^ 1) for j in range(64)]
    far_pairs = [(j, (j + 1) % 64) for j in range(1, 64, 2)] + [((j + 1) % 64, j) for j in range(1, 64, 2)]
    down = [(j, j - 2) for j in range(2, 64, 2)]
    up = [(j - 2, j) for j in range(2, 64, 2)]

    outs = (
        shape(128, 128, BF16), shape(128, 128, BF16), shape(512, 128, BF16), shape(4, 128, jnp.int32),
        shape(4, 128, jnp.int32),
    )
    near, far, *early = call(
        pack_kernel, outs,
        (in_hbm(lists), in_hbm(own_nodes), in_hbm(senders[0]), in_hbm(receivers[0])), [HBM] * 4,
        scratch=[pltpu.VMEM((2, 128), jnp.int32), pltpu.SemaphoreType.DMA((4,))],
        vmem=SMALL,
    )
    block_count, far = lax.optimization_barrier((block_count, far))
    early.append(jnp.pad(block_count, ((0, 7), (0, 127))))
    far = lax.ppermute(far, DOM, far_pairs)
    near = lax.ppermute(near, DOM, near_pairs)

    sources = (
        edges[0].reshape(512, 128),
        edge_w1, line(edge_b1), edge_w2, line(edge_b2), line(edge_gain), line(edge_shift),
        node_w1, line(node_b1), node_w2, line(node_b2), line(node_gain), line(node_shift),
        node_cot[0], edge_cot[0].reshape(512, 128),
    )
    prepared = prepare(early, sources)
    node_out, edge_out, grad_edge, local_grad, keep, send = compute(near, far, early[0], prepared)

    scale = 1.0 / math.sqrt(lax.axis_size(DOM) * lax.axis_size("x") * 512)
    planes, columns = lax.axis_size(PLANE), lax.axis_size(COLUMN)
    arrived = lax.ppermute(send, "c", [(0, 1), (1, 0)])
    pair = (keep + arrived[:ROWS].astype(F32)).astype(BF16)
    near_back = arrived[ROWS : ROWS + 128]

    def carry(pair, mine, other):
        upward, downward = lax.ppermute(other, DOM, up), lax.ppermute(mine, DOM, down)
        return pair, jnp.concatenate([upward, downward], axis=0)

    def reduce(pair, mine, other):
        tiles = lax.all_to_all(pair.reshape(planes, -1, 128), PLANE, 0, 0, tiled=True)
        piece = jnp.sum(tiles.astype(F32), axis=0).astype(BF16)
        copies = jnp.broadcast_to(piece, (columns, *piece.shape))
        tiles = lax.all_to_all(copies, COLUMN, 0, 0, tiled=True)
        piece = (jnp.sum(tiles.astype(F32), axis=0) * scale).astype(BF16)
        copies = jnp.broadcast_to(piece, (planes, *piece.shape))
        tiles = lax.all_to_all(copies, PLANE, 0, 0, tiled=True)
        whole = tiles.reshape(ROWS, 128)
        return whole, whole[0:256]

    result, turned = lax.cond(
        lax.axis_index("c") == 0, carry, reduce, pair, send[ROWS + 128 :], arrived[ROWS + 128 :]
    )
    received = lax.ppermute(result, "c", [(0, 1), (1, 0)])
    downward = lax.ppermute(turned[128:], "c", [(0, 1), (1, 0)])
    grad_node, weight_grads = call(
        finish_kernel, (shape(512, 128, BF16), shape(LIVE_ROWS, 128, F32)),
        (local_grad, near_back, turned, downward, result, received, lists), [VMEM] * 7, (HBM,) * 2,
        [
            pltpu.VMEM((512, 128), BF16), pltpu.VMEM((LIVE_ROWS, 128), F32), pltpu.SemaphoreType.DMA((2,))
        ],
        vmem=SMALL,
    )
    return (
        node_out[None],
        edge_out.reshape(1, 4, 128, 128),
        grad_node[None],
        grad_edge.reshape(1, 4, 128, 128),
        weight_grads.reshape(LIVE_ROWS * 128),
    )


def solution(mesh):
    finer = Mesh(mesh.devices.reshape(4, 8, 2, mesh.shape["grp"]), ("y", "z", "c", "x"))
    by_row = P("x", DOM)
    return jax.shard_map(
        layer,
        mesh=finer,
        in_specs=(by_row,) * 8 + (P(),) * 12,
        out_specs=(by_row,) * 4 + (P(),),
        check_vma=False,
    )
```

```python
import math

import jax
import jax.numpy as jnp
from jax import lax
from jax.experimental import pallas as pl
from jax.experimental.pallas import tpu as pltpu
from jax.sharding import Mesh
from jax.sharding import PartitionSpec as P

DOM = ("y", "z", "c")
PLANE = ("y", "x")
COLUMN = ("z",)
EPSILON = 1e-05
F32 = jnp.float32
BF16 = jnp.bfloat16
ROWS = 1024
LIVE_ROWS = 904
SMALL = 8 << 20
VMEM = pl.BlockSpec(memory_space=pltpu.VMEM)
SMEM = pl.BlockSpec(memory_space=pltpu.SMEM)
HBM = pl.BlockSpec(memory_space=pltpu.HBM)


def dot(left, right):
    return jnp.dot(left, right, preferred_element_type=F32)


def dot_nt(left, right):
    return lax.dot_general(left, right, (((1,), (1,)), ((), ())), preferred_element_type=F32)


def dot_tn(left, right):
    return lax.dot_general(left, right, (((0,), (0,)), ((), ())), preferred_element_type=F32)


def as_bf16(mask):
    return jnp.where(mask, jnp.ones((), BF16), jnp.zeros((), BF16))


def pick_rows(row, count):
    column = jnp.transpose(jnp.broadcast_to(row, (128, 128))).astype(jnp.int16)
    lanes = lax.broadcasted_iota(jnp.int16, (128, 128), 1)
    tiles = [as_bf16(column - jnp.int16(128 * j) == lanes) for j in range(count // 128)]
    return jnp.concatenate(tiles, axis=1)


def place_rows(row, count):
    lines = lax.broadcasted_iota(jnp.int16, (128, 128), 0)
    wide = jnp.broadcast_to(row, (128, 128)).astype(jnp.int16)
    tiles = [as_bf16(wide - jnp.int16(128 * j) == lines) for j in range(count // 128)]
    return jnp.concatenate(tiles, axis=0)


def split(value):
    high = value.astype(BF16)
    low = (value - high.astype(F32)).astype(BF16)
    return jnp.concatenate([high, low], axis=1)


def joined(value):
    return value[:, :128] + value[:, 128:]


def pack_kernel(*refs):
    sources, (near, far), landed, (lists, arrive) = refs[:4], refs[4:6], refs[6:9], refs[9:]
    loads = [
        pltpu.make_async_copy(a, b, arrive.at[k])
        for k, (a, b) in enumerate(zip(sources, (lists, *landed)))
    ]
    for load in loads:
        load.start()
    nodes = landed[0]
    for load in loads[:2]:
        load.wait()
    core = lax.axis_index("c")
    near[...] = dot(pick_rows(lists[pl.ds(1 - core, 1), :], 512), nodes[...]).astype(BF16)
    far[...] = dot(pick_rows(lists[pl.ds(core, 1), :], 512), nodes[...]).astype(BF16)
    for load in loads[2:]:
        load.wait()


def norm_forward(second):
    average = jnp.mean(second, axis=-1, keepdims=True)
    centred = second - average
    variance = jnp.mean(centred * centred, axis=-1, keepdims=True)
    inverse = lax.rsqrt(variance + EPSILON)
    return centred * inverse, inverse


def norm_backward(cot, normed, inverse, gain):
    scaled = cot * gain
    return inverse * (
        scaled
        - jnp.mean(scaled, axis=-1, keepdims=True)
        - normed * jnp.mean(scaled * normed, axis=-1, keepdims=True)
    )


def partial_sum(value):
    return jnp.sum(value.reshape(-1, 8, 128), axis=0)


def total(value):
    return jnp.sum(value, axis=0, keepdims=True)


def prepare_kernel(nodes, senders, receivers, count, *refs):
    sources, landed, (receiver, partial, live, pick_send, pick_recv, place_recv, place_send), (arrive,) = (
        refs[:15], refs[15:30], refs[30:37], refs[37:],
    )
    loads = [pltpu.make_async_copy(a, b, arrive.at[k]) for k, (a, b) in enumerate(zip(sources, landed))]
    for load in loads:
        load.start()
    edges, ew1, eb1 = landed[:3]
    line = lax.broadcasted_iota(jnp.int32, (512, 128), 0)
    live[...] = jnp.where(line < count[0:1, 0:1] * 128, 1.0, 0.0).astype(F32)
    for b in range(4):
        rows = pl.ds(b * 128, 128)
        send_row, recv_row = senders[pl.ds(b, 1), :], receivers[pl.ds(b, 1), :]
        pick_send[rows, :] = pick_rows(send_row, 768)
        pick_recv[rows, :] = pick_rows(recv_row, 512)
        place_recv[:, rows] = place_rows(recv_row, 512)
        place_send[:, rows] = place_rows(send_row, 768)
    for load in loads:
        load.wait()
    low = dot(pick_recv[...], nodes[...]).astype(BF16)
    receiver[...] = low
    partial[...] = dot(jnp.concatenate([edges[...], low], axis=1), around(ew1)) + eb1[...]


def around(weight):
    return jnp.concatenate([weight[0:128, :], weight[256:384, :]], axis=0)


def main_kernel(near, far, nodes, *refs):
    (
        (edges, ew1, _, ew2, eb2, egain, eshift, nw1, nb1, nw2, nb2, ngain, nshift, node_cot, edge_cot),
        (receiver, partial, live, pick_send, pick_recv, place_recv, place_send),
        (node_out, edge_out, grad_edge, local_grad, keep, send),
        left,
        (
            table, messages, hidden, slope, normed, inverse, spread, dxs, dxr, sender, first_low, second_low,
            node_inputs, node_hidden, node_first, node_second, leave,
        ),
    ) = refs[:15], refs[15:22], refs[22:28], refs[28:31], refs[31:]
    stores = [
        pltpu.make_async_copy(a, b, leave.at[k])
        for k, (a, b) in enumerate(zip(left, (edge_out, node_out, grad_edge)))
    ]
    edge_left, node_left, grad_left = left
    core = lax.axis_index("c")
    table[pl.ds(0, 512), :] = nodes[...]
    table[pl.ds(pl.multiple_of(640 - 128 * core, 128), 128), :] = near[...]
    place = lax.axis_index("y") * lax.axis_size("z") + lax.axis_index("z")
    last = lax.axis_size("y") * lax.axis_size("z") - 1
    alone = place == core * last
    table[pl.ds(pl.multiple_of(512 + 128 * core, 128), 128), :] = jnp.where(alone, 0.0, far[...].astype(F32)).astype(BF16)

    own = edges[...]
    low = dot(pick_send[...], table[...]).astype(BF16)
    sender[...] = low
    first = partial[...] + dot(low, ew1[128:256, :])
    sigmoid = jax.nn.sigmoid(first)
    low = (first * sigmoid).astype(BF16)
    hidden[...] = low
    slope[...] = sigmoid * (1.0 + first * (1.0 - sigmoid))
    n, inv = norm_forward(dot(low, ew2[...]) + eb2[...])
    normed[...] = n
    inverse[...] = inv
    message = (n * egain[...] + eshift[...]) * live[...]
    edge_left[...] = (own.astype(F32) + message).astype(BF16)
    messages[...] = split(message)

    stores[0].start()
    sums = [jnp.zeros((8, 128), F32) for _ in range(8)]
    aggregate = joined(dot(place_recv[...], messages[...])).astype(BF16)
    own = nodes[...]
    gathered = jnp.concatenate([own, aggregate], axis=1)
    node_inputs[...] = gathered
    first = dot(gathered, nw1[...]) + nb1[...]
    sigmoid = jax.nn.sigmoid(first)
    low = (first * sigmoid).astype(BF16)
    node_hidden[...] = low
    n, inv = norm_forward(dot(low, nw2[...]) + nb2[...])
    node_left[...] = (own.astype(F32) + (n * ngain[...] + nshift[...])).astype(BF16)
    cot = node_cot[...].astype(F32)
    g2 = norm_backward(cot, n, inv, ngain[...])
    g2_low = g2.astype(BF16)
    g1 = dot_nt(g2_low, nw2[...]) * (sigmoid * (1.0 + first * (1.0 - sigmoid)))
    g1_low = g1.astype(BF16)
    node_first[...] = g1_low
    node_second[...] = g2_low
    back = dot_nt(g1_low, nw1[...])
    local_grad[...] = cot + back[:, :128]
    spread[...] = split(back[:, 128:])
    for k, piece in enumerate((g1, g2, cot * n, cot)):
        sums[4 + k] += partial_sum(piece)
    stores[1].start()

    edge_grad = edge_cot[...].astype(F32)
    cot = live[...] * (edge_grad + joined(dot(pick_recv[...], spread[...])))
    n = normed[...]
    g2 = norm_backward(cot, n, inverse[...], egain[...])
    g2_low = g2.astype(BF16)
    g1 = dot_nt(g2_low, ew2[...]) * slope[...]
    g1_low = g1.astype(BF16)
    first_low[...] = g1_low
    second_low[...] = g2_low
    back = dot_nt(g1_low, ew1[...])
    grad_left[...] = (edge_grad + back[:, :128]).astype(BF16)
    dxs[...] = split(back[:, 128:256])
    dxr[...] = split(back[:, 256:])
    for k, piece in enumerate((g1, g2, cot * n, cot)):
        sums[k] += partial_sum(piece)
    stores[2].start()

    lower = joined(dot(place_send[512:640, :], dxs[...])).astype(BF16)
    upper = joined(dot(place_send[640:768, :], dxs[...])).astype(BF16)
    is_first = core == 0
    send[ROWS : ROWS + 128, :] = jnp.where(is_first, upper, lower)
    send[ROWS + 128 :, :] = jnp.where(is_first, lower, upper)

    keep[0:128, :] = dot_tn(edges[...], first_low[...])
    keep[128:256, :] = dot_tn(sender[...], first_low[...])
    keep[256:384, :] = dot_tn(receiver[...], first_low[...])
    keep[384:385, :] = total(sums[0])
    keep[385:513, :] = dot_tn(hidden[...], second_low[...])
    keep[513:514, :] = total(sums[1])
    keep[514:515, :] = total(sums[2])
    keep[515:516, :] = total(sums[3])
    keep[516:772, :] = dot_tn(node_inputs[...], node_first[...])
    keep[772:773, :] = total(sums[4])
    keep[773:901, :] = dot_tn(node_hidden[...], node_second[...])
    keep[901:902, :] = total(sums[5])
    keep[902:903, :] = total(sums[6])
    keep[903:904, :] = total(sums[7])
    keep[904:1024, :] = jnp.zeros((120, 128), F32)
    send[0:ROWS, :] = keep[...].astype(BF16)

    for b in range(4):
        rows = pl.ds(b * 128, 128)
        both = dot(place_send[rows, :], dxs[...]) + dot(place_recv[rows, :], dxr[...])
        local_grad[rows, :] += joined(both)
    for store in stores:
        store.wait()


def finish_kernel(
    local_grad, near, result, received, lists, grad_node, weight_grads, node_left, weight_left, leave
):
    core = lax.axis_index("c")
    is_first = core == 0
    stores = [
        pltpu.make_async_copy(weight_left, weight_grads, leave.at[0]),
        pltpu.make_async_copy(node_left, grad_node, leave.at[1]),
    ]
    whole = jnp.where(is_first, received[0:LIVE_ROWS, :].astype(F32), result[0:LIVE_ROWS, :].astype(F32))
    weight_left[...] = whole
    stores[0].start()
    upward, downward = result[ROWS + 128 :, :], received[ROWS : ROWS + 128, :]
    far = jnp.where(is_first, upward.astype(F32), downward.astype(F32)).astype(BF16)
    added = dot(place_rows(lists[pl.ds(1 - core, 1), :], 512), near[...])
    added += dot(place_rows(lists[pl.ds(core, 1), :], 512), far)
    node_left[...] = (local_grad[...] + added).astype(BF16)
    stores[1].start()
    for store in stores:
        store.wait()


def call(body, out_shape, operands, in_specs=None, out_specs=None, scratch=(), flops=1000000, vmem=None):
    return pl.pallas_call(
        body,
        out_shape=out_shape,
        in_specs=in_specs or [VMEM] * len(operands),
        out_specs=out_specs or jax.tree.map(lambda _: VMEM, out_shape),
        scratch_shapes=scratch,
        compiler_params=pltpu.CompilerParams(vmem_limit_bytes=vmem),
        cost_estimate=pl.CostEstimate(flops=flops, bytes_accessed=1000000, transcendentals=0),
    )(*operands)


def in_hbm(value):
    return pltpu.with_memory_space_constraint(value, pltpu.HBM)


def shape(rows, width, kind):
    return jax.ShapeDtypeStruct((rows, width), kind)


def prepare(early, sources):
    outs = tuple(jax.ShapeDtypeStruct(source.shape, source.dtype) for source in sources) + (
        shape(512, 128, BF16), shape(512, 128, F32), shape(512, 128, F32), shape(512, 768, BF16),
        shape(512, 512, BF16), shape(512, 512, BF16), shape(768, 512, BF16),
    )
    return call(
        prepare_kernel, outs, (*early, *(in_hbm(source) for source in sources)),
        [VMEM] * 4 + [HBM] * 15, scratch=[pltpu.SemaphoreType.DMA((15,))], flops=400000000, vmem=16 << 20,
    )


def compute(near, far, nodes, prepared):
    outs = (
        shape(512, 128, BF16), shape(512, 128, BF16), shape(512, 128, BF16), shape(512, 128, F32),
        shape(ROWS, 128, F32), shape(ROWS + 256, 128, BF16),
    )
    scratch = [
        pltpu.VMEM(dims, kind)
        for dims, kind in (
            ((512, 128), BF16), ((512, 128), BF16), ((512, 128), BF16),
            ((768, 128), BF16), ((512, 256), BF16), ((512, 128), BF16), ((512, 128), F32),
            ((512, 128), F32), ((512, 1), F32), ((512, 256), BF16), ((512, 256), BF16), ((512, 256), BF16),
            ((512, 128), BF16), ((512, 128), BF16), ((512, 128), BF16), ((512, 256), BF16), ((512, 128), BF16),
            ((512, 128), BF16), ((512, 128), BF16),
        )
    ] + [pltpu.SemaphoreType.DMA((3,))]
    return call(
        main_kernel, outs, (near, far, nodes, *prepared), [VMEM] * 25,
        (HBM,) * 3 + (VMEM,) * 3, scratch, 2000000000, 24 << 20,
    )


def layer(
    nodes, edges, senders, receivers, block_count, send_rows, node_cot, edge_cot,
    edge_w1, edge_b1, edge_w2, edge_b2, edge_gain, edge_shift,
    node_w1, node_b1, node_w2, node_b2, node_gain, node_shift,
):
    own_nodes = nodes[0]
    lists = send_rows[0, 0]
    line = lambda vector: vector.reshape(1, 128)
    near_pairs = [(j, j ^ 1) for j in range(64)]
    far_pairs = [(0, 0), (63, 63)] + [(j, j + 1) for j in range(1, 63, 2)] + [(j + 1, j) for j in range(1, 63, 2)]
    down = [(j, j - 2) for j in range(2, 64, 2)]
    up = [(j - 2, j) for j in range(2, 64, 2)]

    outs = (
        shape(128, 128, BF16), shape(128, 128, BF16), shape(512, 128, BF16), shape(4, 128, jnp.int32),
        shape(4, 128, jnp.int32),
    )
    near, far, *early = call(
        pack_kernel, outs,
        (in_hbm(lists), in_hbm(own_nodes), in_hbm(senders[0]), in_hbm(receivers[0])), [HBM] * 4,
        scratch=[pltpu.VMEM((2, 128), jnp.int32), pltpu.SemaphoreType.DMA((4,))],
        vmem=SMALL,
    )
    block_count, far = lax.optimization_barrier((block_count, far))
    early.append(jnp.pad(block_count, ((0, 7), (0, 127))))
    far = lax.ppermute(far, DOM, far_pairs)
    near = lax.ppermute(near, DOM, near_pairs)

    sources = (
        edges[0].reshape(512, 128),
        edge_w1, line(edge_b1), edge_w2, line(edge_b2), line(edge_gain), line(edge_shift),
        node_w1, line(node_b1), node_w2, line(node_b2), line(node_gain), line(node_shift),
        node_cot[0], edge_cot[0].reshape(512, 128),
    )
    prepared = prepare(early, sources)
    node_out, edge_out, grad_edge, local_grad, keep, send = compute(near, far, early[0], prepared)

    scale = 1.0 / math.sqrt(lax.axis_size(DOM) * lax.axis_size("x") * 512)
    planes, columns = lax.axis_size(PLANE), lax.axis_size(COLUMN)
    arrived = lax.ppermute(send, "c", [(0, 1), (1, 0)])
    pair = (keep + arrived[:ROWS].astype(F32)).astype(BF16)
    near_back = arrived[ROWS : ROWS + 128]

    def carry(pair, mine, other):
        upward, downward = lax.ppermute(other, DOM, up), lax.ppermute(mine, DOM, down)
        return jnp.concatenate([pair, downward, upward], axis=0)

    def reduce(pair, mine, other):
        tiles = lax.all_to_all(pair.reshape(planes, -1, 128), PLANE, 0, 0, tiled=True)
        piece = (jnp.sum(tiles.astype(F32), axis=0) * 0.0625).astype(BF16)
        copies = jnp.broadcast_to(piece, (columns, *piece.shape))
        tiles = lax.all_to_all(copies, COLUMN, 0, 0, tiled=True)
        piece = (jnp.sum(tiles.astype(F32), axis=0) * (16.0 * scale)).astype(BF16)
        copies = jnp.broadcast_to(piece, (planes, *piece.shape))
        tiles = lax.all_to_all(copies, PLANE, 0, 0, tiled=True)
        whole = tiles.reshape(ROWS, 128)
        return jnp.concatenate([whole, whole[0:256]], axis=0)

    result = lax.cond(
        lax.axis_index("c") == 0, carry, reduce, pair, send[ROWS + 128 :], arrived[ROWS + 128 :]
    )
    received = lax.ppermute(result, "c", [(0, 1), (1, 0)])
    grad_node, weight_grads = call(
        finish_kernel, (shape(512, 128, BF16), shape(LIVE_ROWS, 128, F32)),
        (local_grad, near_back, result, received, lists), [VMEM] * 5, (HBM,) * 2,
        [
            pltpu.VMEM((512, 128), BF16), pltpu.VMEM((LIVE_ROWS, 128), F32), pltpu.SemaphoreType.DMA((2,))
        ],
        vmem=SMALL,
    )
    return (
        node_out[None],
        edge_out.reshape(1, 4, 128, 128),
        grad_node[None],
        grad_edge.reshape(1, 4, 128, 128),
        weight_grads.reshape(LIVE_ROWS * 128),
    )


def solution(mesh):
    finer = Mesh(mesh.devices.reshape(4, 8, 2, mesh.shape["grp"]), ("y", "z", "c", "x"))
    by_row = P("x", DOM)
    return jax.shard_map(
        layer,
        mesh=finer,
        in_specs=(by_row,) * 8 + (P(),) * 12,
        out_specs=(by_row,) * 4 + (P(),),
        check_vma=False,
    )
```

```python
import math

import jax
import jax.numpy as jnp
from jax import lax
from jax.experimental import pallas as pl
from jax.experimental.pallas import tpu as pltpu
from jax.sharding import Mesh
from jax.sharding import PartitionSpec as P

DOM = ("y", "z", "c")
PLANE = ("y", "x")
COLUMN = ("z",)
EPSILON = 1e-05
F32 = jnp.float32
BF16 = jnp.bfloat16
ROWS = 1024
LIVE_ROWS = 904
SMALL = 8 << 20
VMEM = pl.BlockSpec(memory_space=pltpu.VMEM)
SMEM = pl.BlockSpec(memory_space=pltpu.SMEM)
HBM = pl.BlockSpec(memory_space=pltpu.HBM)


def dot(left, right):
    return jnp.dot(left, right, preferred_element_type=F32)


def dot_nt(left, right):
    return lax.dot_general(left, right, (((1,), (1,)), ((), ())), preferred_element_type=F32)


def dot_tn(left, right):
    return lax.dot_general(left, right, (((0,), (0,)), ((), ())), preferred_element_type=F32)


def as_bf16(mask):
    return jnp.where(mask, jnp.ones((), BF16), jnp.zeros((), BF16))


def pick_rows(row, count):
    column = jnp.transpose(jnp.broadcast_to(row, (128, 128))).astype(jnp.int16)
    lanes = lax.broadcasted_iota(jnp.int16, (128, 128), 1)
    tiles = [as_bf16(column - jnp.int16(128 * j) == lanes) for j in range(count // 128)]
    return jnp.concatenate(tiles, axis=1)


def place_rows(row, count):
    lines = lax.broadcasted_iota(jnp.int16, (128, 128), 0)
    wide = jnp.broadcast_to(row, (128, 128)).astype(jnp.int16)
    tiles = [as_bf16(wide - jnp.int16(128 * j) == lines) for j in range(count // 128)]
    return jnp.concatenate(tiles, axis=0)


def split(value):
    high = value.astype(BF16)
    low = (value - high.astype(F32)).astype(BF16)
    return jnp.concatenate([high, low], axis=1)


def joined(value):
    return value[:, :128] + value[:, 128:]


def pack_kernel(*refs):
    sources, (near, far), landed, (lists, arrive) = refs[:4], refs[4:6], refs[6:9], refs[9:]
    loads = [
        pltpu.make_async_copy(a, b, arrive.at[k])
        for k, (a, b) in enumerate(zip(sources, (lists, *landed)))
    ]
    for load in loads:
        load.start()
    nodes = landed[0]
    for load in loads[:2]:
        load.wait()
    core = lax.axis_index("c")
    near[...] = dot(pick_rows(lists[pl.ds(1 - core, 1), :], 512), nodes[...]).astype(BF16)
    far[...] = dot(pick_rows(lists[pl.ds(core, 1), :], 512), nodes[...]).astype(BF16)
    for load in loads[2:]:
        load.wait()


def norm_forward(second):
    average = jnp.mean(second, axis=-1, keepdims=True)
    centred = second - average
    variance = jnp.mean(centred * centred, axis=-1, keepdims=True)
    inverse = lax.rsqrt(variance + EPSILON)
    return centred * inverse, inverse


def norm_backward(cot, normed, inverse, gain):
    scaled = cot * gain
    return inverse * (
        scaled
        - jnp.mean(scaled, axis=-1, keepdims=True)
        - normed * jnp.mean(scaled * normed, axis=-1, keepdims=True)
    )


def partial_sum(value):
    return jnp.sum(value.reshape(-1, 8, 128), axis=0)


def total(value):
    return jnp.sum(value, axis=0, keepdims=True)


def prepare_kernel(nodes, senders, receivers, count, *refs):
    sources, landed, (receiver, partial, live, pick_send, pick_recv, place_recv, place_send), (arrive,) = (
        refs[:15], refs[15:30], refs[30:37], refs[37:],
    )
    loads = [pltpu.make_async_copy(a, b, arrive.at[k]) for k, (a, b) in enumerate(zip(sources, landed))]
    for load in loads:
        load.start()
    edges, ew1, eb1 = landed[:3]
    line = lax.broadcasted_iota(jnp.int32, (512, 128), 0)
    live[...] = jnp.where(line < count[0:1, 0:1] * 128, 1.0, 0.0).astype(F32)
    for b in range(4):
        rows = pl.ds(b * 128, 128)
        send_row, recv_row = senders[pl.ds(b, 1), :], receivers[pl.ds(b, 1), :]
        pick_send[rows, :] = pick_rows(send_row, 768)
        pick_recv[rows, :] = pick_rows(recv_row, 512)
        place_recv[:, rows] = place_rows(recv_row, 512)
        place_send[:, rows] = place_rows(send_row, 768)
    for load in loads:
        load.wait()
    low = dot(pick_recv[...], nodes[...]).astype(BF16)
    receiver[...] = low
    partial[...] = dot(jnp.concatenate([edges[...], low], axis=1), around(ew1)) + eb1[...]


def around(weight):
    return jnp.concatenate([weight[0:128, :], weight[256:384, :]], axis=0)


def main_kernel(near, far, nodes, *refs):
    (
        (edges, ew1, _, ew2, eb2, egain, eshift, nw1, nb1, nw2, nb2, ngain, nshift, node_cot, edge_cot),
        (receiver, partial, live, pick_send, pick_recv, place_recv, place_send),
        (node_out, edge_out, grad_edge, local_grad, keep, send),
        left,
        (
            table, messages, hidden, slope, normed, inverse, spread, dxs, dxr, sender, first_low, second_low,
            node_inputs, node_hidden, node_first, node_second, leave,
        ),
    ) = refs[:15], refs[15:22], refs[22:28], refs[28:31], refs[31:]
    stores = [
        pltpu.make_async_copy(a, b, leave.at[k])
        for k, (a, b) in enumerate(zip(left, (edge_out, node_out, grad_edge)))
    ]
    edge_left, node_left, grad_left = left
    core = lax.axis_index("c")
    table[pl.ds(0, 512), :] = nodes[...]
    table[pl.ds(pl.multiple_of(640 - 128 * core, 128), 128), :] = near[...]
    place = lax.axis_index("y") * lax.axis_size("z") + lax.axis_index("z")
    last = lax.axis_size("y") * lax.axis_size("z") - 1
    alone = place == core * last
    table[pl.ds(pl.multiple_of(512 + 128 * core, 128), 128), :] = jnp.where(alone, 0.0, far[...].astype(F32)).astype(BF16)

    own = edges[...]
    low = dot(pick_send[...], table[...]).astype(BF16)
    sender[...] = low
    first = partial[...] + dot(low, ew1[128:256, :])
    sigmoid = jax.nn.sigmoid(first)
    low = (first * sigmoid).astype(BF16)
    hidden[...] = low
    slope[...] = sigmoid * (1.0 + first * (1.0 - sigmoid))
    n, inv = norm_forward(dot(low, ew2[...]) + eb2[...])
    normed[...] = n
    inverse[...] = inv
    message = (n * egain[...] + eshift[...]) * live[...]
    edge_left[...] = (own.astype(F32) + message).astype(BF16)
    messages[...] = split(message)

    stores[0].start()
    sums = [jnp.zeros((8, 128), F32) for _ in range(8)]
    aggregate = joined(dot(place_recv[...], messages[...])).astype(BF16)
    own = nodes[...]
    gathered = jnp.concatenate([own, aggregate], axis=1)
    node_inputs[...] = gathered
    first = dot(gathered, nw1[...]) + nb1[...]
    sigmoid = jax.nn.sigmoid(first)
    low = (first * sigmoid).astype(BF16)
    node_hidden[...] = low
    n, inv = norm_forward(dot(low, nw2[...]) + nb2[...])
    node_left[...] = (own.astype(F32) + (n * ngain[...] + nshift[...])).astype(BF16)
    cot = node_cot[...].astype(F32)
    g2 = norm_backward(cot, n, inv, ngain[...])
    g2_low = g2.astype(BF16)
    g1 = dot_nt(g2_low, nw2[...]) * (sigmoid * (1.0 + first * (1.0 - sigmoid)))
    g1_low = g1.astype(BF16)
    node_first[...] = g1_low
    node_second[...] = g2_low
    back = dot_nt(g1_low, nw1[...])
    local_grad[...] = cot + back[:, :128]
    spread[...] = split(back[:, 128:])
    for k, piece in enumerate((g1, g2, cot * n, cot)):
        sums[4 + k] += partial_sum(piece)
    stores[1].start()

    edge_grad = edge_cot[...].astype(F32)
    cot = live[...] * (edge_grad + joined(dot(pick_recv[...], spread[...])))
    n = normed[...]
    g2 = norm_backward(cot, n, inverse[...], egain[...])
    g2_low = g2.astype(BF16)
    g1 = dot_nt(g2_low, ew2[...]) * slope[...]
    g1_low = g1.astype(BF16)
    first_low[...] = g1_low
    second_low[...] = g2_low
    back = dot_nt(g1_low, ew1[...])
    grad_left[...] = (edge_grad + back[:, :128]).astype(BF16)
    dxs[...] = split(back[:, 128:256])
    dxr[...] = split(back[:, 256:])
    for k, piece in enumerate((g1, g2, cot * n, cot)):
        sums[k] += partial_sum(piece)
    stores[2].start()

    lower = joined(dot(place_send[512:640, :], dxs[...])).astype(BF16)
    upper = joined(dot(place_send[640:768, :], dxs[...])).astype(BF16)
    is_first = core == 0
    send[ROWS : ROWS + 128, :] = jnp.where(is_first, upper, lower)
    send[ROWS + 128 :, :] = jnp.where(is_first, lower, upper)

    keep[0:128, :] = dot_tn(edges[...], first_low[...])
    keep[128:256, :] = dot_tn(sender[...], first_low[...])
    keep[256:384, :] = dot_tn(receiver[...], first_low[...])
    keep[384:385, :] = total(sums[0])
    keep[385:513, :] = dot_tn(hidden[...], second_low[...])
    keep[513:514, :] = total(sums[1])
    keep[514:515, :] = total(sums[2])
    keep[515:516, :] = total(sums[3])
    keep[516:772, :] = dot_tn(node_inputs[...], node_first[...])
    keep[772:773, :] = total(sums[4])
    keep[773:901, :] = dot_tn(node_hidden[...], node_second[...])
    keep[901:902, :] = total(sums[5])
    keep[902:903, :] = total(sums[6])
    keep[903:904, :] = total(sums[7])
    keep[904:1024, :] = jnp.zeros((120, 128), F32)
    send[0:ROWS, :] = keep[...].astype(BF16)

    for b in range(4):
        rows = pl.ds(b * 128, 128)
        both = dot(place_send[rows, :], dxs[...]) + dot(place_recv[rows, :], dxr[...])
        local_grad[rows, :] += joined(both)
    for store in stores:
        store.wait()


def finish_kernel(
    local_grad, near, turned, downward, result, received, lists, grad_node, weight_grads, node_left, weight_left, leave
):
    core = lax.axis_index("c")
    is_first = core == 0
    stores = [
        pltpu.make_async_copy(weight_left, weight_grads, leave.at[0]),
        pltpu.make_async_copy(node_left, grad_node, leave.at[1]),
    ]
    whole = jnp.where(is_first, received[0:LIVE_ROWS, :].astype(F32), result[0:LIVE_ROWS, :].astype(F32))
    weight_left[...] = whole
    stores[0].start()
    far = jnp.where(is_first, turned[0:128, :].astype(F32), downward[...].astype(F32)).astype(BF16)
    added = dot(place_rows(lists[pl.ds(1 - core, 1), :], 512), near[...])
    added += dot(place_rows(lists[pl.ds(core, 1), :], 512), far)
    node_left[...] = (local_grad[...] + added).astype(BF16)
    stores[1].start()
    for store in stores:
        store.wait()


def call(body, out_shape, operands, in_specs=None, out_specs=None, scratch=(), flops=1000000, vmem=None):
    return pl.pallas_call(
        body,
        out_shape=out_shape,
        in_specs=in_specs or [VMEM] * len(operands),
        out_specs=out_specs or jax.tree.map(lambda _: VMEM, out_shape),
        scratch_shapes=scratch,
        compiler_params=pltpu.CompilerParams(vmem_limit_bytes=vmem),
        cost_estimate=pl.CostEstimate(flops=flops, bytes_accessed=1000000, transcendentals=0),
    )(*operands)


def in_hbm(value):
    return pltpu.with_memory_space_constraint(value, pltpu.HBM)


def shape(rows, width, kind):
    return jax.ShapeDtypeStruct((rows, width), kind)


def prepare(early, sources):
    outs = tuple(jax.ShapeDtypeStruct(source.shape, source.dtype) for source in sources) + (
        shape(512, 128, BF16), shape(512, 128, F32), shape(512, 128, F32), shape(512, 768, BF16),
        shape(512, 512, BF16), shape(512, 512, BF16), shape(768, 512, BF16),
    )
    return call(
        prepare_kernel, outs, (*early, *(in_hbm(source) for source in sources)),
        [VMEM] * 4 + [HBM] * 15, scratch=[pltpu.SemaphoreType.DMA((15,))], flops=400000000, vmem=16 << 20,
    )


def compute(near, far, nodes, prepared):
    outs = (
        shape(512, 128, BF16), shape(512, 128, BF16), shape(512, 128, BF16), shape(512, 128, F32),
        shape(ROWS, 128, F32), shape(ROWS + 256, 128, BF16),
    )
    scratch = [
        pltpu.VMEM(dims, kind)
        for dims, kind in (
            ((512, 128), BF16), ((512, 128), BF16), ((512, 128), BF16),
            ((768, 128), BF16), ((512, 256), BF16), ((512, 128), BF16), ((512, 128), F32),
            ((512, 128), F32), ((512, 1), F32), ((512, 256), BF16), ((512, 256), BF16), ((512, 256), BF16),
            ((512, 128), BF16), ((512, 128), BF16), ((512, 128), BF16), ((512, 256), BF16), ((512, 128), BF16),
            ((512, 128), BF16), ((512, 128), BF16),
        )
    ] + [pltpu.SemaphoreType.DMA((3,))]
    return call(
        main_kernel, outs, (near, far, nodes, *prepared), [VMEM] * 25,
        (HBM,) * 3 + (VMEM,) * 3, scratch, 2000000000, 24 << 20,
    )


def layer(
    nodes, edges, senders, receivers, block_count, send_rows, node_cot, edge_cot,
    edge_w1, edge_b1, edge_w2, edge_b2, edge_gain, edge_shift,
    node_w1, node_b1, node_w2, node_b2, node_gain, node_shift,
):
    own_nodes = nodes[0]
    lists = send_rows[0, 0]
    line = lambda vector: vector.reshape(1, 128)
    near_pairs = [(j, j ^ 1) for j in range(64)]
    beside = {0: 0, 63: 63} | {j: j + 1 for j in range(1, 63, 2)} | {j + 1: j for j in range(1, 63, 2)}
    far_pairs = [
        (4 * j + x, 4 * k + (x ^ 1 if j == k else x)) for j, k in beside.items() for x in range(4)
    ]
    down = [(j, j - 2) for j in range(2, 64, 2)]
    up = [(j - 2, j) for j in range(2, 64, 2)]

    outs = (
        shape(128, 128, BF16), shape(128, 128, BF16), shape(512, 128, BF16), shape(4, 128, jnp.int32),
        shape(4, 128, jnp.int32),
    )
    near, far, *early = call(
        pack_kernel, outs,
        (in_hbm(lists), in_hbm(own_nodes), in_hbm(senders[0]), in_hbm(receivers[0])), [HBM] * 4,
        scratch=[pltpu.VMEM((2, 128), jnp.int32), pltpu.SemaphoreType.DMA((4,))],
        vmem=SMALL,
    )
    block_count, far = lax.optimization_barrier((block_count, far))
    early.append(jnp.pad(block_count, ((0, 7), (0, 127))))
    far = lax.ppermute(far, (*DOM, "x"), far_pairs)
    near = lax.ppermute(near, DOM, near_pairs)

    sources = (
        edges[0].reshape(512, 128),
        edge_w1, line(edge_b1), edge_w2, line(edge_b2), line(edge_gain), line(edge_shift),
        node_w1, line(node_b1), node_w2, line(node_b2), line(node_gain), line(node_shift),
        node_cot[0], edge_cot[0].reshape(512, 128),
    )
    prepared = prepare(early, sources)
    node_out, edge_out, grad_edge, local_grad, keep, send = compute(near, far, early[0], prepared)

    scale = 1.0 / math.sqrt(lax.axis_size(DOM) * lax.axis_size("x") * 512)
    planes, columns = lax.axis_size(PLANE), lax.axis_size(COLUMN)
    arrived = lax.ppermute(send, "c", [(0, 1), (1, 0)])
    pair = (keep + arrived[:ROWS].astype(F32)).astype(BF16)
    near_back = arrived[ROWS : ROWS + 128]

    def carry(pair, mine, other):
        upward, downward = lax.ppermute(other, DOM, up), lax.ppermute(mine, DOM, down)
        return pair, jnp.concatenate([upward, downward], axis=0)

    def reduce(pair, mine, other):
        tiles = lax.all_to_all(pair.reshape(planes, -1, 128), PLANE, 0, 0, tiled=True)
        piece = (jnp.sum(tiles.astype(F32), axis=0) * 0.0625).astype(BF16)
        copies = jnp.broadcast_to(piece, (columns, *piece.shape))
        tiles = lax.all_to_all(copies, COLUMN, 0, 0, tiled=True)
        piece = (jnp.sum(tiles.astype(F32), axis=0) * (16.0 * scale)).astype(BF16)
        copies = jnp.broadcast_to(piece, (planes, *piece.shape))
        tiles = lax.all_to_all(copies, PLANE, 0, 0, tiled=True)
        whole = tiles.reshape(ROWS, 128)
        return whole, whole[0:256]

    result, turned = lax.cond(
        lax.axis_index("c") == 0, carry, reduce, pair, send[ROWS + 128 :], arrived[ROWS + 128 :]
    )
    received = lax.ppermute(result, "c", [(0, 1), (1, 0)])
    downward = lax.ppermute(turned[128:], "c", [(0, 1), (1, 0)])
    grad_node, weight_grads = call(
        finish_kernel, (shape(512, 128, BF16), shape(LIVE_ROWS, 128, F32)),
        (local_grad, near_back, turned, downward, result, received, lists), [VMEM] * 7, (HBM,) * 2,
        [
            pltpu.VMEM((512, 128), BF16), pltpu.VMEM((LIVE_ROWS, 128), F32), pltpu.SemaphoreType.DMA((2,))
        ],
        vmem=SMALL,
    )
    return (
        node_out[None],
        edge_out.reshape(1, 4, 128, 128),
        grad_node[None],
        grad_edge.reshape(1, 4, 128, 128),
        weight_grads.reshape(LIVE_ROWS * 128),
    )


def solution(mesh):
    finer = Mesh(mesh.devices.reshape(4, 8, 2, mesh.shape["grp"]), ("y", "z", "c", "x"))
    by_row = P("x", DOM)
    return jax.shard_map(
        layer,
        mesh=finer,
        in_specs=(by_row,) * 8 + (P(),) * 12,
        out_specs=(by_row,) * 4 + (P(),),
        check_vma=False,
    )
```

```python
import math

import jax
import jax.numpy as jnp
from jax import lax
from jax.experimental import pallas as pl
from jax.experimental.pallas import tpu as pltpu
from jax.sharding import Mesh
from jax.sharding import PartitionSpec as P

DOM = ("y", "z", "c")
PLANE = ("y", "x")
COLUMN = ("z",)
EPSILON = 1e-05
F32 = jnp.float32
BF16 = jnp.bfloat16
ROWS = 1024
LIVE_ROWS = 904
SMALL = 8 << 20
VMEM = pl.BlockSpec(memory_space=pltpu.VMEM)
SMEM = pl.BlockSpec(memory_space=pltpu.SMEM)
HBM = pl.BlockSpec(memory_space=pltpu.HBM)


def dot(left, right):
    return jnp.dot(left, right, preferred_element_type=F32)


def dot_nt(left, right):
    return lax.dot_general(left, right, (((1,), (1,)), ((), ())), preferred_element_type=F32)


def dot_tn(left, right):
    return lax.dot_general(left, right, (((0,), (0,)), ((), ())), preferred_element_type=F32)


def as_bf16(mask):
    return jnp.where(mask, jnp.ones((), BF16), jnp.zeros((), BF16))


def pick_rows(row, count):
    column = jnp.transpose(jnp.broadcast_to(row, (128, 128))).astype(jnp.int16)
    lanes = lax.broadcasted_iota(jnp.int16, (128, 128), 1)
    tiles = [as_bf16(column - jnp.int16(128 * j) == lanes) for j in range(count // 128)]
    return jnp.concatenate(tiles, axis=1)


def place_rows(row, count):
    lines = lax.broadcasted_iota(jnp.int16, (128, 128), 0)
    wide = jnp.broadcast_to(row, (128, 128)).astype(jnp.int16)
    tiles = [as_bf16(wide - jnp.int16(128 * j) == lines) for j in range(count // 128)]
    return jnp.concatenate(tiles, axis=0)


def split(value):
    high = value.astype(BF16)
    low = (value - high.astype(F32)).astype(BF16)
    return jnp.concatenate([high, low], axis=1)


def joined(value):
    return value[:, :128] + value[:, 128:]


def pack_kernel(*refs):
    sources, (near, far), landed, (lists, arrive) = refs[:4], refs[4:6], refs[6:9], refs[9:]
    loads = [
        pltpu.make_async_copy(a, b, arrive.at[k])
        for k, (a, b) in enumerate(zip(sources, (lists, *landed)))
    ]
    for load in loads:
        load.start()
    nodes = landed[0]
    for load in loads[:2]:
        load.wait()
    core = lax.axis_index("c")
    near[...] = dot(pick_rows(lists[pl.ds(1 - core, 1), :], 512), nodes[...]).astype(BF16)
    far[...] = dot(pick_rows(lists[pl.ds(core, 1), :], 512), nodes[...]).astype(BF16)
    for load in loads[2:]:
        load.wait()


def norm_forward(second):
    average = jnp.mean(second, axis=-1, keepdims=True)
    centred = second - average
    variance = jnp.mean(centred * centred, axis=-1, keepdims=True)
    inverse = lax.rsqrt(variance + EPSILON)
    return centred * inverse, inverse


def norm_backward(cot, normed, inverse, gain):
    scaled = cot * gain
    return inverse * (
        scaled
        - jnp.mean(scaled, axis=-1, keepdims=True)
        - normed * jnp.mean(scaled * normed, axis=-1, keepdims=True)
    )


def partial_sum(value):
    return jnp.sum(value.reshape(-1, 8, 128), axis=0)


def total(value):
    return jnp.sum(value, axis=0, keepdims=True)


def prepare_kernel(nodes, senders, receivers, count, *refs):
    (
        sources, landed,
        (sender, receiver, partial, node_partial, live, pick_halo, pick_recv, place_recv, place_send),
        (pick_own, arrive),
    ) = refs[:15], refs[15:30], refs[30:39], refs[39:]
    loads = [pltpu.make_async_copy(a, b, arrive.at[k]) for k, (a, b) in enumerate(zip(sources, landed))]
    for load in loads:
        load.start()
    edges, ew1, eb1, _, _, _, _, nw1, nb1 = landed[:9]
    line = lax.broadcasted_iota(jnp.int32, (512, 128), 0)
    live[...] = jnp.where(line < count[0:1, 0:1] * 128, 1.0, 0.0).astype(F32)
    for b in range(4):
        rows = pl.ds(b * 128, 128)
        send_row, recv_row = senders[pl.ds(b, 1), :], receivers[pl.ds(b, 1), :]
        picked = pick_rows(send_row, 768)
        pick_own[rows, :] = picked[:, 0:512]
        pick_halo[rows, :] = picked[:, 512:768]
        pick_recv[rows, :] = pick_rows(recv_row, 512)
        place_recv[:, rows] = place_rows(recv_row, 512)
        place_send[:, rows] = place_rows(send_row, 768)
    sent = dot(pick_own[...], nodes[...]).astype(BF16)
    sender[...] = sent
    low = dot(pick_recv[...], nodes[...]).astype(BF16)
    receiver[...] = low
    for load in loads:
        load.wait()
    partial[...] = dot(jnp.concatenate([edges[...], sent, low], axis=1), ew1[...]) + eb1[...]
    node_partial[...] = dot(nodes[...], nw1[0:128, :]) + nb1[...]


def main_kernel(near, far, nodes, *refs):
    (
        (edges, ew1, _, ew2, eb2, egain, eshift, nw1, nb1, nw2, nb2, ngain, nshift, node_cot, edge_cot),
        (own_sender, receiver, partial, node_partial, live, pick_halo, pick_recv, place_recv, place_send),
        (node_out, edge_out, grad_edge, local_grad, keep, send),
        left,
        (
            halo, messages, hidden, slope, normed, inverse, spread, dxs, dxr, sender, first_low, second_low,
            aggregated, node_hidden, node_first, node_second, leave,
        ),
    ) = refs[:15], refs[15:24], refs[24:30], refs[30:33], refs[33:]
    stores = [
        pltpu.make_async_copy(a, b, leave.at[k])
        for k, (a, b) in enumerate(zip(left, (edge_out, node_out, grad_edge)))
    ]
    edge_left, node_left, grad_left = left
    core = lax.axis_index("c")
    halo[pl.ds(pl.multiple_of(128 - 128 * core, 128), 128), :] = near[...]
    place = lax.axis_index("y") * lax.axis_size("z") + lax.axis_index("z")
    last = lax.axis_size("y") * lax.axis_size("z") - 1
    alone = place == core * last
    halo[pl.ds(pl.multiple_of(128 * core, 128), 128), :] = jnp.where(alone, 0.0, far[...].astype(F32)).astype(BF16)

    own = edges[...]
    low = dot(pick_halo[...], halo[...]).astype(BF16)
    sender[...] = own_sender[...] + low
    first = partial[...] + dot(low, ew1[128:256, :])
    sigmoid = jax.nn.sigmoid(first)
    low = (first * sigmoid).astype(BF16)
    hidden[...] = low
    slope[...] = sigmoid * (1.0 + first * (1.0 - sigmoid))
    n, inv = norm_forward(dot(low, ew2[...]) + eb2[...])
    normed[...] = n
    inverse[...] = inv
    message = (n * egain[...] + eshift[...]) * live[...]
    edge_left[...] = (own.astype(F32) + message).astype(BF16)
    messages[...] = split(message)

    stores[0].start()
    sums = [jnp.zeros((8, 128), F32) for _ in range(8)]
    aggregate = joined(dot(place_recv[...], messages[...])).astype(BF16)
    own = nodes[...]
    aggregated[...] = aggregate
    first = node_partial[...] + dot(aggregate, nw1[128:256, :])
    sigmoid = jax.nn.sigmoid(first)
    low = (first * sigmoid).astype(BF16)
    node_hidden[...] = low
    n, inv = norm_forward(dot(low, nw2[...]) + nb2[...])
    node_left[...] = (own.astype(F32) + (n * ngain[...] + nshift[...])).astype(BF16)
    cot = node_cot[...].astype(F32)
    g2 = norm_backward(cot, n, inv, ngain[...])
    g2_low = g2.astype(BF16)
    g1 = dot_nt(g2_low, nw2[...]) * (sigmoid * (1.0 + first * (1.0 - sigmoid)))
    g1_low = g1.astype(BF16)
    node_first[...] = g1_low
    node_second[...] = g2_low
    back = dot_nt(g1_low, nw1[...])
    local_grad[...] = cot + back[:, :128]
    spread[...] = split(back[:, 128:])
    for k, piece in enumerate((g1, g2, cot * n, cot)):
        sums[4 + k] += partial_sum(piece)
    stores[1].start()

    edge_grad = edge_cot[...].astype(F32)
    cot = live[...] * (edge_grad + joined(dot(pick_recv[...], spread[...])))
    n = normed[...]
    g2 = norm_backward(cot, n, inverse[...], egain[...])
    g2_low = g2.astype(BF16)
    g1 = dot_nt(g2_low, ew2[...]) * slope[...]
    g1_low = g1.astype(BF16)
    first_low[...] = g1_low
    second_low[...] = g2_low
    back = dot_nt(g1_low, ew1[...])
    grad_left[...] = (edge_grad + back[:, :128]).astype(BF16)
    dxs[...] = split(back[:, 128:256])
    dxr[...] = split(back[:, 256:])
    for k, piece in enumerate((g1, g2, cot * n, cot)):
        sums[k] += partial_sum(piece)
    stores[2].start()

    lower = joined(dot(place_send[512:640, :], dxs[...])).astype(BF16)
    upper = joined(dot(place_send[640:768, :], dxs[...])).astype(BF16)
    is_first = core == 0
    send[ROWS : ROWS + 128, :] = jnp.where(is_first, upper, lower)
    send[ROWS + 128 :, :] = jnp.where(is_first, lower, upper)

    keep[0:128, :] = dot_tn(edges[...], first_low[...])
    keep[128:256, :] = dot_tn(sender[...], first_low[...])
    keep[256:384, :] = dot_tn(receiver[...], first_low[...])
    keep[384:385, :] = total(sums[0])
    keep[385:513, :] = dot_tn(hidden[...], second_low[...])
    keep[513:514, :] = total(sums[1])
    keep[514:515, :] = total(sums[2])
    keep[515:516, :] = total(sums[3])
    keep[516:644, :] = dot_tn(nodes[...], node_first[...])
    keep[644:772, :] = dot_tn(aggregated[...], node_first[...])
    keep[772:773, :] = total(sums[4])
    keep[773:901, :] = dot_tn(node_hidden[...], node_second[...])
    keep[901:902, :] = total(sums[5])
    keep[902:903, :] = total(sums[6])
    keep[903:904, :] = total(sums[7])
    keep[904:1024, :] = jnp.zeros((120, 128), F32)
    send[0:ROWS, :] = keep[...].astype(BF16)

    for b in range(4):
        rows = pl.ds(b * 128, 128)
        both = dot(place_send[rows, :], dxs[...]) + dot(place_recv[rows, :], dxr[...])
        local_grad[rows, :] += joined(both)
    for store in stores:
        store.wait()


def finish_kernel(
    local_grad, near, turned, downward, result, received, lists, grad_node, weight_grads, node_left, weight_left, leave
):
    core = lax.axis_index("c")
    is_first = core == 0
    stores = [
        pltpu.make_async_copy(weight_left, weight_grads, leave.at[0]),
        pltpu.make_async_copy(node_left, grad_node, leave.at[1]),
    ]
    whole = jnp.where(is_first, received[0:LIVE_ROWS, :].astype(F32), result[0:LIVE_ROWS, :].astype(F32))
    weight_left[...] = whole
    stores[0].start()
    far = jnp.where(is_first, turned[0:128, :].astype(F32), downward[...].astype(F32)).astype(BF16)
    added = dot(place_rows(lists[pl.ds(1 - core, 1), :], 512), near[...])
    added += dot(place_rows(lists[pl.ds(core, 1), :], 512), far)
    node_left[...] = (local_grad[...] + added).astype(BF16)
    stores[1].start()
    for store in stores:
        store.wait()


def call(body, out_shape, operands, in_specs=None, out_specs=None, scratch=(), flops=1000000, vmem=None):
    return pl.pallas_call(
        body,
        out_shape=out_shape,
        in_specs=in_specs or [VMEM] * len(operands),
        out_specs=out_specs or jax.tree.map(lambda _: VMEM, out_shape),
        scratch_shapes=scratch,
        compiler_params=pltpu.CompilerParams(vmem_limit_bytes=vmem),
        cost_estimate=pl.CostEstimate(flops=flops, bytes_accessed=1000000, transcendentals=0),
    )(*operands)


def in_hbm(value):
    return pltpu.with_memory_space_constraint(value, pltpu.HBM)


def shape(rows, width, kind):
    return jax.ShapeDtypeStruct((rows, width), kind)


def prepare(early, sources):
    outs = tuple(jax.ShapeDtypeStruct(source.shape, source.dtype) for source in sources) + (
        shape(512, 128, BF16), shape(512, 128, BF16), shape(512, 128, F32), shape(512, 128, F32),
        shape(512, 128, F32), shape(512, 256, BF16), shape(512, 512, BF16), shape(512, 512, BF16),
        shape(768, 512, BF16),
    )
    return call(
        prepare_kernel, outs, (*early, *(in_hbm(source) for source in sources)),
        [VMEM] * 4 + [HBM] * 15, scratch=[pltpu.VMEM((512, 512), BF16), pltpu.SemaphoreType.DMA((15,))], flops=400000000, vmem=16 << 20,
    )


def compute(near, far, nodes, prepared):
    outs = (
        shape(512, 128, BF16), shape(512, 128, BF16), shape(512, 128, BF16), shape(512, 128, F32),
        shape(ROWS, 128, F32), shape(ROWS + 256, 128, BF16),
    )
    scratch = [
        pltpu.VMEM(dims, kind)
        for dims, kind in (
            ((512, 128), BF16), ((512, 128), BF16), ((512, 128), BF16),
            ((256, 128), BF16), ((512, 256), BF16), ((512, 128), BF16), ((512, 128), F32),
            ((512, 128), F32), ((512, 1), F32), ((512, 256), BF16), ((512, 256), BF16), ((512, 256), BF16),
            ((512, 128), BF16), ((512, 128), BF16), ((512, 128), BF16), ((512, 128), BF16), ((512, 128), BF16),
            ((512, 128), BF16), ((512, 128), BF16),
        )
    ] + [pltpu.SemaphoreType.DMA((3,))]
    return call(
        main_kernel, outs, (near, far, nodes, *prepared), [VMEM] * 27,
        (HBM,) * 3 + (VMEM,) * 3, scratch, 2000000000, 24 << 20,
    )


def layer(
    nodes, edges, senders, receivers, block_count, send_rows, node_cot, edge_cot,
    edge_w1, edge_b1, edge_w2, edge_b2, edge_gain, edge_shift,
    node_w1, node_b1, node_w2, node_b2, node_gain, node_shift,
):
    own_nodes = nodes[0]
    lists = send_rows[0, 0]
    line = lambda vector: vector.reshape(1, 128)
    near_pairs = [(j, j ^ 1) for j in range(64)]
    beside = {0: 0, 63: 63} | {j: j + 1 for j in range(1, 63, 2)} | {j + 1: j for j in range(1, 63, 2)}
    far_pairs = [
        (4 * j + x, 4 * k + (x ^ 1 if j == k else x)) for j, k in beside.items() for x in range(4)
    ]
    down = [(j, j - 2) for j in range(2, 64, 2)]
    up = [(j - 2, j) for j in range(2, 64, 2)]

    outs = (
        shape(128, 128, BF16), shape(128, 128, BF16), shape(512, 128, BF16), shape(4, 128, jnp.int32),
        shape(4, 128, jnp.int32),
    )
    near, far, *early = call(
        pack_kernel, outs,
        (in_hbm(lists), in_hbm(own_nodes), in_hbm(senders[0]), in_hbm(receivers[0])), [HBM] * 4,
        scratch=[pltpu.VMEM((2, 128), jnp.int32), pltpu.SemaphoreType.DMA((4,))],
        vmem=SMALL,
    )
    block_count, far = lax.optimization_barrier((block_count, far))
    early.append(jnp.pad(block_count, ((0, 7), (0, 127))))
    far = lax.ppermute(far, (*DOM, "x"), far_pairs)
    near = lax.ppermute(near, DOM, near_pairs)

    sources = (
        edges[0].reshape(512, 128),
        edge_w1, line(edge_b1), edge_w2, line(edge_b2), line(edge_gain), line(edge_shift),
        node_w1, line(node_b1), node_w2, line(node_b2), line(node_gain), line(node_shift),
        node_cot[0], edge_cot[0].reshape(512, 128),
    )
    prepared = prepare(early, sources)
    node_out, edge_out, grad_edge, local_grad, keep, send = compute(near, far, early[0], prepared)

    scale = 1.0 / math.sqrt(lax.axis_size(DOM) * lax.axis_size("x") * 512)
    planes, columns = lax.axis_size(PLANE), lax.axis_size(COLUMN)
    arrived = lax.ppermute(send, "c", [(0, 1), (1, 0)])
    pair = (keep + arrived[:ROWS].astype(F32)).astype(BF16)
    near_back = arrived[ROWS : ROWS + 128]

    def carry(pair, mine, other):
        upward, downward = lax.ppermute(other, DOM, up), lax.ppermute(mine, DOM, down)
        return pair, jnp.concatenate([upward, downward], axis=0)

    def reduce(pair, mine, other):
        tiles = lax.all_to_all(pair.reshape(planes, -1, 128), PLANE, 0, 0, tiled=True)
        piece = (jnp.sum(tiles.astype(F32), axis=0) * 0.0625).astype(BF16)
        copies = jnp.broadcast_to(piece, (columns, *piece.shape))
        tiles = lax.all_to_all(copies, COLUMN, 0, 0, tiled=True)
        piece = (jnp.sum(tiles.astype(F32), axis=0) * (16.0 * scale)).astype(BF16)
        copies = jnp.broadcast_to(piece, (planes, *piece.shape))
        tiles = lax.all_to_all(copies, PLANE, 0, 0, tiled=True)
        whole = tiles.reshape(ROWS, 128)
        return whole, whole[0:256]

    result, turned = lax.cond(
        lax.axis_index("c") == 0, carry, reduce, pair, send[ROWS + 128 :], arrived[ROWS + 128 :]
    )
    received = lax.ppermute(result, "c", [(0, 1), (1, 0)])
    downward = lax.ppermute(turned[128:], "c", [(0, 1), (1, 0)])
    grad_node, weight_grads = call(
        finish_kernel, (shape(512, 128, BF16), shape(LIVE_ROWS, 128, F32)),
        (local_grad, near_back, turned, downward, result, received, lists), [VMEM] * 7, (HBM,) * 2,
        [
            pltpu.VMEM((512, 128), BF16), pltpu.VMEM((LIVE_ROWS, 128), F32), pltpu.SemaphoreType.DMA((2,))
        ],
        vmem=SMALL,
    )
    return (
        node_out[None],
        edge_out.reshape(1, 4, 128, 128),
        grad_node[None],
        grad_edge.reshape(1, 4, 128, 128),
        weight_grads.reshape(LIVE_ROWS * 128),
    )


def solution(mesh):
    finer = Mesh(mesh.devices.reshape(4, 8, 2, mesh.shape["grp"]), ("y", "z", "c", "x"))
    by_row = P("x", DOM)
    return jax.shard_map(
        layer,
        mesh=finer,
        in_specs=(by_row,) * 8 + (P(),) * 12,
        out_specs=(by_row,) * 4 + (P(),),
        check_vma=False,
    )
```

```python
import math

import jax
import jax.numpy as jnp
from jax import lax
from jax.experimental import pallas as pl
from jax.experimental.pallas import tpu as pltpu
from jax.sharding import Mesh
from jax.sharding import PartitionSpec as P

DOM = ("y", "z", "c")
PLANE = ("y", "x")
COLUMN = ("z",)
EPSILON = 1e-05
F32 = jnp.float32
BF16 = jnp.bfloat16
ROWS = 1024
LIVE_ROWS = 904
SMALL = 8 << 20
VMEM = pl.BlockSpec(memory_space=pltpu.VMEM)
SMEM = pl.BlockSpec(memory_space=pltpu.SMEM)
HBM = pl.BlockSpec(memory_space=pltpu.HBM)


def dot(left, right):
    return jnp.dot(left, right, preferred_element_type=F32)


def dot_nt(left, right):
    return lax.dot_general(left, right, (((1,), (1,)), ((), ())), preferred_element_type=F32)


def dot_tn(left, right):
    return lax.dot_general(left, right, (((0,), (0,)), ((), ())), preferred_element_type=F32)


def as_bf16(mask):
    return jnp.where(mask, jnp.ones((), BF16), jnp.zeros((), BF16))


def pick_rows(row, count):
    column = jnp.transpose(jnp.broadcast_to(row, (128, 128))).astype(jnp.int16)
    lanes = lax.broadcasted_iota(jnp.int16, (128, 128), 1)
    tiles = [as_bf16(column - jnp.int16(128 * j) == lanes) for j in range(count // 128)]
    return jnp.concatenate(tiles, axis=1)


def place_rows(row, count):
    lines = lax.broadcasted_iota(jnp.int16, (128, 128), 0)
    wide = jnp.broadcast_to(row, (128, 128)).astype(jnp.int16)
    tiles = [as_bf16(wide - jnp.int16(128 * j) == lines) for j in range(count // 128)]
    return jnp.concatenate(tiles, axis=0)


def split(value):
    high = value.astype(BF16)
    low = (value - high.astype(F32)).astype(BF16)
    return jnp.concatenate([high, low], axis=1)


def joined(value):
    return value[:, :128] + value[:, 128:]


def pack_kernel(*refs):
    sources, (near, far), landed, (lists, arrive) = refs[:4], refs[4:6], refs[6:9], refs[9:]
    loads = [
        pltpu.make_async_copy(a, b, arrive.at[k])
        for k, (a, b) in enumerate(zip(sources, (lists, *landed)))
    ]
    for load in loads:
        load.start()
    nodes = landed[0]
    for load in loads[:2]:
        load.wait()
    core = lax.axis_index("c")
    near[...] = dot(pick_rows(lists[pl.ds(1 - core, 1), :], 512), nodes[...]).astype(BF16)
    far[...] = dot(pick_rows(lists[pl.ds(core, 1), :], 512), nodes[...]).astype(BF16)
    for load in loads[2:]:
        load.wait()


def norm_forward(second):
    average = jnp.mean(second, axis=-1, keepdims=True)
    centred = second - average
    variance = jnp.mean(centred * centred, axis=-1, keepdims=True)
    inverse = lax.rsqrt(variance + EPSILON)
    return centred * inverse, inverse


def norm_backward(cot, normed, inverse, gain):
    scaled = cot * gain
    return inverse * (
        scaled
        - jnp.mean(scaled, axis=-1, keepdims=True)
        - normed * jnp.mean(scaled * normed, axis=-1, keepdims=True)
    )


def partial_sum(value):
    return jnp.sum(value.reshape(-1, 8, 128), axis=0)


def total(value):
    return jnp.sum(value, axis=0, keepdims=True)


def prepare_kernel(nodes, senders, receivers, count, *refs):
    (
        sources, landed,
        (sender, receiver, partial, node_partial, live, pick_halo, pick_recv, place_recv, place_send),
        (pick_own, arrive),
    ) = refs[:15], refs[15:30], refs[30:39], refs[39:]
    loads = [pltpu.make_async_copy(a, b, arrive.at[k]) for k, (a, b) in enumerate(zip(sources, landed))]
    for load in loads:
        load.start()
    edges, ew1, eb1, _, _, _, _, nw1, nb1 = landed[:9]
    line = lax.broadcasted_iota(jnp.int32, (512, 128), 0)
    live[...] = jnp.where(line < count[0:1, 0:1] * 128, 1.0, 0.0).astype(F32)
    for b in range(4):
        rows = pl.ds(b * 128, 128)
        send_row, recv_row = senders[pl.ds(b, 1), :], receivers[pl.ds(b, 1), :]
        picked = pick_rows(send_row, 768)
        pick_own[rows, :] = picked[:, 0:512]
        pick_halo[rows, :] = picked[:, 512:768]
        pick_recv[rows, :] = pick_rows(recv_row, 512)
        place_recv[:, rows] = place_rows(recv_row, 512)
        place_send[:, rows] = place_rows(send_row, 768)
    sent = dot(pick_own[...], nodes[...]).astype(BF16)
    sender[...] = sent
    low = dot(pick_recv[...], nodes[...]).astype(BF16)
    receiver[...] = low
    for load in loads:
        load.wait()
    partial[...] = dot(jnp.concatenate([edges[...], sent, low], axis=1), ew1[...]) + eb1[...]
    node_partial[...] = dot(nodes[...], nw1[0:128, :]) + nb1[...]


def main_kernel(near, far, nodes, *refs):
    (
        (edges, ew1, _, ew2, eb2, egain, eshift, nw1, nb1, nw2, nb2, ngain, nshift, node_cot, edge_cot),
        (own_sender, receiver, partial, node_partial, live, pick_halo, pick_recv, place_recv, place_send),
        (node_out, edge_out, grad_edge, local_grad, keep, send),
        left,
        (
            halo, messages, hidden, slope, normed, inverse, spread, dxs, dxr, sender, first_low, second_low,
            aggregated, node_hidden, node_first, node_second, leave,
        ),
    ) = refs[:15], refs[15:24], refs[24:30], refs[30:32], refs[32:]
    stores = [
        pltpu.make_async_copy(a, b, leave.at[k])
        for k, (a, b) in enumerate(zip(left, (edge_out, node_out)))
    ]
    edge_left, node_left = left
    core = lax.axis_index("c")
    halo[pl.ds(pl.multiple_of(128 - 128 * core, 128), 128), :] = near[...]
    place = lax.axis_index("y") * lax.axis_size("z") + lax.axis_index("z")
    last = lax.axis_size("y") * lax.axis_size("z") - 1
    alone = place == core * last
    halo[pl.ds(pl.multiple_of(128 * core, 128), 128), :] = jnp.where(alone, 0.0, far[...].astype(F32)).astype(BF16)

    own = edges[...]
    low = dot(pick_halo[...], halo[...]).astype(BF16)
    sender[...] = own_sender[...] + low
    first = partial[...] + dot(low, ew1[128:256, :])
    sigmoid = jax.nn.sigmoid(first)
    low = (first * sigmoid).astype(BF16)
    hidden[...] = low
    slope[...] = sigmoid * (1.0 + first * (1.0 - sigmoid))
    n, inv = norm_forward(dot(low, ew2[...]) + eb2[...])
    normed[...] = n
    inverse[...] = inv
    message = (n * egain[...] + eshift[...]) * live[...]
    edge_left[...] = (own.astype(F32) + message).astype(BF16)
    messages[...] = split(message)

    stores[0].start()
    sums = [jnp.zeros((8, 128), F32) for _ in range(8)]
    aggregate = joined(dot(place_recv[...], messages[...])).astype(BF16)
    own = nodes[...]
    aggregated[...] = aggregate
    first = node_partial[...] + dot(aggregate, nw1[128:256, :])
    sigmoid = jax.nn.sigmoid(first)
    low = (first * sigmoid).astype(BF16)
    node_hidden[...] = low
    n, inv = norm_forward(dot(low, nw2[...]) + nb2[...])
    node_left[...] = (own.astype(F32) + (n * ngain[...] + nshift[...])).astype(BF16)
    cot = node_cot[...].astype(F32)
    g2 = norm_backward(cot, n, inv, ngain[...])
    g2_low = g2.astype(BF16)
    g1 = dot_nt(g2_low, nw2[...]) * (sigmoid * (1.0 + first * (1.0 - sigmoid)))
    g1_low = g1.astype(BF16)
    node_first[...] = g1_low
    node_second[...] = g2_low
    back = dot_nt(g1_low, nw1[...])
    local_grad[...] = cot + back[:, :128]
    spread[...] = split(back[:, 128:])
    for k, piece in enumerate((g1, g2, cot * n, cot)):
        sums[4 + k] += partial_sum(piece)
    stores[1].start()

    edge_grad = edge_cot[...].astype(F32)
    cot = live[...] * (edge_grad + joined(dot(pick_recv[...], spread[...])))
    n = normed[...]
    g2 = norm_backward(cot, n, inverse[...], egain[...])
    g2_low = g2.astype(BF16)
    g1 = dot_nt(g2_low, ew2[...]) * slope[...]
    g1_low = g1.astype(BF16)
    first_low[...] = g1_low
    second_low[...] = g2_low
    back = dot_nt(g1_low, ew1[...])
    grad_edge[...] = (edge_grad + back[:, :128]).astype(BF16)
    dxs[...] = split(back[:, 128:256])
    dxr[...] = split(back[:, 256:])
    for k, piece in enumerate((g1, g2, cot * n, cot)):
        sums[k] += partial_sum(piece)

    lower = joined(dot(place_send[512:640, :], dxs[...])).astype(BF16)
    upper = joined(dot(place_send[640:768, :], dxs[...])).astype(BF16)
    is_first = core == 0
    send[ROWS : ROWS + 128, :] = jnp.where(is_first, upper, lower)
    send[ROWS + 128 :, :] = jnp.where(is_first, lower, upper)

    keep[0:128, :] = dot_tn(edges[...], first_low[...])
    keep[128:256, :] = dot_tn(sender[...], first_low[...])
    keep[256:384, :] = dot_tn(receiver[...], first_low[...])
    keep[384:385, :] = total(sums[0])
    keep[385:513, :] = dot_tn(hidden[...], second_low[...])
    keep[513:514, :] = total(sums[1])
    keep[514:515, :] = total(sums[2])
    keep[515:516, :] = total(sums[3])
    keep[516:644, :] = dot_tn(nodes[...], node_first[...])
    keep[644:772, :] = dot_tn(aggregated[...], node_first[...])
    keep[772:773, :] = total(sums[4])
    keep[773:901, :] = dot_tn(node_hidden[...], node_second[...])
    keep[901:902, :] = total(sums[5])
    keep[902:903, :] = total(sums[6])
    keep[903:904, :] = total(sums[7])
    keep[904:1024, :] = jnp.zeros((120, 128), F32)
    send[0:ROWS, :] = keep[...].astype(BF16)

    for b in range(4):
        rows = pl.ds(b * 128, 128)
        both = dot(place_send[rows, :], dxs[...]) + dot(place_recv[rows, :], dxr[...])
        local_grad[rows, :] += joined(both)
    for store in stores:
        store.wait()


def finish_kernel(
    local_grad, near, turned, downward, result, received, lists, edge_left,
    grad_node, weight_grads, grad_edge, node_left, weight_left, leave,
):
    core = lax.axis_index("c")
    is_first = core == 0
    stores = [
        pltpu.make_async_copy(weight_left, weight_grads, leave.at[0]),
        pltpu.make_async_copy(node_left, grad_node, leave.at[1]),
        pltpu.make_async_copy(edge_left, grad_edge, leave.at[2]),
    ]
    whole = jnp.where(is_first, received[0:LIVE_ROWS, :].astype(F32), result[0:LIVE_ROWS, :].astype(F32))
    weight_left[...] = whole
    stores[0].start()
    stores[2].start()
    far = jnp.where(is_first, turned[0:128, :].astype(F32), downward[...].astype(F32)).astype(BF16)
    added = dot(place_rows(lists[pl.ds(1 - core, 1), :], 512), near[...])
    added += dot(place_rows(lists[pl.ds(core, 1), :], 512), far)
    node_left[...] = (local_grad[...] + added).astype(BF16)
    stores[1].start()
    for store in stores:
        store.wait()


def call(body, out_shape, operands, in_specs=None, out_specs=None, scratch=(), flops=1000000, vmem=None):
    return pl.pallas_call(
        body,
        out_shape=out_shape,
        in_specs=in_specs or [VMEM] * len(operands),
        out_specs=out_specs or jax.tree.map(lambda _: VMEM, out_shape),
        scratch_shapes=scratch,
        compiler_params=pltpu.CompilerParams(vmem_limit_bytes=vmem),
        cost_estimate=pl.CostEstimate(flops=flops, bytes_accessed=1000000, transcendentals=0),
    )(*operands)


def in_hbm(value):
    return pltpu.with_memory_space_constraint(value, pltpu.HBM)


def shape(rows, width, kind):
    return jax.ShapeDtypeStruct((rows, width), kind)


def prepare(early, sources):
    outs = tuple(jax.ShapeDtypeStruct(source.shape, source.dtype) for source in sources) + (
        shape(512, 128, BF16), shape(512, 128, BF16), shape(512, 128, F32), shape(512, 128, F32),
        shape(512, 128, F32), shape(512, 256, BF16), shape(512, 512, BF16), shape(512, 512, BF16),
        shape(768, 512, BF16),
    )
    return call(
        prepare_kernel, outs, (*early, *(in_hbm(source) for source in sources)),
        [VMEM] * 4 + [HBM] * 15, scratch=[pltpu.VMEM((512, 512), BF16), pltpu.SemaphoreType.DMA((15,))], flops=400000000, vmem=16 << 20,
    )


def compute(near, far, nodes, prepared):
    outs = (
        shape(512, 128, BF16), shape(512, 128, BF16), shape(512, 128, BF16), shape(512, 128, F32),
        shape(ROWS, 128, F32), shape(ROWS + 256, 128, BF16),
    )
    scratch = [
        pltpu.VMEM(dims, kind)
        for dims, kind in (
            ((512, 128), BF16), ((512, 128), BF16),
            ((256, 128), BF16), ((512, 256), BF16), ((512, 128), BF16), ((512, 128), F32),
            ((512, 128), F32), ((512, 1), F32), ((512, 256), BF16), ((512, 256), BF16), ((512, 256), BF16),
            ((512, 128), BF16), ((512, 128), BF16), ((512, 128), BF16), ((512, 128), BF16), ((512, 128), BF16),
            ((512, 128), BF16), ((512, 128), BF16),
        )
    ] + [pltpu.SemaphoreType.DMA((2,))]
    return call(
        main_kernel, outs, (near, far, nodes, *prepared), [VMEM] * 27,
        (HBM,) * 2 + (VMEM,) * 4, scratch, 2000000000, 24 << 20,
    )


def layer(
    nodes, edges, senders, receivers, block_count, send_rows, node_cot, edge_cot,
    edge_w1, edge_b1, edge_w2, edge_b2, edge_gain, edge_shift,
    node_w1, node_b1, node_w2, node_b2, node_gain, node_shift,
):
    own_nodes = nodes[0]
    lists = send_rows[0, 0]
    line = lambda vector: vector.reshape(1, 128)
    near_pairs = [(j, j ^ 1) for j in range(64)]
    beside = {0: 0, 63: 63} | {j: j + 1 for j in range(1, 63, 2)} | {j + 1: j for j in range(1, 63, 2)}
    far_pairs = [
        (4 * j + x, 4 * k + (x ^ 1 if j == k else x)) for j, k in beside.items() for x in range(4)
    ]
    down = [(j, j - 2) for j in range(2, 64, 2)]
    up = [(j - 2, j) for j in range(2, 64, 2)]

    outs = (
        shape(128, 128, BF16), shape(128, 128, BF16), shape(512, 128, BF16), shape(4, 128, jnp.int32),
        shape(4, 128, jnp.int32),
    )
    near, far, *early = call(
        pack_kernel, outs,
        (in_hbm(lists), in_hbm(own_nodes), in_hbm(senders[0]), in_hbm(receivers[0])), [HBM] * 4,
        scratch=[pltpu.VMEM((2, 128), jnp.int32), pltpu.SemaphoreType.DMA((4,))],
        vmem=SMALL,
    )
    block_count, far = lax.optimization_barrier((block_count, far))
    early.append(jnp.pad(block_count, ((0, 7), (0, 127))))
    far = lax.ppermute(far, (*DOM, "x"), far_pairs)
    near = lax.ppermute(near, DOM, near_pairs)

    sources = (
        edges[0].reshape(512, 128),
        edge_w1, line(edge_b1), edge_w2, line(edge_b2), line(edge_gain), line(edge_shift),
        node_w1, line(node_b1), node_w2, line(node_b2), line(node_gain), line(node_shift),
        node_cot[0], edge_cot[0].reshape(512, 128),
    )
    prepared = prepare(early, sources)
    node_out, edge_out, grad_edge, local_grad, keep, send = compute(near, far, early[0], prepared)

    scale = 1.0 / math.sqrt(lax.axis_size(DOM) * lax.axis_size("x") * 512)
    planes, columns = lax.axis_size(PLANE), lax.axis_size(COLUMN)
    arrived = lax.ppermute(send, "c", [(0, 1), (1, 0)])
    pair = (keep + arrived[:ROWS].astype(F32)).astype(BF16)
    near_back = arrived[ROWS : ROWS + 128]

    def carry(pair, mine, other):
        upward, downward = lax.ppermute(other, DOM, up), lax.ppermute(mine, DOM, down)
        return pair, jnp.concatenate([upward, downward], axis=0)

    def reduce(pair, mine, other):
        tiles = lax.all_to_all(pair.reshape(planes, -1, 128), PLANE, 0, 0, tiled=True)
        piece = (jnp.sum(tiles.astype(F32), axis=0) * 0.0625).astype(BF16)
        copies = jnp.broadcast_to(piece, (columns, *piece.shape))
        tiles = lax.all_to_all(copies, COLUMN, 0, 0, tiled=True)
        piece = (jnp.sum(tiles.astype(F32), axis=0) * (16.0 * scale)).astype(BF16)
        copies = jnp.broadcast_to(piece, (planes, *piece.shape))
        tiles = lax.all_to_all(copies, PLANE, 0, 0, tiled=True)
        whole = tiles.reshape(ROWS, 128)
        return whole, whole[0:256]

    result, turned = lax.cond(
        lax.axis_index("c") == 0, carry, reduce, pair, send[ROWS + 128 :], arrived[ROWS + 128 :]
    )
    received = lax.ppermute(result, "c", [(0, 1), (1, 0)])
    downward = lax.ppermute(turned[128:], "c", [(0, 1), (1, 0)])
    grad_node, weight_grads, grad_edge = call(
        finish_kernel, (shape(512, 128, BF16), shape(LIVE_ROWS, 128, F32), shape(512, 128, BF16)),
        (local_grad, near_back, turned, downward, result, received, lists, grad_edge), [VMEM] * 8, (HBM,) * 3,
        [
            pltpu.VMEM((512, 128), BF16), pltpu.VMEM((LIVE_ROWS, 128), F32), pltpu.SemaphoreType.DMA((3,))
        ],
        vmem=SMALL,
    )
    return (
        node_out[None],
        edge_out.reshape(1, 4, 128, 128),
        grad_node[None],
        grad_edge.reshape(1, 4, 128, 128),
        weight_grads.reshape(LIVE_ROWS * 128),
    )


def solution(mesh):
    finer = Mesh(mesh.devices.reshape(4, 8, 2, mesh.shape["grp"]), ("y", "z", "c", "x"))
    by_row = P("x", DOM)
    return jax.shard_map(
        layer,
        mesh=finer,
        in_specs=(by_row,) * 8 + (P(),) * 12,
        out_specs=(by_row,) * 4 + (P(),),
        check_vma=False,
    )
```
